8 devices in a mesh: dp: 1 (over z), ei: 2 (over y), eo: 4 (over x, core).
Axes of the slice: x: 2, y: 2, z: 1, core: 2. Of those that a mesh axis runs over, the one named last changes fastest.
Arguments:
- x_tokens: bfloat16 [512, 1536], P(('dp', 'ei', 'eo'))
- expert_idx: int32 [512, 8], P(('dp', 'ei', 'eo'))
- gate_vals: float32 [512, 8], P(('dp', 'ei', 'eo'))
- dy_tokens: bfloat16 [512, 1536], P(('dp', 'ei', 'eo'))
- w_gate: bfloat16 [40, 1536, 512], P(('ei', 'eo'))
- w_up: bfloat16 [40, 1536, 512], P(('ei', 'eo'))
- w_down: bfloat16 [40, 512, 1536], P(('ei', 'eo'))
- x_attn: bfloat16 [8, 64, 1536], P(('dp', 'ei', 'eo'))
- w_query: bfloat16 [1536, 24, 64], P(None, ('ei', 'eo'))
- w_key: bfloat16 [1536, 8, 64], P(None, ('ei', 'eo'))
- w_value: bfloat16 [1536, 8, 64], P(None, ('ei', 'eo'))
- w_out: bfloat16 [24, 64, 1536], P(('ei', 'eo'))
Outputs:
- output 1: bfloat16 [512, 1536], P(('dp', 'ei', 'eo'))
- output 2: bfloat16 [512, 1536], P(('dp', 'ei', 'eo'))
- output 3: float32 [512, 8], P(('dp', 'ei', 'eo'))
- output 4: float32 [40, 1536, 512], P(('dp', 'ei', 'eo'))
- output 5: float32 [40, 1536, 512], P(('dp', 'ei', 'eo'))
- output 6: float32 [40, 512, 1536], P(('dp', 'ei', 'eo'))
- output 7: bfloat16 [8, 64, 1536], P(('dp', 'ei', 'eo'))
All inputs are finite; a program needn't handle non-finite values.
Results may differ from the reference program's by a relative error of at most 0.013551.
Values are sent between devices in bfloat16 or wider.
A program may use at most 1 GiB of HBM per device.

```python
import jax
import jax.numpy as jnp
import numpy as np
from jax import lax

TOKENS_DEV = 64
SEQ_LEN = 64
NUM_SRC = 8
D_MODEL = 1536
D_FF = 512
EXPERTS = 40
TOP_K = 8
HEADS = 24
KV_HEADS = 8
HEAD_DIM = 64
CAP_MULT = 4

NUM_TOK = NUM_SRC * TOKENS_DEV
NUM_SEQ = NUM_TOK // SEQ_LEN
CAP_SRC = min(TOKENS_DEV, CAP_MULT * TOKENS_DEV * TOP_K // EXPERTS)
CAP_ALL = NUM_SRC * CAP_SRC


def routing_table(key):
    per_dev = TOKENS_DEV * TOP_K
    hot_num = max(1, per_dev // (2 * CAP_SRC))
    rest_asg = per_dev - hot_num * CAP_SRC
    cold_num = EXPERTS - hot_num
    base_cnt = rest_asg // cold_num
    extra_num = rest_asg - base_cnt * cold_num
    counts = np.array([CAP_SRC] * hot_num + [base_cnt + 1] * extra_num + [base_cnt] * (cold_num - extra_num))
    expert_seq = jnp.asarray(np.repeat(np.arange(EXPERTS), counts), dtype=jnp.int32)

    def one_device(dev_key):
        key_perm, key_rows = jax.random.split(dev_key)
        relabel = jax.random.permutation(key_perm, EXPERTS).astype(jnp.int32)
        table = relabel[expert_seq].reshape(TOP_K, TOKENS_DEV).T
        return table[jax.random.permutation(key_rows, TOKENS_DEV)]

    return jax.vmap(one_device)(jax.random.split(key, NUM_SRC)).reshape(NUM_TOK, TOP_K)


def setup_inputs(seed: int = 0, part: int = 0) -> dict:
    shared_key, part_root = jax.random.split(jax.random.key(seed))
    part_keys = jax.random.split(jax.random.fold_in(part_root, part), 5)
    w_keys = jax.random.split(shared_key, 7)

    def normal_bf16(key, shape, scale):
        return (jax.random.normal(key, shape, jnp.float32) * scale).astype(jnp.bfloat16)

    return {
        'x_tokens': normal_bf16(part_keys[0], (NUM_TOK, D_MODEL), 1.0),
        'expert_idx': routing_table(part_keys[1]),
        'gate_vals': jax.random.uniform(part_keys[2], (NUM_TOK, TOP_K), jnp.float32, 0.05, 0.3),
        'dy_tokens': normal_bf16(part_keys[3], (NUM_TOK, D_MODEL), 1.0),
        'w_gate': normal_bf16(w_keys[0], (EXPERTS, D_MODEL, D_FF), D_MODEL ** -0.5),
        'w_up': normal_bf16(w_keys[1], (EXPERTS, D_MODEL, D_FF), D_MODEL ** -0.5),
        'w_down': normal_bf16(w_keys[2], (EXPERTS, D_FF, D_MODEL), D_FF ** -0.5),
        'x_attn': normal_bf16(part_keys[4], (NUM_SEQ, SEQ_LEN, D_MODEL), 1.0),
        'w_query': normal_bf16(w_keys[3], (D_MODEL, HEADS, HEAD_DIM), D_MODEL ** -0.5),
        'w_key': normal_bf16(w_keys[4], (D_MODEL, KV_HEADS, HEAD_DIM), D_MODEL ** -0.5),
        'w_value': normal_bf16(w_keys[5], (D_MODEL, KV_HEADS, HEAD_DIM), D_MODEL ** -0.5),
        'w_out': normal_bf16(w_keys[6], (HEADS, HEAD_DIM, D_MODEL), (HEADS * HEAD_DIM) ** -0.5),
    }


def moe_part(x_tokens, expert_idx, gate_vals, dy_tokens, w_gate, w_up, w_down):
    num_asg = NUM_TOK * TOP_K
    flat_exp = expert_idx.reshape(num_asg)
    onehot = (flat_exp[:, None] == jnp.arange(EXPERTS, dtype=jnp.int32)[None, :]).astype(jnp.int32)
    ranks = jnp.sum((jnp.cumsum(onehot, axis=0) - 1) * onehot, axis=1)
    slot_owner = jnp.full((EXPERTS * CAP_ALL,), num_asg, jnp.int32)
    slot_owner = slot_owner.at[flat_exp * CAP_ALL + ranks].set(jnp.arange(num_asg, dtype=jnp.int32)).reshape(EXPERTS, CAP_ALL)
    slot_tok = jnp.where(slot_owner < num_asg, slot_owner // TOP_K, NUM_TOK)
    zero_row = jnp.zeros((1, D_MODEL), x_tokens.dtype)
    x_pad = jnp.concatenate([x_tokens, zero_row])
    dy_pad = jnp.concatenate([dy_tokens, zero_row])
    gate_pad = jnp.concatenate([gate_vals.reshape(num_asg), jnp.zeros((1,), gate_vals.dtype)])

    def expert_step(carry, per_exp):
        y_acc, dx_acc, dg_acc = carry
        owner_e, tok_e, w_one, w_three, w_two = per_exp
        x_rows = x_pad[tok_e]
        dy_rows = dy_pad[tok_e].astype(jnp.float32)
        gate_e = gate_pad[owner_e][:, None]
        pre_gate = jnp.dot(x_rows, w_one, preferred_element_type=jnp.float32)
        pre_up = jnp.dot(x_rows, w_three, preferred_element_type=jnp.float32)
        sigmoid_g = jax.nn.sigmoid(pre_gate)
        act_gate = pre_gate * sigmoid_g
        hidden = (act_gate * pre_up).astype(jnp.bfloat16)
        out_wide = jnp.dot(hidden, w_two, preferred_element_type=jnp.float32).astype(jnp.bfloat16).astype(jnp.float32)
        y_acc = y_acc.at[tok_e].add(gate_e * out_wide, mode='drop')
        dg_acc = dg_acc.at[owner_e].add(jnp.sum(dy_rows * out_wide, axis=1), mode='drop')
        d_out = (gate_e * dy_rows).astype(jnp.bfloat16)
        d_hidden = jnp.dot(d_out, w_two.T, preferred_element_type=jnp.float32).astype(jnp.bfloat16).astype(jnp.float32)
        d_pre_gate = (d_hidden * pre_up * sigmoid_g * (1.0 + pre_gate * (1.0 - sigmoid_g))).astype(jnp.bfloat16)
        d_pre_up = (d_hidden * act_gate).astype(jnp.bfloat16)
        d_rows = (jnp.dot(d_pre_gate, w_one.T, preferred_element_type=jnp.float32) + jnp.dot(d_pre_up, w_three.T, preferred_element_type=jnp.float32)).astype(jnp.bfloat16)
        dx_acc = dx_acc.at[tok_e].add(d_rows.astype(jnp.float32), mode='drop')
        grads = (jnp.dot(x_rows.T, d_pre_gate, preferred_element_type=jnp.float32), jnp.dot(x_rows.T, d_pre_up, preferred_element_type=jnp.float32), jnp.dot(hidden.T, d_out, preferred_element_type=jnp.float32))
        return (y_acc, dx_acc, dg_acc), grads

    init = (jnp.zeros((NUM_TOK, D_MODEL), jnp.float32), jnp.zeros((NUM_TOK, D_MODEL), jnp.float32), jnp.zeros((num_asg,), jnp.float32))
    (y_acc, dx_acc, dg_acc), (dw_gate, dw_up, dw_down) = lax.scan(expert_step, init, (slot_owner, slot_tok, w_gate, w_up, w_down))
    return y_acc.astype(jnp.bfloat16), dx_acc.astype(jnp.bfloat16), dg_acc.reshape(NUM_TOK, TOP_K), dw_gate, dw_up, dw_down


def attention_part(x_attn, w_query, w_key, w_value, w_out):
    groups = HEADS // KV_HEADS
    causal = jnp.arange(SEQ_LEN)[:, None] >= jnp.arange(SEQ_LEN)[None, :]
    wq_f32 = w_query.astype(jnp.float32)
    wk_f32 = w_key.astype(jnp.float32)
    wv_f32 = w_value.astype(jnp.float32)
    wo_f32 = w_out.astype(jnp.float32)

    def one_seq(seq_x):
        x_f32 = seq_x.astype(jnp.float32)
        query = jnp.einsum('ld,dhe->lhe', x_f32, wq_f32).astype(jnp.bfloat16).reshape(SEQ_LEN, KV_HEADS, groups, HEAD_DIM)
        keys_h = jnp.einsum('ld,dke->lke', x_f32, wk_f32).astype(jnp.bfloat16)
        vals_h = jnp.einsum('ld,dke->lke', x_f32, wv_f32).astype(jnp.bfloat16)
        scores = jnp.einsum('qkge,ske->kgqs', query.astype(jnp.float32), keys_h.astype(jnp.float32)) * HEAD_DIM ** -0.5
        scores = jnp.where(causal, scores, -1e30)
        probs = jax.nn.softmax(scores, axis=-1).astype(jnp.bfloat16)
        context = jnp.einsum('kgqs,ske->qkge', probs.astype(jnp.float32), vals_h.astype(jnp.float32)).astype(jnp.bfloat16)
        context = context.reshape(SEQ_LEN, HEADS, HEAD_DIM)
        return jnp.einsum('qhe,hed->qd', context.astype(jnp.float32), wo_f32).astype(jnp.bfloat16)

    return lax.map(one_seq, x_attn)


def reference(x_tokens, expert_idx, gate_vals, dy_tokens, w_gate, w_up, w_down, x_attn, w_query, w_key, w_value, w_out):
    y_tokens, dx_tokens, d_gates, dw_gate, dw_up, dw_down = moe_part(x_tokens, expert_idx, gate_vals, dy_tokens, w_gate, w_up, w_down)
    attn_out = attention_part(x_attn, w_query, w_key, w_value, w_out)
    return (y_tokens, dx_tokens, d_gates, dw_gate, dw_up, dw_down, attn_out)
```

```python
import jax
import jax.numpy as jnp
from jax import lax
from jax.sharding import PartitionSpec as P

GROUP_AXES = ('ei', 'eo')
TOKEN_AXES = ('dp', 'ei', 'eo')
F32 = jnp.float32
BF16 = jnp.bfloat16


def attention_partial(x_all, w_query, w_key, w_value, w_out):
    num_seq, seq_len = x_all.shape[0], x_all.shape[1]
    heads, head_dim = w_query.shape[1], w_query.shape[2]
    kv_heads = w_key.shape[1]
    query = jnp.einsum('nld,dhe->nlhe', x_all, w_query, preferred_element_type=F32).astype(BF16)
    query = query.reshape(num_seq, seq_len, kv_heads, heads // kv_heads, head_dim)
    keys_h = jnp.einsum('nld,dke->nlke', x_all, w_key, preferred_element_type=F32).astype(BF16)
    vals_h = jnp.einsum('nld,dke->nlke', x_all, w_value, preferred_element_type=F32).astype(BF16)
    scores = jnp.einsum('nqkge,nske->nkgqs', query, keys_h, preferred_element_type=F32) * head_dim ** -0.5
    causal = jnp.arange(seq_len)[:, None] >= jnp.arange(seq_len)[None, :]
    probs = jax.nn.softmax(jnp.where(causal, scores, -1e30), axis=-1).astype(BF16)
    context = jnp.einsum('nkgqs,nske->nqkge', probs, vals_h, preferred_element_type=F32).astype(BF16)
    context = context.reshape(num_seq, seq_len, heads, head_dim)
    return jnp.einsum('nqhe,hed->nqd', context, w_out, preferred_element_type=F32)


def solution(mesh):
    def gather(x):
        return lax.all_gather(x, GROUP_AXES, axis=0, tiled=True)

    def scatter(x):
        return lax.psum_scatter(x, GROUP_AXES, scatter_dimension=0, tiled=True)

    def local_step(x_tokens, expert_idx, gate_vals, dy_tokens, w_gate, w_up, w_down, x_attn, w_query, w_key, w_value, w_out):
        exp_loc = w_gate.shape[0]
        first = (lax.axis_index('ei') * mesh.shape['eo'] + lax.axis_index('eo')) * exp_loc
        x = gather(x_tokens)
        dy = gather(dy_tokens)
        idx = gather(expert_idx)
        gates = gather(gate_vals)
        y_part = jnp.zeros(x.shape, F32)
        dx_part = jnp.zeros(x.shape, F32)
        dg_part = jnp.zeros(gates.shape, F32)
        dws = []
        dyf = dy.astype(F32)
        for e in range(exp_loc):
            hit = idx == first + e
            mask = jnp.any(hit, axis=1)[:, None]
            gate = jnp.sum(jnp.where(hit, gates, 0.0), axis=1)[:, None]
            a = jnp.where(mask, jnp.dot(x, w_gate[e], preferred_element_type=F32), 0.0)
            b = jnp.where(mask, jnp.dot(x, w_up[e], preferred_element_type=F32), 0.0)
            sig = jax.nn.sigmoid(a)
            act = a * sig
            h = (act * b).astype(BF16)
            o = jnp.dot(h, w_down[e], preferred_element_type=F32).astype(BF16).astype(F32)
            y_part += gate * o
            dg_part += jnp.where(hit, jnp.sum(dyf * o, axis=1)[:, None], 0.0)
            d_o = (gate * dyf).astype(BF16)
            dh = jnp.dot(d_o, w_down[e].T, preferred_element_type=F32).astype(BF16).astype(F32)
            da = (dh * b * sig * (1.0 + a * (1.0 - sig))).astype(BF16)
            db = (dh * act).astype(BF16)
            dxe = jnp.dot(da, w_gate[e].T, preferred_element_type=F32) + jnp.dot(db, w_up[e].T, preferred_element_type=F32)
            dx_part += dxe.astype(BF16).astype(F32)
            dws.append((jnp.dot(x.T, da, preferred_element_type=F32), jnp.dot(x.T, db, preferred_element_type=F32), jnp.dot(h.T, d_o, preferred_element_type=F32)))
        dw_gate, dw_up, dw_down = (jnp.stack(ws) for ws in zip(*dws))
        y_tokens = scatter(y_part).astype(BF16)
        dx_tokens = scatter(dx_part).astype(BF16)
        d_gates = scatter(dg_part)
        attn_part = attention_partial(gather(x_attn), w_query, w_key, w_value, w_out)
        attn_out = scatter(attn_part).astype(BF16)
        return y_tokens, dx_tokens, d_gates, dw_gate, dw_up, dw_down, attn_out

    spec_rows = P(TOKEN_AXES, None)
    spec_seqs = P(TOKEN_AXES, None, None)
    spec_experts = P(GROUP_AXES, None, None)
    spec_heads = P(None, GROUP_AXES, None)
    return jax.shard_map(local_step, mesh=mesh,
                         in_specs=(spec_rows, spec_rows, spec_rows, spec_rows, spec_experts, spec_experts, spec_experts, spec_seqs, spec_heads, spec_heads, spec_heads, spec_experts),
                         out_specs=(spec_rows, spec_rows, spec_rows, spec_seqs, spec_seqs, spec_seqs, spec_seqs),
                         check_vma=False)
```

```python
import jax
import jax.numpy as jnp
from jax import lax
from jax.experimental import pallas as pl
from jax.experimental.pallas import tpu as pltpu
from jax.sharding import PartitionSpec as P

GROUP_AXES = ('ei', 'eo')
TOKEN_AXES = ('dp', 'ei', 'eo')
F32 = jnp.float32
BF16 = jnp.bfloat16
MESH_ID = pl.DeviceIdType.MESH
HALVES = 2
NUM_DEV = 8
LANES = 128


def dot_nn(lhs, rhs):
    return jnp.dot(lhs, rhs, preferred_element_type=F32)


def dot_nt(lhs, rhs):
    return lax.dot_general(lhs, rhs, (((1,), (1,)), ((), ())), preferred_element_type=F32)


def dot_tn(lhs, rhs):
    return lax.dot_general(lhs, rhs, (((0,), (0,)), ((), ())), preferred_element_type=F32)


class Place:
    def __init__(self):
        i = lax.axis_index('ei')
        o = lax.axis_index('eo')
        x = lax.div(o, 2)
        c = lax.rem(o, 2)
        self.core = c
        self.chip = i * 2 + x
        self.dev = {}
        self.block = {}
        for flip_y in (0, 1):
            for flip_x in (0, 1):
                for flip_c in (0, 1):
                    yy = 1 - i if flip_y else i
                    xx = 1 - x if flip_x else x
                    cc = 1 - c if flip_c else c
                    name = ('y' if flip_y else '') + ('x' if flip_x else '') + ('c' if flip_c else '')
                    self.dev[name] = (0, yy, xx * 2 + cc)
                    self.block[name] = cc * 4 + yy * 2 + xx
        self.chips = {'': self.chip, 'x': i * 2 + 1 - x, 'y': (1 - i) * 2 + x, 'yx': (1 - i) * 2 + 1 - x}


class Link:
    def __init__(self, pool, src, dst, land, device):
        send, recv = pool.take()
        self.out = pltpu.make_async_remote_copy(src_ref=src, dst_ref=dst, send_sem=send, recv_sem=recv, device_id=device, device_id_type=MESH_ID)
        self.inn = pltpu.make_async_remote_copy(src_ref=land, dst_ref=land, send_sem=send, recv_sem=recv, device_id=device, device_id_type=MESH_ID)

    def start(self):
        self.out.start()

    def arrive(self):
        self.inn.wait_recv()

    def sent(self):
        self.out.wait_send()


class Pool:
    def __init__(self, sends, recvs):
        self.sends, self.recvs, self.used = sends, recvs, 0

    def take(self):
        k = self.used
        self.used += 1
        return self.sends.at[k], self.recvs.at[k]


class Gather:
    def __init__(self, pool, place, buf, rows):
        def at(name, lo=0, n=rows):
            return buf.at[pl.ds(pl.multiple_of(place.block[name] * rows + lo, 8), n), :]

        half = rows // 2
        own = at('')
        dev = place.dev
        self.to_x = Link(pool, own, own, at('x'), dev['x'])
        self.to_y = Link(pool, own, own, at('y'), dev['y'])
        self.to_c = Link(pool, own, own, at('c'), dev['c'])
        self.relay_x = Link(pool, at('y', 0, half), at('y', 0, half), at('yx', 0, half), dev['x'])
        self.relay_y = Link(pool, at('x', half, half), at('x', half, half), at('yx', half, half), dev['y'])
        self.core_x = Link(pool, at('x'), at('x'), at('xc'), dev['c'])
        self.core_y = Link(pool, at('y'), at('y'), at('yc'), dev['c'])
        self.core_d = Link(pool, at('yx'), at('yx'), at('yxc'), dev['c'])
        self.links = (self.to_x, self.to_y, self.to_c, self.relay_x, self.relay_y, self.core_x, self.core_y, self.core_d)

    def begin(self):
        self.to_x.start()
        self.to_y.start()
        self.to_c.start()

    def relay(self):
        self.to_y.arrive()
        self.relay_x.start()
        self.to_x.arrive()
        self.relay_y.start()
        self.core_y.start()
        self.core_x.start()

    def last(self):
        self.relay_x.arrive()
        self.relay_y.arrive()
        self.core_d.start()

    def finish(self):
        self.to_c.arrive()
        self.core_x.arrive()
        self.core_y.arrive()
        self.core_d.arrive()

    def drain(self):
        for link in self.links:
            link.sent()


class Scatter:
    def __init__(self, pool, place, part, from_core, from_x, from_y, last_x, last_y, rows):
        half = rows // 2
        self.half, self.part, self.rows, self.place = half, part, rows, place
        self.from_core, self.from_x, self.from_y, self.last_x, self.last_y = from_core, from_x, from_y, last_x, last_y
        four = 4 * rows
        self.mine = pl.multiple_of(place.core * four, 8)
        other = part.at[pl.ds(pl.multiple_of((1 - place.core) * four, 8), four), :]
        dev = place.dev
        self.core = Link(pool, other, from_core, from_core, dev['c'])
        self.x0 = Link(pool, self.at('x', 0), from_x.at[0], from_x.at[0], dev['x'])
        self.x1 = Link(pool, self.at('yx', 0), from_x.at[1], from_x.at[1], dev['x'])
        self.y0 = Link(pool, self.at('y', half), from_y.at[0], from_y.at[0], dev['y'])
        self.y1 = Link(pool, self.at('yx', half), from_y.at[1], from_y.at[1], dev['y'])
        self.end_y = Link(pool, self.at('y', 0), last_y, last_y, dev['y'])
        self.end_x = Link(pool, self.at('x', half), last_x, last_x, dev['x'])
        self.links = (self.core, self.x0, self.x1, self.y0, self.y1, self.end_y, self.end_x)

    def at(self, name, lo):
        return self.part.at[pl.ds(pl.multiple_of(self.place.block[name] * self.rows + lo, 8), self.half), :]

    def begin(self):
        self.core.start()

    def middle(self):
        self.core.arrive()
        mine = pl.ds(self.mine, 4 * self.rows)
        self.part[mine, :] = self.part[mine, :] + self.from_core[...]
        self.x1.start()
        self.y1.start()
        self.x0.start()
        self.y0.start()

    def late(self):
        self.x1.arrive()
        here = self.at('y', 0)
        here[...] = here[...] + self.from_x[1]
        self.end_y.start()
        self.y1.arrive()
        here = self.at('x', self.half)
        here[...] = here[...] + self.from_y[1]
        self.end_x.start()

    def finish(self, out):
        half = self.half
        self.x0.arrive()
        self.y0.arrive()
        self.end_y.arrive()
        self.end_x.arrive()
        out[0:half, :] = (self.at('', 0)[...] + self.from_x[0] + self.last_y[...]).astype(BF16)
        out[half:2 * half, :] = (self.at('', half)[...] + self.from_y[0] + self.last_x[...]).astype(BF16)

    def drain(self):
        for link in self.links:
            link.sent()


def scatter_shapes(rows, width):
    half = rows // 2
    return [pltpu.VMEM((4 * rows, width), F32), pltpu.VMEM((2, half, width), F32), pltpu.VMEM((2, half, width), F32),
            pltpu.VMEM((half, width), F32), pltpu.VMEM((half, width), F32)]


NUM_LINKS = 7 + 14 + 8 * 5 + 7 * 5


def attention(xa, wqkv, wo, ctx, part, dims):
    seq, kv_dim, heads, head_dim = dims
    q_dim = heads * head_dim
    rows = xa.shape[0]
    pair = 2 * seq
    row = lax.broadcasted_iota(jnp.int32, (pair, pair), 0)
    col = lax.broadcasted_iota(jnp.int32, (pair, pair), 1)
    causal = (row >= col) & ((row >= seq) == (col >= seq))
    for p in range(rows // pair):
        qkv = dot_nn(xa[p * pair:(p + 1) * pair, :], wqkv[...]).astype(BF16)
        keys = qkv[:, q_dim:q_dim + kv_dim]
        vals = qkv[:, q_dim + kv_dim:q_dim + 2 * kv_dim]
        outs = []
        for h in range(heads):
            scores = dot_nt(qkv[:, h * head_dim:(h + 1) * head_dim], keys) * head_dim ** -0.5
            scores = jnp.where(causal, scores, -1e30)
            top = jnp.max(scores, axis=1, keepdims=True)
            ex = jnp.exp(scores - top)
            probs = (ex / jnp.sum(ex, axis=1, keepdims=True)).astype(BF16)
            outs.append(dot_nn(probs, vals).astype(BF16))
        ctx[p * pair:(p + 1) * pair, :] = jnp.concatenate(outs, axis=1)
    for p in range(rows // pair):
        part[p * pair:(p + 1) * pair, :] = dot_nn(ctx[p * pair:(p + 1) * pair, :], wo[...])


def make_layer_kernel(tok, d_model, d_ff, exp_loc, attn_dims):
    r = tok // HALVES
    m = r * NUM_DEV
    tile = 512
    units = HALVES * exp_loc

    def kernel(x_in, dy_in, xa_in, gt_in, wg_in, wu_in, wd_in, wqkv, wo,
               y_out, dx_out, attn_out, dg_out, x_all, dy_all, da_all, db_all, h_all, gates_out,
               xb, dyb, xab, gtb, gcol, wg, wu, wd, y_part, dx_part, at_part, ctx, s1, s2, d_o, dgc, dgt, stage,
               ry0, ry1, ry2, ry3, ry4, rd0, rd1, rd2, rd3, rd4, ra0, ra1, ra2, ra3, ra4,
               send_sems, recv_sems, w_sems, in_sems, out_sems, stage_sems):
        place = Place()
        pool = Pool(send_sems, recv_sems)
        dev, block = place.dev, place.block
        me = block['']

        def own_rows(buf, rows):
            return buf.at[pl.ds(pl.multiple_of(me * rows, 8), rows), :]

        loads = []
        for h in range(HALVES):
            loads.append(pltpu.make_async_copy(x_in.at[h * r:(h + 1) * r, :], own_rows(xb.at[h], r), in_sems.at[h]))
            loads.append(pltpu.make_async_copy(dy_in.at[h * r:(h + 1) * r, :], own_rows(dyb.at[h], r), in_sems.at[2 + h]))
        loads.append(pltpu.make_async_copy(xa_in, own_rows(xab, tok), in_sems.at[4]))
        for load in loads:
            load.start()
        weights = []
        for e in range(exp_loc):
            weights.append([pltpu.make_async_copy(src.at[e], dst.at[e], w_sems.at[e, k]) for k, (src, dst) in enumerate(((wg_in, wg), (wu_in, wu), (wd_in, wd)))])
        for ws in weights:
            for w in ws:
                w.start()

        barrier = pltpu.get_barrier_semaphore()
        peers = [name for name in dev if name]
        for name in peers:
            pl.semaphore_signal(barrier, inc=1, device_id=dev[name], device_id_type=MESH_ID)
        pl.semaphore_wait(barrier, len(peers))

        routes = [Link(pool, gt_in.at[block[name]], gtb.at[me], gtb.at[block[name]], dev[name]) for name in peers]
        gx = [Gather(pool, place, xb.at[h], r) for h in range(HALVES)]
        gdy = [Gather(pool, place, dyb.at[h], r) for h in range(HALVES)]
        gxa = Gather(pool, place, xab, tok)
        sy = [Scatter(pool, place, y_part.at[h], ry0.at[h], ry1.at[h], ry2.at[h], ry3.at[h], ry4.at[h], r) for h in range(HALVES)]
        sdx = [Scatter(pool, place, dx_part.at[h], rd0.at[h], rd1.at[h], rd2.at[h], rd3.at[h], rd4.at[h], r) for h in range(HALVES)]
        sat = Scatter(pool, place, at_part, ra0, ra1, ra2, ra3, ra4, tok)
        dg_links = [[Link(pool, dgt.at[h, 1 - place.core if 'c' in name else place.core], dg_out.at[me, h], dg_out.at[block[name], h], dev[name]) for name in peers] for h in range(HALVES)]

        for link in routes:
            link.start()
        gtb[me] = gt_in[me]
        for load in loads:
            load.wait()
        gx[0].begin()
        gdy[0].begin()
        gx[1].begin()
        gdy[1].begin()
        gxa.begin()
        y_part[...] = jnp.zeros_like(y_part)
        dx_part[...] = jnp.zeros_like(dx_part)
        dgc[...] = jnp.zeros_like(dgc)
        gcol[...] = jnp.zeros_like(gcol)
        for link in routes:
            link.arrive()
        wide = jnp.concatenate([gtb[...].reshape(NUM_DEV * 8, LANES), jnp.zeros((LANES - NUM_DEV * 8, LANES), F32)], axis=0).T
        for h in range(HALVES):
            for b in range(NUM_DEV):
                gcol[h, b * r:(b + 1) * r, 0:8] = wide[h * r:(h + 1) * r, b * 8:(b + 1) * 8]
        for g in (gx[0], gdy[0], gx[1], gdy[1], gxa):
            g.relay()
        for g in (gx[0], gdy[0], gx[1], gdy[1], gxa):
            g.last()
        for g in (gx[0], gdy[0], gx[1], gdy[1], gxa):
            g.finish()
        attention(xab, wqkv, wo, ctx, at_part, attn_dims)
        sat.begin()

        def staged(u, k):
            h, e = lax.div(u, exp_loc), lax.rem(u, exp_loc)
            slot = lax.rem(u, 2)
            dst = (da_all, db_all, h_all)[k].at[e, pl.ds(pl.multiple_of(h * m, 8), m), :]
            return pltpu.make_async_copy(stage.at[slot, k], dst, stage_sems.at[slot, k])

        lane = lax.broadcasted_iota(jnp.int32, (m, LANES), 1)

        def unit(u, _):
            h, e = lax.div(u, exp_loc), lax.rem(u, exp_loc)
            slot = lax.rem(u, 2)

            @pl.when(u < exp_loc)
            def _():
                for k, (src, dst) in enumerate(((wg_in, wg), (wu_in, wu), (wd_in, wd))):
                    pltpu.make_async_copy(src.at[e], dst.at[e], w_sems.at[e, k]).wait()

            @pl.when(u >= 2)
            def _():
                for k in range(3):
                    staged(u - 2, k).wait()

            @pl.when(u == 1)
            def _():
                sat.middle()

            @pl.when(u == 5)
            def _():
                sy[0].begin()
                sdx[0].begin()
                sat.late()

            @pl.when(u == 6)
            def _():
                sy[0].middle()
                sdx[0].middle()

            @pl.when(u == 8)
            def _():
                sy[0].late()
                sdx[0].late()

            gate = jnp.sum(jnp.where(lane == e, gcol[h], 0.0), axis=1, keepdims=True)
            mask = gate > 0.0
            a = jnp.where(mask, dot_nn(xb[h], wg[e]), 0.0)
            b = jnp.where(mask, dot_nn(xb[h], wu[e]), 0.0)
            sig = jax.nn.sigmoid(a)
            act = a * sig
            stage[slot, 2] = (act * b).astype(BF16)
            s1[...] = b * sig * (1.0 + a * (1.0 - sig))
            s2[...] = act
            dots = jnp.zeros((m, LANES), F32)
            for n in range(d_model // tile):
                cols = pl.ds(n * tile, tile)
                o = dot_nn(stage[slot, 2], wd[e, :, cols]).astype(BF16).astype(F32)
                dy = dyb[h, :, cols].astype(F32)
                y_part[h, :, cols] += gate * o
                prod = dy * o
                for k in range(tile // LANES):
                    dots += prod[:, k * LANES:(k + 1) * LANES]
                d_o[:, cols] = (gate * dy).astype(BF16)
            dgc[h] = jnp.where(lane == e, jnp.sum(dots, axis=1, keepdims=True), dgc[h])
            dh = dot_nt(d_o[...], wd[e]).astype(BF16).astype(F32)
            stage[slot, 0] = (dh * s1[...]).astype(BF16)
            stage[slot, 1] = (dh * s2[...]).astype(BF16)
            for k in range(3):
                staged(u, k).start()
            for n in range(d_model // tile):
                cols = pl.ds(n * tile, tile)
                dxe = dot_nt(stage[slot, 0], wg[e, cols, :]) + dot_nt(stage[slot, 1], wu[e, cols, :])
                dx_part[h, :, cols] += dxe.astype(BF16).astype(F32)
            return 0

        lax.fori_loop(0, units, unit, 0)

        sy[1].begin()
        sdx[1].begin()
        for h in range(HALVES):
            turned = dgc[h].T
            for c in range(2):
                dgt[h, c] = turned[0:8, c * LANES:(c + 1) * LANES]
        saves = [pltpu.make_async_copy(xb, x_all, out_sems.at[0]), pltpu.make_async_copy(dyb, dy_all, out_sems.at[1]), pltpu.make_async_copy(gcol, gates_out, out_sems.at[2])]
        for save in saves:
            save.start()
        for h in range(HALVES):
            for link in dg_links[h]:
                link.start()
            dg_out[me, h] = dgt[h, place.core]
        sy[1].middle()
        sdx[1].middle()
        sat.finish(attn_out)
        for s, out in ((sy[0], y_out), (sdx[0], dx_out)):
            s.finish(out.at[0:r, :])
        sy[1].late()
        sdx[1].late()
        for h in range(HALVES):
            for link in dg_links[h]:
                link.arrive()
        for s, out in ((sy[1], y_out), (sdx[1], dx_out)):
            s.finish(out.at[r:2 * r, :])
        for u in (units - 2, units - 1):
            for k in range(3):
                staged(jnp.int32(u), k).wait()
        for save in saves:
            save.wait()
        for item in gx + gdy + [gxa] + sy + sdx + [sat]:
            item.drain()
        for link in routes + dg_links[0] + dg_links[1]:
            link.sent()
        assert pool.used == NUM_LINKS

    return kernel, r, m


def weight_grads(x_ref, dy_ref, gates_ref, da_ref, db_ref, h_ref, dwg_ref, dwu_ref, dwd_ref, d_o):
    e = pl.program_id(0)
    n = pl.program_id(1)

    @pl.when(n == 0)
    def _():
        lane = lax.broadcasted_iota(jnp.int32, gates_ref.shape, 1)
        gate = jnp.sum(jnp.where(lane == e, gates_ref[...], 0.0), axis=1, keepdims=True)
        d_o[...] = (gate * dy_ref[...].astype(F32)).astype(BF16)

    width = dwg_ref.shape[0]
    cols = pl.ds(pl.multiple_of(n * width, LANES), width)
    xt = x_ref[:, cols]
    dwg_ref[...] = dot_tn(xt, da_ref[...])
    dwu_ref[...] = dot_tn(xt, db_ref[...])
    dwd_ref[...] = dot_tn(h_ref[...], d_o[:, cols])


def solution(mesh):
    num_dev = mesh.shape['ei'] * mesh.shape['eo']
    assert num_dev == NUM_DEV

    def local_step(x_tokens, expert_idx, gate_vals, dy_tokens, w_gate, w_up, w_down, x_attn, w_query, w_key, w_value, w_out):
        tok, d_model = x_tokens.shape
        top_k = expert_idx.shape[1]
        exp_loc, _, d_ff = w_gate.shape
        seq = x_attn.shape[1]
        heads, head_dim = w_query.shape[1], w_query.shape[2]
        kv_dim = w_key.shape[1] * head_dim
        q_dim = heads * head_dim
        ids = jnp.arange(NUM_DEV * exp_loc, dtype=jnp.int32).reshape(NUM_DEV, exp_loc, 1, 1)
        table = jnp.sum(jnp.where(expert_idx.T[None, None] == ids, gate_vals.T[None, None], 0.0), axis=2)
        table = jnp.pad(table, ((0, 0), (0, 8 - exp_loc), (0, LANES - tok)))
        gt = table.reshape(4, 2, 8, LANES).transpose(1, 0, 2, 3).reshape(NUM_DEV, 8, LANES)
        pad = -(q_dim + 2 * kv_dim) % LANES
        wqkv = jnp.concatenate([w_query.reshape(d_model, q_dim), w_key.reshape(d_model, kv_dim), w_value.reshape(d_model, kv_dim), jnp.zeros((d_model, pad), BF16)], axis=1)
        wo = w_out.reshape(q_dim, d_model)
        kernel, r, m = make_layer_kernel(tok, d_model, d_ff, exp_loc, (seq, kv_dim, heads, head_dim))
        any_spec = pl.BlockSpec(memory_space=pl.ANY)
        vmem_spec = pl.BlockSpec(memory_space=pltpu.VMEM)
        shape = jax.ShapeDtypeStruct
        total = tok * NUM_DEV

        def half_shapes():
            return [pltpu.VMEM((HALVES,) + s.shape, s.dtype) for s in scatter_shapes(r, d_model)]

        y, dx, attn, dgt, x_all, dy_all, da, db, hid, gates = pl.pallas_call(
            kernel,
            out_shape=(shape((tok, d_model), BF16), shape((tok, d_model), BF16), shape((tok, d_model), BF16), shape((NUM_DEV, HALVES, 8, LANES), F32),
                       shape((HALVES, m, d_model), BF16), shape((HALVES, m, d_model), BF16),
                       shape((exp_loc, total, d_ff), BF16), shape((exp_loc, total, d_ff), BF16), shape((exp_loc, total, d_ff), BF16), shape((HALVES, m, LANES), F32)),
            in_specs=[any_spec, any_spec, any_spec, vmem_spec, any_spec, any_spec, any_spec, vmem_spec, vmem_spec],
            out_specs=(vmem_spec,) * 4 + (any_spec,) * 6,
            scratch_shapes=[pltpu.VMEM((HALVES, m, d_model), BF16), pltpu.VMEM((HALVES, m, d_model), BF16), pltpu.VMEM((total, d_model), BF16),
                            pltpu.VMEM((NUM_DEV, 8, LANES), F32), pltpu.VMEM((HALVES, m, LANES), F32),
                            pltpu.VMEM((exp_loc, d_model, d_ff), BF16), pltpu.VMEM((exp_loc, d_model, d_ff), BF16), pltpu.VMEM((exp_loc, d_ff, d_model), BF16),
                            pltpu.VMEM((HALVES, m, d_model), F32), pltpu.VMEM((HALVES, m, d_model), F32), pltpu.VMEM((total, d_model), F32), pltpu.VMEM((total, q_dim), BF16),
                            pltpu.VMEM((m, d_ff), F32), pltpu.VMEM((m, d_ff), F32), pltpu.VMEM((m, d_model), BF16),
                            pltpu.VMEM((HALVES, m, LANES), F32), pltpu.VMEM((HALVES, 2, 8, LANES), F32), pltpu.VMEM((2, 3, m, d_ff), BF16)]
            + half_shapes() + half_shapes() + scatter_shapes(tok, d_model)
            + [pltpu.SemaphoreType.DMA((NUM_LINKS,)), pltpu.SemaphoreType.DMA((NUM_LINKS,)), pltpu.SemaphoreType.DMA((exp_loc, 3)),
               pltpu.SemaphoreType.DMA((5,)), pltpu.SemaphoreType.DMA((3,)), pltpu.SemaphoreType.DMA((2, 3))],
            compiler_params=pltpu.CompilerParams(collective_id=0, has_side_effects=True, vmem_limit_bytes=67000000),
            name='layer',
        )(x_tokens, dy_tokens, x_attn.reshape(tok, d_model), gt, w_gate, w_up, w_down, wqkv, wo)

        width = 512
        steps = d_model // width
        dw_gate, dw_up, dw_down = pl.pallas_call(
            weight_grads,
            grid=(exp_loc, steps),
            out_shape=(shape((exp_loc, d_model, d_ff), F32), shape((exp_loc, d_model, d_ff), F32), shape((exp_loc, d_ff, d_model), F32)),
            in_specs=[pl.BlockSpec((total, d_model), lambda e, n: (0, 0)), pl.BlockSpec((total, d_model), lambda e, n: (0, 0)), pl.BlockSpec((total, LANES), lambda e, n: (0, 0)),
                      pl.BlockSpec((None, total, d_ff), lambda e, n: (e, 0, 0)), pl.BlockSpec((None, total, d_ff), lambda e, n: (e, 0, 0)), pl.BlockSpec((None, total, d_ff), lambda e, n: (e, 0, 0))],
            out_specs=(pl.BlockSpec((None, width, d_ff), lambda e, n: (e, n, 0)), pl.BlockSpec((None, width, d_ff), lambda e, n: (e, n, 0)), pl.BlockSpec((None, d_ff, width), lambda e, n: (e, 0, n))),
            scratch_shapes=[pltpu.VMEM((total, d_model), BF16)],
            compiler_params=pltpu.CompilerParams(vmem_limit_bytes=60000000),
            cost_estimate=pl.CostEstimate(flops=3 * 2 * total * d_model * d_ff * exp_loc, bytes_accessed=3 * 4 * exp_loc * d_model * d_ff, transcendentals=0),
            name='weight_grads',
        )(x_all.reshape(total, d_model), dy_all.reshape(total, d_model), gates.reshape(total, LANES), da, db, hid)

        chip = lax.axis_index('ei') * 2 + lax.div(lax.axis_index('eo'), 2)
        mine = lax.dynamic_slice_in_dim(dgt, chip * r, r, axis=3)[:, :, :exp_loc]
        mine = mine.reshape(2, 4, HALVES, exp_loc, r).transpose(1, 0, 3, 2, 4).reshape(NUM_DEV * exp_loc, 1, tok)
        ids = jnp.arange(NUM_DEV * exp_loc, dtype=jnp.int32)[:, None, None]
        d_gates = jnp.sum(jnp.where(expert_idx.T[None] == ids, mine, 0.0), axis=0).T
        return y, dx, d_gates, dw_gate, dw_up, dw_down, attn.reshape(x_attn.shape)

    spec_rows = P(TOKEN_AXES, None)
    spec_seqs = P(TOKEN_AXES, None, None)
    spec_experts = P(GROUP_AXES, None, None)
    spec_heads = P(None, GROUP_AXES, None)
    return jax.shard_map(local_step, mesh=mesh,
                         in_specs=(spec_rows, spec_rows, spec_rows, spec_rows, spec_experts, spec_experts, spec_experts, spec_seqs, spec_heads, spec_heads, spec_heads, spec_experts),
                         out_specs=(spec_rows, spec_rows, spec_rows, spec_seqs, spec_seqs, spec_seqs, spec_seqs),
                         check_vma=False)
```

```python
import jax
import jax.numpy as jnp
from jax import lax
from jax.experimental import pallas as pl
from jax.experimental.pallas import tpu as pltpu
from jax.sharding import PartitionSpec as P

GROUP_AXES = ('ei', 'eo')
TOKEN_AXES = ('dp', 'ei', 'eo')
F32 = jnp.float32
BF16 = jnp.bfloat16
MESH_ID = pl.DeviceIdType.MESH
HALVES = 2
NUM_DEV = 8
LANES = 128


def dot_nn(lhs, rhs):
    return jnp.dot(lhs, rhs, preferred_element_type=F32)


def dot_nt(lhs, rhs):
    return lax.dot_general(lhs, rhs, (((1,), (1,)), ((), ())), preferred_element_type=F32)


def dot_tn(lhs, rhs):
    return lax.dot_general(lhs, rhs, (((0,), (0,)), ((), ())), preferred_element_type=F32)


class Place:
    def __init__(self):
        i = lax.axis_index('ei')
        o = lax.axis_index('eo')
        x = lax.div(o, 2)
        c = lax.rem(o, 2)
        self.core = c
        self.chip = i * 2 + x
        self.dev = {}
        self.block = {}
        for flip_y in (0, 1):
            for flip_x in (0, 1):
                for flip_c in (0, 1):
                    yy = 1 - i if flip_y else i
                    xx = 1 - x if flip_x else x
                    cc = 1 - c if flip_c else c
                    name = ('y' if flip_y else '') + ('x' if flip_x else '') + ('c' if flip_c else '')
                    self.dev[name] = (0, yy, xx * 2 + cc)
                    self.block[name] = cc * 4 + yy * 2 + xx
        self.chips = {'': self.chip, 'x': i * 2 + 1 - x, 'y': (1 - i) * 2 + x, 'yx': (1 - i) * 2 + 1 - x}


class Link:
    def __init__(self, pool, src, dst, land, device):
        send, recv = pool.take()
        self.out = pltpu.make_async_remote_copy(src_ref=src, dst_ref=dst, send_sem=send, recv_sem=recv, device_id=device, device_id_type=MESH_ID)
        self.inn = pltpu.make_async_remote_copy(src_ref=land, dst_ref=land, send_sem=send, recv_sem=recv, device_id=device, device_id_type=MESH_ID)

    def start(self):
        self.out.start()

    def arrive(self):
        self.inn.wait_recv()

    def sent(self):
        self.out.wait_send()


class Pool:
    def __init__(self, sends, recvs):
        self.sends, self.recvs, self.used = sends, recvs, 0

    def take(self):
        k = self.used
        self.used += 1
        return self.sends.at[k], self.recvs.at[k]


class Gather:
    def __init__(self, pool, place, buf, rows):
        def at(name, lo=0, n=rows):
            return buf.at[pl.ds(pl.multiple_of(place.block[name] * rows + lo, 8), n), :]

        half = rows // 2
        own = at('')
        dev = place.dev
        self.to_x = Link(pool, own, own, at('x'), dev['x'])
        self.to_y = Link(pool, own, own, at('y'), dev['y'])
        self.to_c = Link(pool, own, own, at('c'), dev['c'])
        self.relay_x = Link(pool, at('y', 0, half), at('y', 0, half), at('yx', 0, half), dev['x'])
        self.relay_y = Link(pool, at('x', half, half), at('x', half, half), at('yx', half, half), dev['y'])
        self.core_x = Link(pool, at('x'), at('x'), at('xc'), dev['c'])
        self.core_y = Link(pool, at('y'), at('y'), at('yc'), dev['c'])
        self.core_d = Link(pool, at('yx'), at('yx'), at('yxc'), dev['c'])
        self.links = (self.to_x, self.to_y, self.to_c, self.relay_x, self.relay_y, self.core_x, self.core_y, self.core_d)

    def begin(self):
        self.to_x.start()
        self.to_y.start()
        self.to_c.start()

    def relay(self):
        self.to_y.arrive()
        self.relay_x.start()
        self.to_x.arrive()
        self.relay_y.start()
        self.core_y.start()
        self.core_x.start()

    def last(self):
        self.relay_x.arrive()
        self.relay_y.arrive()
        self.core_d.start()

    def finish(self):
        self.to_c.arrive()
        self.core_x.arrive()
        self.core_y.arrive()
        self.core_d.arrive()

    def drain(self):
        for link in self.links:
            link.sent()


class Scatter:
    def __init__(self, pool, place, part, from_core, from_x, from_y, last_x, last_y, rows):
        half = rows // 2
        self.half, self.part, self.rows, self.place = half, part, rows, place
        self.from_core, self.from_x, self.from_y, self.last_x, self.last_y = from_core, from_x, from_y, last_x, last_y
        four = 4 * rows
        self.mine = pl.multiple_of(place.core * four, 8)
        other = part.at[pl.ds(pl.multiple_of((1 - place.core) * four, 8), four), :]
        dev = place.dev
        self.core = Link(pool, other, from_core, from_core, dev['c'])
        self.x0 = Link(pool, self.at('x', 0), from_x.at[0], from_x.at[0], dev['x'])
        self.x1 = Link(pool, self.at('yx', 0), from_x.at[1], from_x.at[1], dev['x'])
        self.y0 = Link(pool, self.at('y', half), from_y.at[0], from_y.at[0], dev['y'])
        self.y1 = Link(pool, self.at('yx', half), from_y.at[1], from_y.at[1], dev['y'])
        self.end_y = Link(pool, self.at('y', 0), last_y, last_y, dev['y'])
        self.end_x = Link(pool, self.at('x', half), last_x, last_x, dev['x'])
        self.links = (self.core, self.x0, self.x1, self.y0, self.y1, self.end_y, self.end_x)

    def at(self, name, lo):
        return self.part.at[pl.ds(pl.multiple_of(self.place.block[name] * self.rows + lo, 8), self.half), :]

    def begin(self):
        self.core.start()

    def middle(self):
        self.core.arrive()
        mine = pl.ds(self.mine, 4 * self.rows)
        self.part[mine, :] = self.part[mine, :] + self.from_core[...]
        self.x1.start()
        self.y1.start()
        self.x0.start()
        self.y0.start()

    def late(self):
        self.x1.arrive()
        here = self.at('y', 0)
        here[...] = here[...] + self.from_x[1]
        self.end_y.start()
        self.y1.arrive()
        here = self.at('x', self.half)
        here[...] = here[...] + self.from_y[1]
        self.end_x.start()

    def finish(self, out):
        half = self.half
        self.x0.arrive()
        self.y0.arrive()
        self.end_y.arrive()
        self.end_x.arrive()
        out[0:half, :] = (self.at('', 0)[...] + self.from_x[0] + self.last_y[...]).astype(BF16)
        out[half:2 * half, :] = (self.at('', half)[...] + self.from_y[0] + self.last_x[...]).astype(BF16)

    def drain(self):
        for link in self.links:
            link.sent()


def scatter_shapes(rows, width):
    half = rows // 2
    return [pltpu.VMEM((4 * rows, width), F32), pltpu.VMEM((2, half, width), F32), pltpu.VMEM((2, half, width), F32),
            pltpu.VMEM((half, width), F32), pltpu.VMEM((half, width), F32)]


NUM_LINKS = 7 + 14 + 8 * 5 + 7 * 5


def attention(xa, wqkv, wo, ctx, part, dims):
    seq, kv_dim, heads, head_dim = dims
    q_dim = heads * head_dim
    rows = xa.shape[0]
    pair = 2 * seq
    row = lax.broadcasted_iota(jnp.int32, (pair, pair), 0)
    col = lax.broadcasted_iota(jnp.int32, (pair, pair), 1)
    causal = (row >= col) & ((row >= seq) == (col >= seq))
    for p in range(rows // pair):
        qkv = dot_nn(xa[p * pair:(p + 1) * pair, :], wqkv[...]).astype(BF16)
        keys = qkv[:, q_dim:q_dim + kv_dim]
        vals = qkv[:, q_dim + kv_dim:q_dim + 2 * kv_dim]
        outs = []
        for h in range(heads):
            scores = dot_nt(qkv[:, h * head_dim:(h + 1) * head_dim], keys) * head_dim ** -0.5
            scores = jnp.where(causal, scores, -1e30)
            top = jnp.max(scores, axis=1, keepdims=True)
            ex = jnp.exp(scores - top)
            probs = (ex / jnp.sum(ex, axis=1, keepdims=True)).astype(BF16)
            outs.append(dot_nn(probs, vals).astype(BF16))
        ctx[p * pair:(p + 1) * pair, :] = jnp.concatenate(outs, axis=1)
    for p in range(rows // pair):
        part[p * pair:(p + 1) * pair, :] = dot_nn(ctx[p * pair:(p + 1) * pair, :], wo[...])


def make_layer_kernel(tok, d_model, d_ff, exp_loc, attn_dims):
    r = tok // HALVES
    m = r * NUM_DEV
    tile = 512
    units = HALVES * exp_loc

    def kernel(x_in, dy_in, xa_in, gt_in, wg_in, wu_in, wd_in, wqkv, wo,
               y_out, dx_out, attn_out, dg_out, xt_all, dy_all, da_all, db_all, ht_all, gates_out,
               xb, dyb, xab, gtb, gcol, wg, wu, wd, y_part, dx_part, at_part, ctx, s1, s2, d_o, dgc, dgt, stage, hid, stage_t, xt,
               ry0, ry1, ry2, ry3, ry4, rd0, rd1, rd2, rd3, rd4, ra0, ra1, ra2, ra3, ra4,
               send_sems, recv_sems, w_sems, in_sems, out_sems, stage_sems):
        place = Place()
        pool = Pool(send_sems, recv_sems)
        dev, block = place.dev, place.block
        me = block['']

        def own_rows(buf, rows):
            return buf.at[pl.ds(pl.multiple_of(me * rows, 8), rows), :]

        loads = []
        for h in range(HALVES):
            loads.append(pltpu.make_async_copy(x_in.at[h * r:(h + 1) * r, :], own_rows(xb.at[h], r), in_sems.at[h]))
            loads.append(pltpu.make_async_copy(dy_in.at[h * r:(h + 1) * r, :], own_rows(dyb.at[h], r), in_sems.at[2 + h]))
        loads.append(pltpu.make_async_copy(xa_in, own_rows(xab, tok), in_sems.at[4]))
        for load in loads:
            load.start()
        weights = []
        for e in range(exp_loc):
            weights.append([pltpu.make_async_copy(src.at[e], dst.at[e], w_sems.at[e, k]) for k, (src, dst) in enumerate(((wg_in, wg), (wu_in, wu), (wd_in, wd)))])
        for ws in weights:
            for w in ws:
                w.start()

        barrier = pltpu.get_barrier_semaphore()
        peers = [name for name in dev if name]
        for name in peers:
            pl.semaphore_signal(barrier, inc=1, device_id=dev[name], device_id_type=MESH_ID)
        pl.semaphore_wait(barrier, len(peers))

        routes = [Link(pool, gt_in.at[block[name]], gtb.at[me], gtb.at[block[name]], dev[name]) for name in peers]
        gx = [Gather(pool, place, xb.at[h], r) for h in range(HALVES)]
        gdy = [Gather(pool, place, dyb.at[h], r) for h in range(HALVES)]
        gxa = Gather(pool, place, xab, tok)
        sy = [Scatter(pool, place, y_part.at[h], ry0.at[h], ry1.at[h], ry2.at[h], ry3.at[h], ry4.at[h], r) for h in range(HALVES)]
        sdx = [Scatter(pool, place, dx_part.at[h], rd0.at[h], rd1.at[h], rd2.at[h], rd3.at[h], rd4.at[h], r) for h in range(HALVES)]
        sat = Scatter(pool, place, at_part, ra0, ra1, ra2, ra3, ra4, tok)
        dg_links = [[Link(pool, dgt.at[h, 1 - place.core if 'c' in name else place.core], dg_out.at[me, h], dg_out.at[block[name], h], dev[name]) for name in peers] for h in range(HALVES)]

        for link in routes:
            link.start()
        gtb[me] = gt_in[me]
        for load in loads:
            load.wait()
        gx[0].begin()
        gdy[0].begin()
        y_part[...] = jnp.zeros_like(y_part)
        dx_part[...] = jnp.zeros_like(dx_part)
        dgc[...] = jnp.zeros_like(dgc)
        gcol[...] = jnp.zeros_like(gcol)
        gx[0].relay()
        gx[1].begin()
        gdy[0].relay()
        gdy[1].begin()
        for link in routes:
            link.arrive()
        wide = jnp.concatenate([gtb[...].reshape(NUM_DEV * 8, LANES), jnp.zeros((LANES - NUM_DEV * 8, LANES), F32)], axis=0).T
        for h in range(HALVES):
            for b in range(NUM_DEV):
                gcol[h, b * r:(b + 1) * r, 0:8] = wide[h * r:(h + 1) * r, b * 8:(b + 1) * 8]
        gx[0].last()
        gx[0].finish()

        def staged(u, k):
            h, e = lax.div(u, exp_loc), lax.rem(u, exp_loc)
            slot = lax.rem(u, 2)
            part = pl.ds(pl.multiple_of(h * m, LANES), m)
            if k == 2:
                return pltpu.make_async_copy(stage_t.at[slot], ht_all.at[e, :, part], stage_sems.at[slot, k])
            return pltpu.make_async_copy(stage.at[slot, k], (da_all, db_all)[k].at[e, part, :], stage_sems.at[slot, k])

        lane = lax.broadcasted_iota(jnp.int32, (m, LANES), 1)

        def at1():
            gdy[1].relay()

        def at2():
            gx[1].last()

        def at3():
            gdy[1].last()
            gx[1].finish()

        def at4():
            gxa.relay()
            gdy[1].finish()

        def at5():
            sy[0].begin()
            sdx[0].begin()
            gxa.last()

        def at6():
            sy[0].middle()
            sdx[0].middle()
            gxa.finish()

        def at8():
            sy[0].late()

        early = {1: at1, 2: at2, 3: at3, 4: at4, 5: at5, 6: at6, 8: at8}

        def mid0():
            gdy[0].last()
            gdy[0].finish()
            gx[1].relay()
            gxa.begin()

        def unit(u, _):
            h, e = lax.div(u, exp_loc), lax.rem(u, exp_loc)
            slot = lax.rem(u, 2)

            @pl.when(u < exp_loc)
            def _():
                for k, (src, dst) in enumerate(((wg_in, wg), (wu_in, wu), (wd_in, wd))):
                    pltpu.make_async_copy(src.at[e], dst.at[e], w_sems.at[e, k]).wait()

            @pl.when(u >= 2)
            def _():
                for k in range(3):
                    staged(u - 2, k).wait()

            for k, events in early.items():
                pl.when(u == k)(events)

            gate = jnp.sum(jnp.where(lane == e, gcol[h], 0.0), axis=1, keepdims=True)
            mask = gate > 0.0
            a = jnp.where(mask, dot_nn(xb[h], wg[e]), 0.0)
            b = jnp.where(mask, dot_nn(xb[h], wu[e]), 0.0)
            sig = jax.nn.sigmoid(a)
            act = a * sig
            hid[...] = (act * b).astype(BF16)
            stage_t[slot] = hid[...].T
            s1[...] = b * sig * (1.0 + a * (1.0 - sig))
            s2[...] = act
            pl.when(u == 0)(mid0)
            dots = jnp.zeros((m, LANES), F32)
            for n in range(d_model // tile):
                cols = pl.ds(n * tile, tile)
                o = dot_nn(hid[...], wd[e, :, cols]).astype(BF16).astype(F32)
                dy = dyb[h, :, cols].astype(F32)
                y_part[h, :, cols] += gate * o
                prod = dy * o
                for k in range(tile // LANES):
                    dots += prod[:, k * LANES:(k + 1) * LANES]
                d_o[:, cols] = (gate * dy).astype(BF16)
            dgc[h] = jnp.where(lane == e, jnp.sum(dots, axis=1, keepdims=True), dgc[h])
            dh = dot_nt(d_o[...], wd[e]).astype(BF16).astype(F32)
            stage[slot, 0] = (dh * s1[...]).astype(BF16)
            stage[slot, 1] = (dh * s2[...]).astype(BF16)
            for k in range(3):
                staged(u, k).start()
            for n in range(d_model // tile):
                cols = pl.ds(n * tile, tile)
                dxe = dot_nt(stage[slot, 0], wg[e, cols, :]) + dot_nt(stage[slot, 1], wu[e, cols, :])
                dx_part[h, :, cols] += dxe.astype(BF16).astype(F32)
            return 0

        lax.fori_loop(0, units, unit, 0)

        sy[1].begin()
        sdx[1].begin()
        sdx[0].late()
        sy[1].middle()
        sdx[1].middle()
        attention(xab, wqkv, wo, ctx, at_part, attn_dims)
        sat.begin()
        for h in range(HALVES):
            turned = dgc[h].T
            for c in range(2):
                dgt[h, c] = turned[0:8, c * LANES:(c + 1) * LANES]
            xt[:, h * m:(h + 1) * m] = xb[h].T
        saves = [pltpu.make_async_copy(xt, xt_all, out_sems.at[0]), pltpu.make_async_copy(dyb, dy_all, out_sems.at[1]), pltpu.make_async_copy(gcol, gates_out, out_sems.at[2])]
        for save in saves:
            save.start()
        for h in range(HALVES):
            for link in dg_links[h]:
                link.start()
            dg_out[me, h] = dgt[h, place.core]
        sat.middle()
        for s, out in ((sy[0], y_out), (sdx[0], dx_out)):
            s.finish(out.at[0:r, :])
        sy[1].late()
        sdx[1].late()
        sat.late()
        for h in range(HALVES):
            for link in dg_links[h]:
                link.arrive()
        for s, out in ((sy[1], y_out), (sdx[1], dx_out)):
            s.finish(out.at[r:2 * r, :])
        sat.finish(attn_out)
        for u in (units - 2, units - 1):
            for k in range(3):
                staged(jnp.int32(u), k).wait()
        for save in saves:
            save.wait()
        for item in gx + gdy + [gxa] + sy + sdx + [sat]:
            item.drain()
        for link in routes + dg_links[0] + dg_links[1]:
            link.sent()
        assert pool.used == NUM_LINKS

    return kernel, r, m


def weight_grads(xt_ref, dy_ref, gates_ref, da_ref, db_ref, ht_ref, dwg_ref, dwu_ref, dwd_ref):
    lane = lax.broadcasted_iota(jnp.int32, gates_ref.shape, 1)
    gate = jnp.sum(jnp.where(lane == pl.program_id(0), gates_ref[...], 0.0), axis=1, keepdims=True)
    d_o = (gate * dy_ref[...].astype(F32)).astype(BF16)
    dwg_ref[...] = dot_nn(xt_ref[...], da_ref[...])
    dwu_ref[...] = dot_nn(xt_ref[...], db_ref[...])
    dwd_ref[...] = dot_nn(ht_ref[...], d_o)


def solution(mesh):
    num_dev = mesh.shape['ei'] * mesh.shape['eo']
    assert num_dev == NUM_DEV

    def local_step(x_tokens, expert_idx, gate_vals, dy_tokens, w_gate, w_up, w_down, x_attn, w_query, w_key, w_value, w_out):
        tok, d_model = x_tokens.shape
        top_k = expert_idx.shape[1]
        exp_loc, _, d_ff = w_gate.shape
        seq = x_attn.shape[1]
        heads, head_dim = w_query.shape[1], w_query.shape[2]
        kv_dim = w_key.shape[1] * head_dim
        q_dim = heads * head_dim
        ids = jnp.arange(NUM_DEV * exp_loc, dtype=jnp.int32).reshape(NUM_DEV, exp_loc, 1, 1)
        table = jnp.sum(jnp.where(expert_idx.T[None, None] == ids, gate_vals.T[None, None], 0.0), axis=2)
        table = jnp.pad(table, ((0, 0), (0, 8 - exp_loc), (0, LANES - tok)))
        gt = table.reshape(4, 2, 8, LANES).transpose(1, 0, 2, 3).reshape(NUM_DEV, 8, LANES)
        pad = -(q_dim + 2 * kv_dim) % LANES
        wqkv = jnp.concatenate([w_query.reshape(d_model, q_dim), w_key.reshape(d_model, kv_dim), w_value.reshape(d_model, kv_dim), jnp.zeros((d_model, pad), BF16)], axis=1)
        wo = w_out.reshape(q_dim, d_model)
        kernel, r, m = make_layer_kernel(tok, d_model, d_ff, exp_loc, (seq, kv_dim, heads, head_dim))
        any_spec = pl.BlockSpec(memory_space=pl.ANY)
        vmem_spec = pl.BlockSpec(memory_space=pltpu.VMEM)
        shape = jax.ShapeDtypeStruct
        total = tok * NUM_DEV

        def half_shapes():
            return [pltpu.VMEM((HALVES,) + s.shape, s.dtype) for s in scatter_shapes(r, d_model)]

        y, dx, attn, dgt, xt, dy_all, da, db, ht, gates = pl.pallas_call(
            kernel,
            out_shape=(shape((tok, d_model), BF16), shape((tok, d_model), BF16), shape((tok, d_model), BF16), shape((NUM_DEV, HALVES, 8, LANES), F32),
                       shape((d_model, total), BF16), shape((HALVES, m, d_model), BF16),
                       shape((exp_loc, total, d_ff), BF16), shape((exp_loc, total, d_ff), BF16), shape((exp_loc, d_ff, total), BF16), shape((HALVES, m, LANES), F32)),
            in_specs=[any_spec, any_spec, any_spec, vmem_spec, any_spec, any_spec, any_spec, vmem_spec, vmem_spec],
            out_specs=(vmem_spec,) * 4 + (any_spec,) * 6,
            scratch_shapes=[pltpu.VMEM((HALVES, m, d_model), BF16), pltpu.VMEM((HALVES, m, d_model), BF16), pltpu.VMEM((total, d_model), BF16),
                            pltpu.VMEM((NUM_DEV, 8, LANES), F32), pltpu.VMEM((HALVES, m, LANES), F32),
                            pltpu.VMEM((exp_loc, d_model, d_ff), BF16), pltpu.VMEM((exp_loc, d_model, d_ff), BF16), pltpu.VMEM((exp_loc, d_ff, d_model), BF16),
                            pltpu.VMEM((HALVES, m, d_model), F32), pltpu.VMEM((HALVES, m, d_model), F32), pltpu.VMEM((total, d_model), F32), pltpu.VMEM((total, q_dim), BF16),
                            pltpu.VMEM((m, d_ff), F32), pltpu.VMEM((m, d_ff), F32), pltpu.VMEM((m, d_model), BF16),
                            pltpu.VMEM((HALVES, m, LANES), F32), pltpu.VMEM((HALVES, 2, 8, LANES), F32), pltpu.VMEM((2, 2, m, d_ff), BF16),
                            pltpu.VMEM((m, d_ff), BF16), pltpu.VMEM((2, d_ff, m), BF16), pltpu.VMEM((d_model, total), BF16)]
            + half_shapes() + half_shapes() + scatter_shapes(tok, d_model)
            + [pltpu.SemaphoreType.DMA((NUM_LINKS,)), pltpu.SemaphoreType.DMA((NUM_LINKS,)), pltpu.SemaphoreType.DMA((exp_loc, 3)),
               pltpu.SemaphoreType.DMA((5,)), pltpu.SemaphoreType.DMA((3,)), pltpu.SemaphoreType.DMA((2, 3))],
            compiler_params=pltpu.CompilerParams(collective_id=0, has_side_effects=True, vmem_limit_bytes=67000000),
            name='layer',
        )(x_tokens, dy_tokens, x_attn.reshape(tok, d_model), gt, w_gate, w_up, w_down, wqkv, wo)

        width = 512
        steps = d_model // width
        dw_gate, dw_up, dw_down = pl.pallas_call(
            weight_grads,
            grid=(exp_loc, steps),
            out_shape=(shape((exp_loc, d_model, d_ff), F32), shape((exp_loc, d_model, d_ff), F32), shape((exp_loc, d_ff, d_model), F32)),
            in_specs=[pl.BlockSpec((width, total), lambda e, n: (n, 0)), pl.BlockSpec((total, width), lambda e, n: (0, n)), pl.BlockSpec((total, LANES), lambda e, n: (0, 0)),
                      pl.BlockSpec((None, total, d_ff), lambda e, n: (e, 0, 0)), pl.BlockSpec((None, total, d_ff), lambda e, n: (e, 0, 0)), pl.BlockSpec((None, d_ff, total), lambda e, n: (e, 0, 0))],
            out_specs=(pl.BlockSpec((None, width, d_ff), lambda e, n: (e, n, 0)), pl.BlockSpec((None, width, d_ff), lambda e, n: (e, n, 0)), pl.BlockSpec((None, d_ff, width), lambda e, n: (e, 0, n))),
            compiler_params=pltpu.CompilerParams(vmem_limit_bytes=60000000),
            cost_estimate=pl.CostEstimate(flops=3 * 2 * total * d_model * d_ff * exp_loc, bytes_accessed=3 * 4 * exp_loc * d_model * d_ff, transcendentals=0),
            name='weight_grads',
        )(xt, dy_all.reshape(total, d_model), gates.reshape(total, LANES), da, db, ht)

        chip = lax.axis_index('ei') * 2 + lax.div(lax.axis_index('eo'), 2)
        mine = lax.dynamic_slice_in_dim(dgt, chip * r, r, axis=3)[:, :, :exp_loc]
        mine = mine.reshape(2, 4, HALVES, exp_loc, r).transpose(1, 0, 3, 2, 4).reshape(NUM_DEV * exp_loc, 1, tok)
        ids = jnp.arange(NUM_DEV * exp_loc, dtype=jnp.int32)[:, None, None]
        d_gates = jnp.sum(jnp.where(expert_idx.T[None] == ids, mine, 0.0), axis=0).T
        return y, dx, d_gates, dw_gate, dw_up, dw_down, attn.reshape(x_attn.shape)

    spec_rows = P(TOKEN_AXES, None)
    spec_seqs = P(TOKEN_AXES, None, None)
    spec_experts = P(GROUP_AXES, None, None)
    spec_heads = P(None, GROUP_AXES, None)
    return jax.shard_map(local_step, mesh=mesh,
                         in_specs=(spec_rows, spec_rows, spec_rows, spec_rows, spec_experts, spec_experts, spec_experts, spec_seqs, spec_heads, spec_heads, spec_heads, spec_experts),
                         out_specs=(spec_rows, spec_rows, spec_rows, spec_seqs, spec_seqs, spec_seqs, spec_seqs),
                         check_vma=False)
```

```python
import functools

import jax
import jax.numpy as jnp
from jax import lax
from jax.experimental import pallas as pl
from jax.experimental.pallas import tpu as pltpu
from jax.sharding import PartitionSpec as P

GROUP_AXES = ('ei', 'eo')
TOKEN_AXES = ('dp', 'ei', 'eo')
F32 = jnp.float32
BF16 = jnp.bfloat16
MESH_ID = pl.DeviceIdType.MESH
HALVES = 2
NUM_DEV = 8
LANES = 128


def dot_nn(lhs, rhs):
    return jnp.dot(lhs, rhs, preferred_element_type=F32)


def dot_nt(lhs, rhs):
    return lax.dot_general(lhs, rhs, (((1,), (1,)), ((), ())), preferred_element_type=F32)


def dot_tn(lhs, rhs):
    return lax.dot_general(lhs, rhs, (((0,), (0,)), ((), ())), preferred_element_type=F32)


class Place:
    def __init__(self):
        i = lax.axis_index('ei')
        o = lax.axis_index('eo')
        x = lax.div(o, 2)
        c = lax.rem(o, 2)
        self.core = c
        self.chip = i * 2 + x
        self.dev = {}
        self.block = {}
        self.flat = {}
        for flip_y in (0, 1):
            for flip_x in (0, 1):
                for flip_c in (0, 1):
                    yy = 1 - i if flip_y else i
                    xx = 1 - x if flip_x else x
                    cc = 1 - c if flip_c else c
                    name = ('y' if flip_y else '') + ('x' if flip_x else '') + ('c' if flip_c else '')
                    self.dev[name] = (0, yy, xx * 2 + cc)
                    self.block[name] = cc * 4 + yy * 2 + xx
                    self.flat[name] = yy * 4 + xx * 2 + cc


class Link:
    def __init__(self, pool, src, dst, land, device):
        send, recv = pool.take()
        self.out = pltpu.make_async_remote_copy(src_ref=src, dst_ref=dst, send_sem=send, recv_sem=recv, device_id=device, device_id_type=MESH_ID)
        self.inn = pltpu.make_async_remote_copy(src_ref=land, dst_ref=land, send_sem=send, recv_sem=recv, device_id=device, device_id_type=MESH_ID)

    def start(self):
        self.out.start()

    def arrive(self):
        self.inn.wait_recv()

    def sent(self):
        self.out.wait_send()


class Pool:
    def __init__(self, sends, recvs):
        self.sends, self.recvs, self.used = sends, recvs, 0

    def take(self):
        k = self.used
        self.used += 1
        return self.sends.at[k], self.recvs.at[k]


class Gather:
    def __init__(self, pool, place, buf, rows):
        def at(name, lo=0, n=rows):
            return buf.at[pl.ds(pl.multiple_of(place.block[name] * rows + lo, 8), n), :]

        half = rows // 2
        own = at('')
        dev = place.dev
        self.to_x = Link(pool, own, own, at('x'), dev['x'])
        self.to_y = Link(pool, own, own, at('y'), dev['y'])
        self.to_c = Link(pool, own, own, at('c'), dev['c'])
        self.relay_x = Link(pool, at('y', 0, half), at('y', 0, half), at('yx', 0, half), dev['x'])
        self.relay_y = Link(pool, at('x', half, half), at('x', half, half), at('yx', half, half), dev['y'])
        self.core_x = Link(pool, at('x'), at('x'), at('xc'), dev['c'])
        self.core_y = Link(pool, at('y'), at('y'), at('yc'), dev['c'])
        self.core_d = Link(pool, at('yx'), at('yx'), at('yxc'), dev['c'])
        self.links = (self.to_x, self.to_y, self.to_c, self.relay_x, self.relay_y, self.core_x, self.core_y, self.core_d)

    def begin(self):
        self.to_x.start()
        self.to_y.start()
        self.to_c.start()

    def relay(self):
        self.to_y.arrive()
        self.relay_x.start()
        self.to_x.arrive()
        self.relay_y.start()
        self.core_y.start()
        self.core_x.start()

    def last(self):
        self.relay_x.arrive()
        self.relay_y.arrive()
        self.core_d.start()

    def finish(self):
        self.to_c.arrive()
        self.core_x.arrive()
        self.core_y.arrive()
        self.core_d.arrive()

    def drain(self):
        for link in self.links:
            link.sent()


class Scatter:
    def __init__(self, pool, place, part, from_core, from_x, from_y, last_x, last_y, rows):
        half = rows // 2
        self.half, self.part, self.rows, self.place = half, part, rows, place
        self.from_core, self.from_x, self.from_y, self.last_x, self.last_y = from_core, from_x, from_y, last_x, last_y
        four = 4 * rows
        self.mine = pl.multiple_of(place.core * four, 8)
        other = part.at[pl.ds(pl.multiple_of((1 - place.core) * four, 8), four), :]
        dev = place.dev
        self.core = Link(pool, other, from_core, from_core, dev['c'])
        self.x0 = Link(pool, self.at('x', 0), from_x.at[0], from_x.at[0], dev['x'])
        self.x1 = Link(pool, self.at('yx', 0), from_x.at[1], from_x.at[1], dev['x'])
        self.y0 = Link(pool, self.at('y', half), from_y.at[0], from_y.at[0], dev['y'])
        self.y1 = Link(pool, self.at('yx', half), from_y.at[1], from_y.at[1], dev['y'])
        self.end_y = Link(pool, self.at('y', 0), last_y, last_y, dev['y'])
        self.end_x = Link(pool, self.at('x', half), last_x, last_x, dev['x'])
        self.links = (self.core, self.x0, self.x1, self.y0, self.y1, self.end_y, self.end_x)

    def at(self, name, lo):
        return self.part.at[pl.ds(pl.multiple_of(self.place.block[name] * self.rows + lo, 8), self.half), :]

    def begin(self):
        self.core.start()

    def middle(self):
        self.core.arrive()
        mine = pl.ds(self.mine, 4 * self.rows)
        self.part[mine, :] = self.part[mine, :] + self.from_core[...]
        self.x1.start()
        self.y1.start()
        self.x0.start()
        self.y0.start()

    def late(self):
        self.x1.arrive()
        here = self.at('y', 0)
        here[...] = here[...] + self.from_x[1]
        self.end_y.start()
        self.y1.arrive()
        here = self.at('x', self.half)
        here[...] = here[...] + self.from_y[1]
        self.end_x.start()

    def finish(self, out):
        half = self.half
        self.x0.arrive()
        self.y0.arrive()
        self.end_y.arrive()
        self.end_x.arrive()
        out[0:half, :] = (self.at('', 0)[...] + self.from_x[0] + self.last_y[...]).astype(BF16)
        out[half:2 * half, :] = (self.at('', half)[...] + self.from_y[0] + self.last_x[...]).astype(BF16)

    def drain(self):
        for link in self.links:
            link.sent()


def scatter_shapes(rows, width):
    half = rows // 2
    return [pltpu.VMEM((4 * rows, width), F32), pltpu.VMEM((2, half, width), F32), pltpu.VMEM((2, half, width), F32),
            pltpu.VMEM((half, width), F32), pltpu.VMEM((half, width), F32)]


NUM_LINKS = 7 + 14 + 8 * 5 + 7 * 5


def attention_pair(xa, wqkv, wo, part, first, dims):
    seq, kv_dim, heads, head_dim = dims
    q_dim = heads * head_dim
    pair = 2 * seq
    rows = pl.ds(pl.multiple_of(first, pair), pair)
    row = lax.broadcasted_iota(jnp.int32, (pair, pair), 0)
    col = lax.broadcasted_iota(jnp.int32, (pair, pair), 1)
    causal = (row >= col) & ((row >= seq) == (col >= seq))
    qkv = dot_nt(xa[rows, :], wqkv[...]).astype(BF16)
    keys = qkv[:, q_dim:q_dim + kv_dim]
    vals = qkv[:, q_dim + kv_dim:q_dim + 2 * kv_dim]
    outs = []
    for h in range(heads):
        scores = dot_nt(qkv[:, h * head_dim:(h + 1) * head_dim], keys) * head_dim ** -0.5
        scores = jnp.where(causal, scores, -1e30)
        top = jnp.max(scores, axis=1, keepdims=True)
        ex = jnp.exp(scores - top)
        probs = (ex / jnp.sum(ex, axis=1, keepdims=True)).astype(BF16)
        outs.append(dot_nn(probs, vals).astype(BF16))
    part[rows, :] = dot_nn(jnp.concatenate(outs, axis=1), wo[...])


def make_layer_kernel(tok, d_model, d_ff, exp_loc, attn_dims):
    r = tok // HALVES
    m = r * NUM_DEV
    tile = 512
    units = HALVES * exp_loc

    def kernel(x_in, dy_in, xa_in, gt_in, idx_in, wg_in, wu_in, wd_in, wq_in, wk_in, wv_in, wo_in,
               y_out, dx_out, attn_out, dg_out, xt_all, dy_all, da_all, db_all, ht_all, gates_out,
               xb, dyb, xab, gtb, gcol, wg, wu, wd, y_part, dx_part, at_part, wqkv, wo, s1, s2, d_o, dgc, dgt, stage, hid, stage_t, xt, dgl,
               ry0, ry1, ry2, ry3, ry4, rd0, rd1, rd2, rd3, rd4, ra0, ra1, ra2, ra3, ra4,
               send_sems, recv_sems, w_sems, in_sems, aw_sems, out_sems, stage_sems):
        place = Place()
        pool = Pool(send_sems, recv_sems)
        dev, block = place.dev, place.block
        me = block['']

        def own_rows(buf, rows):
            return buf.at[pl.ds(pl.multiple_of(me * rows, 8), rows), :]

        loads = []
        for h in range(HALVES):
            loads.append(pltpu.make_async_copy(x_in.at[h * r:(h + 1) * r, :], own_rows(xb.at[h], r), in_sems.at[h]))
            loads.append(pltpu.make_async_copy(dy_in.at[h * r:(h + 1) * r, :], own_rows(dyb.at[h], r), in_sems.at[2 + h]))
        loads.append(pltpu.make_async_copy(xa_in, own_rows(xab, tok), in_sems.at[4]))
        for load in loads:
            load.start()
        q_dim, kv_dim = wq_in.shape[0], wk_in.shape[0]
        attn_loads = [pltpu.make_async_copy(wq_in, wqkv.at[0:q_dim, :], aw_sems.at[0]), pltpu.make_async_copy(wk_in, wqkv.at[q_dim:q_dim + kv_dim, :], aw_sems.at[1]),
                      pltpu.make_async_copy(wv_in, wqkv.at[q_dim + kv_dim:q_dim + 2 * kv_dim, :], aw_sems.at[2]), pltpu.make_async_copy(wo_in, wo, aw_sems.at[3])]
        for load in attn_loads:
            load.start()
        weights = []
        for e in range(exp_loc):
            weights.append([pltpu.make_async_copy(src.at[e], dst.at[e], w_sems.at[e, k]) for k, (src, dst) in enumerate(((wg_in, wg), (wu_in, wu), (wd_in, wd)))])
        for ws in weights:
            for w in ws:
                w.start()

        barrier = pltpu.get_barrier_semaphore()
        peers = [name for name in dev if name]
        for name in peers:
            pl.semaphore_signal(barrier, inc=1, device_id=dev[name], device_id_type=MESH_ID)
        pl.semaphore_wait(barrier, len(peers))

        routes = [Link(pool, gt_in.at[place.flat[name]], gtb.at[me], gtb.at[block[name]], dev[name]) for name in peers]
        gx = [Gather(pool, place, xb.at[h], r) for h in range(HALVES)]
        gdy = [Gather(pool, place, dyb.at[h], r) for h in range(HALVES)]
        gxa = Gather(pool, place, xab, tok)
        sy = [Scatter(pool, place, y_part.at[h], ry0.at[h], ry1.at[h], ry2.at[h], ry3.at[h], ry4.at[h], r) for h in range(HALVES)]
        sdx = [Scatter(pool, place, dx_part.at[h], rd0.at[h], rd1.at[h], rd2.at[h], rd3.at[h], rd4.at[h], r) for h in range(HALVES)]
        sat = Scatter(pool, place, at_part, ra0, ra1, ra2, ra3, ra4, tok)
        dg_links = [[Link(pool, dgt.at[h, 1 - place.core if 'c' in name else place.core], dgl.at[me, h], dgl.at[block[name], h], dev[name]) for name in peers] for h in range(HALVES)]

        for link in routes:
            link.start()
        gtb[me] = gt_in[place.flat['']]
        for load in loads:
            load.wait()
        gxa.begin()
        gx[0].begin()
        gdy[0].begin()
        dgc[...] = jnp.zeros_like(dgc)
        gcol[...] = jnp.zeros_like(gcol)
        y_part[...] = jnp.zeros_like(y_part)
        dx_part[...] = jnp.zeros_like(dx_part)
        for load in attn_loads:
            load.wait()

        def pair(name):
            attention_pair(xab, wqkv, wo, at_part, lax.div(block[name], 2) * (2 * tok), attn_dims)

        gxa.relay()
        pair('')
        gx[0].relay()
        gxa.to_c.arrive()
        gxa.core_x.arrive()
        pair('c')
        gdy[0].relay()
        gx[1].begin()
        gdy[1].begin()
        gxa.last()
        pair('y')
        gx[0].last()
        gxa.core_y.arrive()
        gxa.core_d.arrive()
        pair('yc')
        sat.begin()
        for link in routes:
            link.arrive()
        wide = jnp.concatenate([gtb[...].reshape(NUM_DEV * 8, LANES), jnp.zeros((LANES - NUM_DEV * 8, LANES), F32)], axis=0).T
        for h in range(HALVES):
            for b in range(NUM_DEV):
                gcol[h, b * r:(b + 1) * r, 0:8] = wide[h * r:(h + 1) * r, b * 8:(b + 1) * 8]
        gx[0].finish()

        def staged(u, k):
            h, e = lax.div(u, exp_loc), lax.rem(u, exp_loc)
            slot = lax.rem(u, 2)
            part = pl.ds(pl.multiple_of(h * m, LANES), m)
            if k == 2:
                return pltpu.make_async_copy(stage_t.at[slot], ht_all.at[e, :, part], stage_sems.at[slot, k])
            return pltpu.make_async_copy(stage.at[slot, k], (da_all, db_all)[k].at[e, part, :], stage_sems.at[slot, k])

        lane = lax.broadcasted_iota(jnp.int32, (m, LANES), 1)

        def at2():
            gx[1].last()

        def at3():
            gdy[1].last()
            gx[1].finish()

        def at4():
            gdy[1].finish()

        def at5():
            sy[0].begin()
            sdx[0].begin()

        def at6():
            sy[0].middle()
            sdx[0].middle()

        def at8():
            sat.finish(attn_out)

        early = {1: gx[1].relay, 2: at2, 3: at3, 4: at4, 5: at5, 6: at6, 8: at8}

        def mid0():
            gdy[0].last()
            gdy[0].finish()

        def mid1():
            gdy[1].relay()
            sat.middle()

        mid = {0: mid0, 1: mid1, 5: sat.late, 9: sy[0].late}

        def unit(u, _):
            h, e = lax.div(u, exp_loc), lax.rem(u, exp_loc)
            slot = lax.rem(u, 2)

            @pl.when(u < exp_loc)
            def _():
                for k, (src, dst) in enumerate(((wg_in, wg), (wu_in, wu), (wd_in, wd))):
                    pltpu.make_async_copy(src.at[e], dst.at[e], w_sems.at[e, k]).wait()

            @pl.when(u >= 2)
            def _():
                for k in range(3):
                    staged(u - 2, k).wait()

            for k, events in early.items():
                pl.when(u == k)(events)

            gate = jnp.sum(jnp.where(lane == e, gcol[h], 0.0), axis=1, keepdims=True)
            mask = gate > 0.0
            a = jnp.where(mask, dot_nn(xb[h], wg[e]), 0.0)
            b = jnp.where(mask, dot_nn(xb[h], wu[e]), 0.0)
            sig = jax.nn.sigmoid(a)
            act = a * sig
            hid[...] = (act * b).astype(BF16)
            stage_t[slot] = hid[...].T
            s1[...] = b * sig * (1.0 + a * (1.0 - sig))
            s2[...] = act
            for k, events in mid.items():
                pl.when(u == k)(events)
            dots = jnp.zeros((m, LANES), F32)
            for n in range(d_model // tile):
                cols = pl.ds(n * tile, tile)
                o = dot_nn(hid[...], wd[e, :, cols]).astype(BF16).astype(F32)
                dy = dyb[h, :, cols].astype(F32)
                y_part[h, :, cols] += gate * o
                prod = dy * o
                for k in range(tile // LANES):
                    dots += prod[:, k * LANES:(k + 1) * LANES]
                d_o[:, cols] = (gate * dy).astype(BF16)
            dgc[h] = jnp.where(lane == e, jnp.sum(dots, axis=1, keepdims=True), dgc[h])
            dh = dot_nt(d_o[...], wd[e]).astype(BF16).astype(F32)
            stage[slot, 0] = (dh * s1[...]).astype(BF16)
            stage[slot, 1] = (dh * s2[...]).astype(BF16)
            for k in range(3):
                staged(u, k).start()
            for n in range(d_model // tile):
                cols = pl.ds(n * tile, tile)
                dxe = dot_nt(stage[slot, 0], wg[e, cols, :]) + dot_nt(stage[slot, 1], wu[e, cols, :])
                dx_part[h, :, cols] += dxe.astype(BF16).astype(F32)
            return 0

        lax.fori_loop(0, units, unit, 0)

        sy[1].begin()
        sdx[1].begin()
        for h in range(HALVES):
            turned = dgc[h].T
            for c in range(2):
                dgt[h, c] = turned[0:8, c * LANES:(c + 1) * LANES]
        sdx[0].late()
        sy[1].middle()
        sdx[1].middle()
        for h in range(HALVES):
            for link in dg_links[h]:
                link.start()
            dgl[me, h] = dgt[h, place.core]
            xt[:, h * m:(h + 1) * m] = xb[h].T
        saves = [pltpu.make_async_copy(xt, xt_all, out_sems.at[0]), pltpu.make_async_copy(dyb, dy_all, out_sems.at[1]), pltpu.make_async_copy(gcol, gates_out, out_sems.at[2])]
        for save in saves:
            save.start()
        for s, out in ((sy[0], y_out), (sdx[0], dx_out)):
            s.finish(out.at[0:r, :])
        for h in range(HALVES):
            for link in dg_links[h]:
                link.arrive()
        for h in range(HALVES):
            slots = idx_in[:, h * r:(h + 1) * r]
            total = jnp.zeros(slots.shape, F32)
            for b in range(NUM_DEV):
                first = ((b // 2) % 2 * 4 + b % 2 * 2 + b // 4) * exp_loc
                rows = dgl[b, h]
                mine = jnp.zeros((8, r), F32)
                for q in range(LANES // r):
                    mine = jnp.where(place.chip == q, rows[:, q * r:(q + 1) * r], mine)
                for e in range(exp_loc):
                    total = jnp.where(slots == first + e, mine[e:e + 1, :], total)
            dg_out[:, h * r:(h + 1) * r] = total
        sy[1].late()
        sdx[1].late()
        for s, out in ((sy[1], y_out), (sdx[1], dx_out)):
            s.finish(out.at[r:2 * r, :])
        for u in (units - 2, units - 1):
            for k in range(3):
                staged(jnp.int32(u), k).wait()
        for save in saves:
            save.wait()
        for item in gx + gdy + [gxa] + sy + sdx + [sat]:
            item.drain()
        for link in routes + dg_links[0] + dg_links[1]:
            link.sent()
        assert pool.used == NUM_LINKS

    return kernel, r, m


def weight_grads(width, slots, xt_in, dy_in, g_in, da_in, db_in, ht_in, y_in, dx_in, at_in, dg_in,
                 dwg, dwu, dwd, y_out, dx_out, at_out, dg_out,
                 xt, dy, g, da, db, ht, sg, su, sd, y, dx, at, dg, x_sems, d_sems, g_sem, e_sems, o_sems, p_sems):
    exp_loc = da.shape[0]
    steps = dy.shape[1] // width

    def load(e, k):
        src, dst = ((da_in, da), (db_in, db), (ht_in, ht))[k]
        return pltpu.make_async_copy(src.at[e], dst.at[e], e_sems.at[e, k])

    def x_load(n):
        rows = slice(n * width, (n + 1) * width)
        return pltpu.make_async_copy(xt_in.at[rows, :], xt.at[rows, :], x_sems.at[n])

    def dy_load(n):
        cols = slice(n * width, (n + 1) * width)
        return pltpu.make_async_copy(dy_in.at[:, cols], dy.at[:, cols], d_sems.at[n])

    g_load = pltpu.make_async_copy(g_in, g, g_sem)
    for copy in (x_load(0), load(0, 0), load(0, 1), load(0, 2), dy_load(0), g_load):
        copy.start()
    for n in range(1, steps):
        x_load(n).start()
        dy_load(n).start()
    for e in range(1, exp_loc):
        for k in range(3):
            load(e, k).start()
    passing = ((y_in, y, y_out), (dx_in, dx, dx_out), (at_in, at, at_out), (dg_in, dg, dg_out))
    take = [pltpu.make_async_copy(src, mid, p_sems.at[k, 0]) for k, (src, mid, _) in enumerate(passing)]
    give = [pltpu.make_async_copy(mid, dst, p_sems.at[k, 1]) for k, (_, mid, dst) in enumerate(passing)]
    for copy in take:
        copy.start()

    def store(s, k):
        e, n = lax.div(s, steps), lax.rem(s, steps)
        slot = lax.rem(s, slots)
        part = pl.ds(pl.multiple_of(n * width, LANES), width)
        if k == 2:
            return pltpu.make_async_copy(sd.at[slot], dwd.at[e, :, part], o_sems.at[slot, k])
        return pltpu.make_async_copy((sg, su)[k].at[slot], (dwg, dwu)[k].at[e, part, :], o_sems.at[slot, k])

    lane = lax.broadcasted_iota(jnp.int32, g.shape, 1)

    def step(s, _):
        e, n = lax.div(s, steps), lax.rem(s, steps)
        slot = lax.rem(s, slots)
        for k in range(steps):
            @pl.when(s == k)
            def _():
                x_load(k).wait()

        @pl.when(n == 0)
        def _():
            load(e, 0).wait()
            load(e, 1).wait()

        @pl.when(s >= slots)
        def _():
            for k in range(3):
                store(s - slots, k).wait()

        part = pl.ds(pl.multiple_of(n * width, LANES), width)
        sg[slot] = dot_nn(xt[part, :], da[e])
        store(s, 0).start()
        su[slot] = dot_nn(xt[part, :], db[e])
        store(s, 1).start()

        @pl.when(n == 0)
        def _():
            load(e, 2).wait()

        @pl.when(s == 0)
        def _():
            g_load.wait()

        @pl.when(s == 3)
        def _():
            for copy in take:
                copy.wait()
            for copy in give:
                copy.start()

        for k in range(steps):
            @pl.when(s == k)
            def _():
                dy_load(k).wait()

        gate = jnp.sum(jnp.where(lane == e, g[...], 0.0), axis=1, keepdims=True)
        d_o = (gate * dy[:, part].astype(F32)).astype(BF16)
        sd[slot] = dot_nn(ht[e], d_o)
        store(s, 2).start()
        return 0

    lax.fori_loop(0, exp_loc * steps, step, 0)
    for s in range(exp_loc * steps - slots, exp_loc * steps):
        for k in range(3):
            store(jnp.int32(s), k).wait()
    for copy in give:
        copy.wait()


def solution(mesh):
    num_dev = mesh.shape['ei'] * mesh.shape['eo']
    assert num_dev == NUM_DEV

    def local_step(x_tokens, expert_idx, gate_vals, dy_tokens, w_gate, w_up, w_down, x_attn, w_query, w_key, w_value, w_out):
        tok, d_model = x_tokens.shape
        top_k = expert_idx.shape[1]
        exp_loc, _, d_ff = w_gate.shape
        seq = x_attn.shape[1]
        heads, head_dim = w_query.shape[1], w_query.shape[2]
        kv_dim = w_key.shape[1] * head_dim
        q_dim = heads * head_dim
        ids = jnp.arange(NUM_DEV * exp_loc, dtype=jnp.int32).reshape(NUM_DEV, exp_loc, 1, 1)
        table = jnp.sum(jnp.where(expert_idx.T[None, None] == ids, gate_vals.T[None, None], 0.0), axis=2)
        table = jnp.pad(table, ((0, 0), (0, 8 - exp_loc), (0, LANES - tok)))
        wq = w_query.transpose(1, 2, 0).reshape(q_dim, d_model)
        wk = w_key.transpose(1, 2, 0).reshape(kv_dim, d_model)
        wv = w_value.transpose(1, 2, 0).reshape(kv_dim, d_model)
        wo = w_out.reshape(q_dim, d_model)
        kernel, r, m = make_layer_kernel(tok, d_model, d_ff, exp_loc, (seq, kv_dim, heads, head_dim))
        any_spec = pl.BlockSpec(memory_space=pl.ANY)
        vmem_spec = pl.BlockSpec(memory_space=pltpu.VMEM)
        shape = jax.ShapeDtypeStruct
        total = tok * NUM_DEV

        def half_shapes():
            return [pltpu.VMEM((HALVES,) + s.shape, s.dtype) for s in scatter_shapes(r, d_model)]

        y, dx, attn, dgt, xt, dy_all, da, db, ht, gates = pl.pallas_call(
            kernel,
            out_shape=(shape((tok, d_model), BF16), shape((tok, d_model), BF16), shape((tok, d_model), BF16), shape((top_k, tok), F32),
                       shape((d_model, total), BF16), shape((HALVES, m, d_model), BF16),
                       shape((exp_loc, total, d_ff), BF16), shape((exp_loc, total, d_ff), BF16), shape((exp_loc, d_ff, total), BF16), shape((HALVES, m, LANES), F32)),
            in_specs=[any_spec, any_spec, any_spec, vmem_spec, vmem_spec] + [any_spec] * 7,
            out_specs=(vmem_spec,) * 4 + (any_spec,) * 6,
            scratch_shapes=[pltpu.VMEM((HALVES, m, d_model), BF16), pltpu.VMEM((HALVES, m, d_model), BF16), pltpu.VMEM((total, d_model), BF16),
                            pltpu.VMEM((NUM_DEV, 8, LANES), F32), pltpu.VMEM((HALVES, m, LANES), F32),
                            pltpu.VMEM((exp_loc, d_model, d_ff), BF16), pltpu.VMEM((exp_loc, d_model, d_ff), BF16), pltpu.VMEM((exp_loc, d_ff, d_model), BF16),
                            pltpu.VMEM((HALVES, m, d_model), F32), pltpu.VMEM((HALVES, m, d_model), F32), pltpu.VMEM((total, d_model), F32), pltpu.VMEM((q_dim + 2 * kv_dim, d_model), BF16), pltpu.VMEM((q_dim, d_model), BF16),
                            pltpu.VMEM((m, d_ff), F32), pltpu.VMEM((m, d_ff), F32), pltpu.VMEM((m, d_model), BF16),
                            pltpu.VMEM((HALVES, m, LANES), F32), pltpu.VMEM((HALVES, 2, 8, LANES), F32), pltpu.VMEM((2, 2, m, d_ff), BF16),
                            pltpu.VMEM((m, d_ff), BF16), pltpu.VMEM((2, d_ff, m), BF16), pltpu.VMEM((d_model, total), BF16), pltpu.VMEM((NUM_DEV, HALVES, 8, LANES), F32)]
            + half_shapes() + half_shapes() + scatter_shapes(tok, d_model)
            + [pltpu.SemaphoreType.DMA((NUM_LINKS,)), pltpu.SemaphoreType.DMA((NUM_LINKS,)), pltpu.SemaphoreType.DMA((exp_loc, 3)),
               pltpu.SemaphoreType.DMA((5,)), pltpu.SemaphoreType.DMA((4,)), pltpu.SemaphoreType.DMA((3,)), pltpu.SemaphoreType.DMA((2, 3))],
            compiler_params=pltpu.CompilerParams(collective_id=0, has_side_effects=True, vmem_limit_bytes=67000000),
            name='layer',
        )(x_tokens, dy_tokens, x_attn.reshape(tok, d_model), table, expert_idx.T, w_gate, w_up, w_down, wq, wk, wv, wo)

        width, slots = 512, 4
        steps = d_model // width
        small = (y, dx, attn, dgt)
        dw_gate, dw_up, dw_down, y, dx, attn, dgt = pl.pallas_call(
            functools.partial(weight_grads, width, slots),
            out_shape=(shape((exp_loc, d_model, d_ff), F32), shape((exp_loc, d_model, d_ff), F32), shape((exp_loc, d_ff, d_model), F32)) + tuple(shape(v.shape, v.dtype) for v in small),
            in_specs=[any_spec] * 10,
            out_specs=(any_spec,) * 7,
            scratch_shapes=[pltpu.VMEM((d_model, total), BF16), pltpu.VMEM((total, d_model), BF16), pltpu.VMEM((total, LANES), F32),
                            pltpu.VMEM((exp_loc, total, d_ff), BF16), pltpu.VMEM((exp_loc, total, d_ff), BF16), pltpu.VMEM((exp_loc, d_ff, total), BF16),
                            pltpu.VMEM((slots, width, d_ff), F32), pltpu.VMEM((slots, width, d_ff), F32), pltpu.VMEM((slots, d_ff, width), F32)]
            + [pltpu.VMEM(v.shape, v.dtype) for v in small]
            + [pltpu.SemaphoreType.DMA((steps,)), pltpu.SemaphoreType.DMA((steps,)), pltpu.SemaphoreType.DMA(()), pltpu.SemaphoreType.DMA((exp_loc, 3)),
               pltpu.SemaphoreType.DMA((slots, 3)), pltpu.SemaphoreType.DMA((4, 2))],
            compiler_params=pltpu.CompilerParams(vmem_limit_bytes=66000000),
            name='weight_grads',
        )(xt, dy_all.reshape(total, d_model), gates.reshape(total, LANES), da, db, ht, y, dx, attn, dgt)
        return y, dx, dgt.T, dw_gate, dw_up, dw_down, attn.reshape(x_attn.shape)

    spec_rows = P(TOKEN_AXES, None)
    spec_seqs = P(TOKEN_AXES, None, None)
    spec_experts = P(GROUP_AXES, None, None)
    spec_heads = P(None, GROUP_AXES, None)
    return jax.shard_map(local_step, mesh=mesh,
                         in_specs=(spec_rows, spec_rows, spec_rows, spec_rows, spec_experts, spec_experts, spec_experts, spec_seqs, spec_heads, spec_heads, spec_heads, spec_experts),
                         out_specs=(spec_rows, spec_rows, spec_rows, spec_seqs, spec_seqs, spec_seqs, spec_seqs),
                         check_vma=False)
```

```python
import functools

import jax
import jax.numpy as jnp
from jax import lax
from jax.experimental import pallas as pl
from jax.experimental.pallas import tpu as pltpu
from jax.sharding import PartitionSpec as P

GROUP_AXES = ('ei', 'eo')
TOKEN_AXES = ('dp', 'ei', 'eo')
F32 = jnp.float32
BF16 = jnp.bfloat16
MESH_ID = pl.DeviceIdType.MESH
HALVES = 2
NUM_DEV = 8
LANES = 128


def dot_nn(lhs, rhs):
    return jnp.dot(lhs, rhs, preferred_element_type=F32)


def dot_nt(lhs, rhs):
    return lax.dot_general(lhs, rhs, (((1,), (1,)), ((), ())), preferred_element_type=F32)


def dot_tn(lhs, rhs):
    return lax.dot_general(lhs, rhs, (((0,), (0,)), ((), ())), preferred_element_type=F32)


class Place:
    def __init__(self):
        i = lax.axis_index('ei')
        o = lax.axis_index('eo')
        x = lax.div(o, 2)
        c = lax.rem(o, 2)
        self.core = c
        self.chip = i * 2 + x
        self.dev = {}
        self.block = {}
        self.flat = {}
        self.pair = {}
        self.chips = {}
        for flip_y in (0, 1):
            for flip_x in (0, 1):
                for flip_c in (0, 1):
                    yy = 1 - i if flip_y else i
                    xx = 1 - x if flip_x else x
                    cc = 1 - c if flip_c else c
                    name = ('y' if flip_y else '') + ('x' if flip_x else '') + ('c' if flip_c else '')
                    self.dev[name] = (0, yy, xx * 2 + cc)
                    self.block[name] = cc * 4 + yy * 2 + xx
                    self.flat[name] = yy * 4 + xx * 2 + cc
                    self.pair[name] = (yy * 2 + xx) * 2 + cc
                    self.chips[name] = yy * 2 + xx


class Link:
    def __init__(self, pool, src, dst, land, device):
        send, recv = pool.take()
        self.out = pltpu.make_async_remote_copy(src_ref=src, dst_ref=dst, send_sem=send, recv_sem=recv, device_id=device, device_id_type=MESH_ID)
        self.inn = pltpu.make_async_remote_copy(src_ref=land, dst_ref=land, send_sem=send, recv_sem=recv, device_id=device, device_id_type=MESH_ID)

    def start(self):
        self.out.start()

    def arrive(self):
        self.inn.wait_recv()

    def sent(self):
        self.out.wait_send()


class Pool:
    def __init__(self, sends, recvs):
        self.sends, self.recvs, self.used = sends, recvs, 0

    def take(self):
        k = self.used
        self.used += 1
        return self.sends.at[k], self.recvs.at[k]


class Gather:
    def __init__(self, pool, place, buf, rows, index):
        def at(name, lo=0, n=rows):
            return buf.at[pl.ds(pl.multiple_of(index[name] * rows + lo, 8), n), :]

        half = rows // 2
        own = at('')
        dev = place.dev
        self.to_x = Link(pool, own, own, at('x'), dev['x'])
        self.to_y = Link(pool, own, own, at('y'), dev['y'])
        self.to_c = Link(pool, own, own, at('c'), dev['c'])
        self.relay_x = Link(pool, at('y', 0, half), at('y', 0, half), at('yx', 0, half), dev['x'])
        self.relay_y = Link(pool, at('x', half, half), at('x', half, half), at('yx', half, half), dev['y'])
        self.core_x = Link(pool, at('x'), at('x'), at('xc'), dev['c'])
        self.core_y = Link(pool, at('y'), at('y'), at('yc'), dev['c'])
        self.core_d = Link(pool, at('yx'), at('yx'), at('yxc'), dev['c'])
        self.early = None
        self.links = (self.to_x, self.to_y, self.to_c, self.relay_x, self.relay_y, self.core_x, self.core_y, self.core_d)

    def begin(self):
        self.to_x.start()
        self.to_y.start()
        self.to_c.start()

    def after(self):
        self.early = True
        self.to_x.sent()
        self.to_y.sent()

    def relay(self):
        self.to_y.arrive()
        self.relay_x.start()
        self.to_x.arrive()
        self.relay_y.start()
        self.core_x.start()
        self.core_y.start()

    def last(self):
        self.relay_x.arrive()
        self.relay_y.arrive()
        self.core_d.start()

    def finish(self):
        self.to_c.arrive()
        self.core_x.arrive()
        self.core_y.arrive()
        self.core_d.arrive()

    def drain(self):
        for link in self.links[0 if self.early is None else 2:]:
            link.sent()


class Scatter:
    def __init__(self, pool, place, part, from_core, from_x, from_y, last_x, last_y, rows):
        half = rows // 2
        self.half, self.part, self.rows, self.place = half, part, rows, place
        self.from_core, self.from_x, self.from_y, self.last_x, self.last_y = from_core, from_x, from_y, last_x, last_y
        four = 4 * rows
        self.mine = pl.multiple_of(place.core * four, 8)
        other = part.at[pl.ds(pl.multiple_of((1 - place.core) * four, 8), four), :]
        dev = place.dev
        self.core = Link(pool, other, from_core, from_core, dev['c'])
        self.x0 = Link(pool, self.at('x', 0), from_x.at[0], from_x.at[0], dev['x'])
        self.x1 = Link(pool, self.at('yx', 0), from_x.at[1], from_x.at[1], dev['x'])
        self.y0 = Link(pool, self.at('y', half), from_y.at[0], from_y.at[0], dev['y'])
        self.y1 = Link(pool, self.at('yx', half), from_y.at[1], from_y.at[1], dev['y'])
        self.end_y = Link(pool, self.at('y', 0), last_y, last_y, dev['y'])
        self.end_x = Link(pool, self.at('x', half), last_x, last_x, dev['x'])
        self.links = (self.core, self.x0, self.x1, self.y0, self.y1, self.end_y, self.end_x)

    def at(self, name, lo):
        return self.part.at[pl.ds(pl.multiple_of(self.place.block[name] * self.rows + lo, 8), self.half), :]

    def begin(self):
        self.core.start()

    def middle(self):
        self.core.arrive()
        mine = pl.ds(self.mine, 4 * self.rows)
        self.part[mine, :] = self.part[mine, :] + self.from_core[...]
        self.x1.start()
        self.y1.start()
        self.x0.start()
        self.y0.start()

    def late(self):
        self.x1.arrive()
        here = self.at('y', 0)
        here[...] = here[...] + self.from_x[1]
        self.end_y.start()
        self.y1.arrive()
        here = self.at('x', self.half)
        here[...] = here[...] + self.from_y[1]
        self.end_x.start()

    def finish(self, out):
        half = self.half
        self.x0.arrive()
        self.y0.arrive()
        self.end_y.arrive()
        self.end_x.arrive()
        out[0:half, :] = (self.at('', 0)[...] + self.from_x[0] + self.last_y[...]).astype(BF16)
        out[half:2 * half, :] = (self.at('', half)[...] + self.from_y[0] + self.last_x[...]).astype(BF16)

    def drain(self):
        for link in self.links:
            link.sent()


def scatter_shapes(rows, width):
    half = rows // 2
    return [pltpu.VMEM((4 * rows, width), F32), pltpu.VMEM((2, half, width), F32), pltpu.VMEM((2, half, width), F32),
            pltpu.VMEM((half, width), F32), pltpu.VMEM((half, width), F32)]


NUM_LINKS = 7 + 14 + 8 * 5 + 7 * 5


def attention_pair(xa, wqkv, wo, part, chip, chips, dims):
    seq, kv_dim, heads, head_dim = dims
    q_dim = heads * head_dim
    pair = 2 * seq
    rows = pl.ds(pl.multiple_of(chip * pair, pair), pair)
    row = lax.broadcasted_iota(jnp.int32, (pair, pair), 0)
    col = lax.broadcasted_iota(jnp.int32, (pair, pair), 1)
    causal = (row >= col) & ((row >= seq) == (col >= seq))
    qkv = dot_nt(xa[rows, :], wqkv[...]).astype(BF16)
    keys = qkv[:, q_dim:q_dim + kv_dim]
    vals = qkv[:, q_dim + kv_dim:q_dim + 2 * kv_dim]
    outs = []
    for h in range(heads):
        scores = dot_nt(qkv[:, h * head_dim:(h + 1) * head_dim], keys) * head_dim ** -0.5
        scores = jnp.where(causal, scores, -1e30)
        top = jnp.max(scores, axis=1, keepdims=True)
        ex = jnp.exp(scores - top)
        probs = (ex / jnp.sum(ex, axis=1, keepdims=True)).astype(BF16)
        outs.append(dot_nn(probs, vals).astype(BF16))
    out = dot_nn(jnp.concatenate(outs, axis=1), wo[...])
    for c in range(2):
        part[pl.ds(pl.multiple_of((c * chips + chip) * seq, seq), seq), :] = out[c * seq:(c + 1) * seq, :]


def make_layer_kernel(tok, d_model, d_ff, exp_loc, attn_dims):
    r = tok // HALVES
    m = r * NUM_DEV
    tile = 512

    def kernel(x_in, dy_in, xa_in, gt_in, idx_in, wg_in, wu_in, wd_in, wq_in, wk_in, wv_in, wo_in,
               y_out, dx_out, attn_out, dg_out, xt_all, dy_all, da_all, db_all, ht_all, gates_out,
               xb, dyb, xab, gtb, gcol, wg, wu, wd, y_part, dx_part, at_part, wqkv, wo, s1, s2, d_o, dgc, dgt, stage, hid, stage_t, xt, dgl,
               ry0, ry1, ry2, ry3, ry4, rd0, rd1, rd2, rd3, rd4, ra0, ra1, ra2, ra3, ra4,
               send_sems, recv_sems, w_sems, in_sems, aw_sems, out_sems, stage_sems):
        place = Place()
        pool = Pool(send_sems, recv_sems)
        dev, block = place.dev, place.block
        me = block['']

        def own_rows(buf, rows, index=me):
            return buf.at[pl.ds(pl.multiple_of(index * rows, 8), rows), :]

        loads = []
        for h in range(HALVES):
            loads.append(pltpu.make_async_copy(x_in.at[h * r:(h + 1) * r, :], own_rows(xb.at[h], r), in_sems.at[h]))
            loads.append(pltpu.make_async_copy(dy_in.at[h * r:(h + 1) * r, :], own_rows(dyb.at[h], r), in_sems.at[2 + h]))
        loads.append(pltpu.make_async_copy(xa_in, own_rows(xab, tok, place.pair['']), in_sems.at[4]))
        for load in loads:
            load.start()
        q_dim, kv_dim = wq_in.shape[0], wk_in.shape[0]
        attn_loads = [pltpu.make_async_copy(wq_in, wqkv.at[0:q_dim, :], aw_sems.at[0]), pltpu.make_async_copy(wk_in, wqkv.at[q_dim:q_dim + kv_dim, :], aw_sems.at[1]),
                      pltpu.make_async_copy(wv_in, wqkv.at[q_dim + kv_dim:q_dim + 2 * kv_dim, :], aw_sems.at[2]), pltpu.make_async_copy(wo_in, wo, aw_sems.at[3])]
        for load in attn_loads:
            load.start()
        weights = []
        for e in range(exp_loc):
            weights.append([pltpu.make_async_copy(src.at[e], dst.at[e], w_sems.at[e, k]) for k, (src, dst) in enumerate(((wg_in, wg), (wu_in, wu), (wd_in, wd)))])
        barrier = pltpu.get_barrier_semaphore()
        peers = [name for name in dev if name]
        for name in peers:
            pl.semaphore_signal(barrier, inc=1, device_id=dev[name], device_id_type=MESH_ID)
        pl.semaphore_wait(barrier, len(peers))

        routes = [Link(pool, gt_in.at[place.flat[name]], gtb.at[me], gtb.at[block[name]], dev[name]) for name in peers]
        gx = [Gather(pool, place, xb.at[h], r, block) for h in range(HALVES)]
        gdy = [Gather(pool, place, dyb.at[h], r, block) for h in range(HALVES)]
        gxa = Gather(pool, place, xab, tok, place.pair)
        sy = [Scatter(pool, place, y_part.at[h], ry0.at[h], ry1.at[h], ry2.at[h], ry3.at[h], ry4.at[h], r) for h in range(HALVES)]
        sdx = [Scatter(pool, place, dx_part.at[h], rd0.at[h], rd1.at[h], rd2.at[h], rd3.at[h], rd4.at[h], r) for h in range(HALVES)]
        sat = Scatter(pool, place, at_part, ra0, ra1, ra2, ra3, ra4, tok)
        dg_links = [[Link(pool, dgt.at[h, 1 - place.core if 'c' in name else place.core], dgl.at[me, h], dgl.at[block[name], h], dev[name]) for name in peers] for h in range(HALVES)]

        for load in loads:
            load.wait()
        gxa.begin()
        for link in routes:
            link.start()
        gtb[me] = gt_in[place.flat['']]
        for ws in weights:
            for w in ws:
                w.start()
        dgc[...] = jnp.zeros_like(dgc)
        gcol[...] = jnp.zeros_like(gcol)
        y_part[...] = jnp.zeros_like(y_part)
        dx_part[...] = jnp.zeros_like(dx_part)
        for load in attn_loads:
            load.wait()

        def pair(name):
            attention_pair(xab, wqkv, wo, at_part, place.chips[name], NUM_DEV // 2, attn_dims)

        gxa.to_c.arrive()
        pair('')
        gxa.after()
        gx[0].begin()
        gxa.relay()
        gdy[0].begin()
        gxa.core_x.arrive()
        pair('x')
        gx[0].relay()
        gxa.core_y.arrive()
        pair('y')
        gx[1].begin()
        gxa.last()
        gdy[0].relay()
        gdy[1].begin()
        gx[0].last()
        gxa.core_d.arrive()
        pair('yx')
        sat.begin()
        for link in routes:
            link.arrive()
        wide = jnp.concatenate([gtb[...].reshape(NUM_DEV * 8, LANES), jnp.zeros((LANES - NUM_DEV * 8, LANES), F32)], axis=0).T
        for h in range(HALVES):
            for b in range(NUM_DEV):
                gcol[h, b * r:(b + 1) * r, 0:8] = wide[h * r:(h + 1) * r, b * 8:(b + 1) * 8]
        gdy[0].last()
        gx[0].finish()
        gdy[0].finish()

        def staged(h, e, k):
            slot = h * 2 + lax.rem(e, 2)
            part = pl.ds(h * m, m)
            if k == 2:
                return pltpu.make_async_copy(stage_t.at[slot], ht_all.at[e, :, part], stage_sems.at[slot, k])
            return pltpu.make_async_copy(stage.at[slot, k], (da_all, db_all)[k].at[e, part, :], stage_sems.at[slot, k])

        lane = lax.broadcasted_iota(jnp.int32, (m, LANES), 1)

        def gate_of(h, e):
            return jnp.sum(jnp.where(lane == e, gcol[h], 0.0), axis=1, keepdims=True)

        def phase(h, events, step, kinds):
            def body(e, _):
                for k, event in events.items():
                    pl.when(e == k)(event)

                @pl.when(e >= 2)
                def _():
                    for k in kinds:
                        staged(h, e - 2, k).wait()

                step(h, e)
                for k in kinds:
                    staged(h, e, k).start()
                return 0

            lax.fori_loop(0, exp_loc, body, 0)

        def forward(h, e):
            if h == 0:
                for k, (src, dst) in enumerate(((wg_in, wg), (wu_in, wu), (wd_in, wd))):
                    pltpu.make_async_copy(src.at[e], dst.at[e], w_sems.at[e, k]).wait()
            gate = gate_of(h, e)
            mask = gate > 0.0
            a = jnp.where(mask, dot_nn(xb[h], wg[e]), 0.0)
            b = jnp.where(mask, dot_nn(xb[h], wu[e]), 0.0)
            sig = jax.nn.sigmoid(a)
            act = a * sig
            hid[...] = (act * b).astype(BF16)
            stage_t[h * 2 + lax.rem(e, 2)] = hid[...].T
            s1[e] = b * sig * (1.0 + a * (1.0 - sig))
            s2[e] = act
            dots = jnp.zeros((m, LANES), F32)
            for n in range(d_model // tile):
                cols = pl.ds(n * tile, tile)
                o = dot_nn(hid[...], wd[e, :, cols]).astype(BF16).astype(F32)
                y_part[h, :, cols] += gate * o
                prod = dyb[h, :, cols].astype(F32) * o
                for k in range(tile // LANES):
                    dots += prod[:, k * LANES:(k + 1) * LANES]
            dgc[h] = jnp.where(lane == e, jnp.sum(dots, axis=1, keepdims=True), dgc[h])

        def backward(h, e):
            slot = h * 2 + lax.rem(e, 2)
            gate = gate_of(h, e)
            for n in range(d_model // tile):
                cols = pl.ds(n * tile, tile)
                d_o[:, cols] = (gate * dyb[h, :, cols].astype(F32)).astype(BF16)
            dh = dot_nt(d_o[...], wd[e]).astype(BF16).astype(F32)
            stage[slot, 0] = (dh * s1[e]).astype(BF16)
            stage[slot, 1] = (dh * s2[e]).astype(BF16)
            for n in range(d_model // tile):
                cols = pl.ds(n * tile, tile)
                dxe = dot_nt(stage[slot, 0], wg[e, cols, :]) + dot_nt(stage[slot, 1], wu[e, cols, :])
                dx_part[h, :, cols] += dxe.astype(BF16).astype(F32)

        def send_dg(h):
            turned = dgc[h].T
            for c in range(2):
                dgt[h, c] = turned[0:8, c * LANES:(c + 1) * LANES]
            for link in dg_links[h]:
                link.start()
            dgl[me, h] = dgt[h, place.core]

        def fa1():
            gx[1].relay()
            sat.middle()

        def fa2():
            gdy[1].relay()

        def fa3():
            gx[1].last()

        phase(0, {1: fa1, 2: fa2, 3: fa3}, forward, (2,))
        sy[0].begin()
        send_dg(0)
        gx[1].finish()

        def ba1():
            gdy[1].last()
            sy[0].middle()

        def ba2():
            sat.late()

        phase(0, {1: ba1, 2: ba2}, backward, (0, 1))
        gdy[1].finish()
        sdx[0].begin()

        def fb1():
            sdx[0].middle()
            sy[0].late()

        def fb2():
            sat.finish(attn_out)

        phase(1, {1: fb1, 2: fb2}, forward, (2,))
        sy[1].begin()
        send_dg(1)

        def bb1():
            sy[1].middle()
            sdx[0].late()

        def bb3():
            sy[0].finish(y_out.at[0:r, :])

        phase(1, {1: bb1, 3: bb3}, backward, (0, 1))
        sdx[1].begin()
        sy[1].late()
        for h in range(HALVES):
            xt[:, h * m:(h + 1) * m] = xb[h].T
        sdx[1].middle()
        saves = [pltpu.make_async_copy(xt, xt_all, out_sems.at[0]), pltpu.make_async_copy(dyb, dy_all, out_sems.at[1]), pltpu.make_async_copy(gcol, gates_out, out_sems.at[2])]
        for save in saves:
            save.start()
        sdx[0].finish(dx_out.at[0:r, :])
        for h in range(HALVES):
            for link in dg_links[h]:
                link.arrive()
        for h in range(HALVES):
            slots = idx_in[:, h * r:(h + 1) * r]
            total = jnp.zeros(slots.shape, F32)
            for b in range(NUM_DEV):
                first = ((b // 2) % 2 * 4 + b % 2 * 2 + b // 4) * exp_loc
                rows = dgl[b, h]
                mine = jnp.zeros((8, r), F32)
                for q in range(LANES // r):
                    mine = jnp.where(place.chip == q, rows[:, q * r:(q + 1) * r], mine)
                for e in range(exp_loc):
                    total = jnp.where(slots == first + e, mine[e:e + 1, :], total)
            dg_out[:, h * r:(h + 1) * r] = total
        sdx[1].late()
        for s, out in ((sy[1], y_out), (sdx[1], dx_out)):
            s.finish(out.at[r:2 * r, :])
        for save in saves:
            save.wait()
        for h in range(HALVES):
            for e in (exp_loc - 2, exp_loc - 1):
                for k in range(3):
                    staged(h, jnp.int32(e), k).wait()
        for item in gx + gdy + [gxa] + sy + sdx + [sat]:
            item.drain()
        for link in routes + dg_links[0] + dg_links[1]:
            link.sent()
        assert pool.used == NUM_LINKS

    return kernel, r, m


def weight_grads(width, slots, xt_in, dy_in, g_in, da_in, db_in, ht_in, y_in, dx_in, at_in, dg_in,
                 dwg, dwu, dwd, y_out, dx_out, at_out, dg_out,
                 xt, dy, g, da, db, ht, sg, su, sd, y, dx, at, dg, x_sems, d_sems, g_sem, e_sems, o_sems, p_sems):
    exp_loc = da.shape[0]
    steps = dy.shape[1] // width

    def load(e, k):
        src, dst = ((da_in, da), (db_in, db), (ht_in, ht))[k]
        return pltpu.make_async_copy(src.at[e], dst.at[e], e_sems.at[e, k])

    def x_load(n):
        rows = slice(n * width, (n + 1) * width)
        return pltpu.make_async_copy(xt_in.at[rows, :], xt.at[rows, :], x_sems.at[n])

    def dy_load(n):
        cols = slice(n * width, (n + 1) * width)
        return pltpu.make_async_copy(dy_in.at[:, cols], dy.at[:, cols], d_sems.at[n])

    g_load = pltpu.make_async_copy(g_in, g, g_sem)
    for copy in (x_load(0), load(0, 0), load(0, 1), load(0, 2), dy_load(0), g_load):
        copy.start()
    for n in range(1, steps):
        x_load(n).start()
        dy_load(n).start()
    for e in range(1, exp_loc):
        for k in range(3):
            load(e, k).start()
    passing = ((y_in, y, y_out), (dx_in, dx, dx_out), (at_in, at, at_out), (dg_in, dg, dg_out))
    take = [pltpu.make_async_copy(src, mid, p_sems.at[k, 0]) for k, (src, mid, _) in enumerate(passing)]
    give = [pltpu.make_async_copy(mid, dst, p_sems.at[k, 1]) for k, (_, mid, dst) in enumerate(passing)]
    for copy in take:
        copy.start()

    def store(s, k):
        e, n = lax.div(s, steps), lax.rem(s, steps)
        slot = lax.rem(s, slots)
        part = pl.ds(pl.multiple_of(n * width, LANES), width)
        if k == 2:
            return pltpu.make_async_copy(sd.at[slot], dwd.at[e, :, part], o_sems.at[slot, k])
        return pltpu.make_async_copy((sg, su)[k].at[slot], (dwg, dwu)[k].at[e, part, :], o_sems.at[slot, k])

    lane = lax.broadcasted_iota(jnp.int32, g.shape, 1)

    def step(s, _):
        e, n = lax.div(s, steps), lax.rem(s, steps)
        slot = lax.rem(s, slots)
        for k in range(steps):
            @pl.when(s == k)
            def _():
                x_load(k).wait()

        @pl.when(n == 0)
        def _():
            load(e, 0).wait()
            load(e, 1).wait()

        @pl.when(s >= slots)
        def _():
            for k in range(3):
                store(s - slots, k).wait()

        part = pl.ds(pl.multiple_of(n * width, LANES), width)
        sg[slot] = dot_nn(xt[part, :], da[e])
        store(s, 0).start()
        su[slot] = dot_nn(xt[part, :], db[e])
        store(s, 1).start()

        @pl.when(n == 0)
        def _():
            load(e, 2).wait()

        @pl.when(s == 0)
        def _():
            g_load.wait()

        @pl.when(s == 3)
        def _():
            for copy in take:
                copy.wait()
            for copy in give:
                copy.start()

        for k in range(steps):
            @pl.when(s == k)
            def _():
                dy_load(k).wait()

        gate = jnp.sum(jnp.where(lane == e, g[...], 0.0), axis=1, keepdims=True)
        d_o = (gate * dy[:, part].astype(F32)).astype(BF16)
        sd[slot] = dot_nn(ht[e], d_o)
        store(s, 2).start()
        return 0

    lax.fori_loop(0, exp_loc * steps, step, 0)
    for s in range(exp_loc * steps - slots, exp_loc * steps):
        for k in range(3):
            store(jnp.int32(s), k).wait()
    for copy in give:
        copy.wait()


def solution(mesh):
    num_dev = mesh.shape['ei'] * mesh.shape['eo']
    assert num_dev == NUM_DEV

    def local_step(x_tokens, expert_idx, gate_vals, dy_tokens, w_gate, w_up, w_down, x_attn, w_query, w_key, w_value, w_out):
        tok, d_model = x_tokens.shape
        top_k = expert_idx.shape[1]
        exp_loc, _, d_ff = w_gate.shape
        seq = x_attn.shape[1]
        heads, head_dim = w_query.shape[1], w_query.shape[2]
        kv_dim = w_key.shape[1] * head_dim
        q_dim = heads * head_dim
        ids = jnp.arange(NUM_DEV * exp_loc, dtype=jnp.int32).reshape(NUM_DEV, exp_loc, 1, 1)
        table = jnp.sum(jnp.where(expert_idx.T[None, None] == ids, gate_vals.T[None, None], 0.0), axis=2)
        table = jnp.pad(table, ((0, 0), (0, 8 - exp_loc), (0, LANES - tok)))
        wq = w_query.transpose(1, 2, 0).reshape(q_dim, d_model)
        wk = w_key.transpose(1, 2, 0).reshape(kv_dim, d_model)
        wv = w_value.transpose(1, 2, 0).reshape(kv_dim, d_model)
        wo = w_out.reshape(q_dim, d_model)
        kernel, r, m = make_layer_kernel(tok, d_model, d_ff, exp_loc, (seq, kv_dim, heads, head_dim))
        any_spec = pl.BlockSpec(memory_space=pl.ANY)
        vmem_spec = pl.BlockSpec(memory_space=pltpu.VMEM)
        shape = jax.ShapeDtypeStruct
        total = tok * NUM_DEV

        def half_shapes():
            return [pltpu.VMEM((HALVES,) + s.shape, s.dtype) for s in scatter_shapes(r, d_model)]

        y, dx, attn, dgt, xt, dy_all, da, db, ht, gates = pl.pallas_call(
            kernel,
            out_shape=(shape((tok, d_model), BF16), shape((tok, d_model), BF16), shape((tok, d_model), BF16), shape((top_k, tok), F32),
                       shape((d_model, total), BF16), shape((HALVES, m, d_model), BF16),
                       shape((exp_loc, total, d_ff), BF16), shape((exp_loc, total, d_ff), BF16), shape((exp_loc, d_ff, total), BF16), shape((HALVES, m, LANES), F32)),
            in_specs=[any_spec, any_spec, any_spec, vmem_spec, vmem_spec] + [any_spec] * 7,
            out_specs=(vmem_spec,) * 4 + (any_spec,) * 6,
            scratch_shapes=[pltpu.VMEM((HALVES, m, d_model), BF16), pltpu.VMEM((HALVES, m, d_model), BF16), pltpu.VMEM((total, d_model), BF16),
                            pltpu.VMEM((NUM_DEV, 8, LANES), F32), pltpu.VMEM((HALVES, m, LANES), F32),
                            pltpu.VMEM((exp_loc, d_model, d_ff), BF16), pltpu.VMEM((exp_loc, d_model, d_ff), BF16), pltpu.VMEM((exp_loc, d_ff, d_model), BF16),
                            pltpu.VMEM((HALVES, m, d_model), F32), pltpu.VMEM((HALVES, m, d_model), F32), pltpu.VMEM((total, d_model), F32), pltpu.VMEM((q_dim + 2 * kv_dim, d_model), BF16), pltpu.VMEM((q_dim, d_model), BF16),
                            pltpu.VMEM((exp_loc, m, d_ff), F32), pltpu.VMEM((exp_loc, m, d_ff), F32), pltpu.VMEM((m, d_model), BF16),
                            pltpu.VMEM((HALVES, m, LANES), F32), pltpu.VMEM((HALVES, 2, 8, LANES), F32), pltpu.VMEM((2 * HALVES, 2, m, d_ff), BF16),
                            pltpu.VMEM((m, d_ff), BF16), pltpu.VMEM((2 * HALVES, d_ff, m), BF16), pltpu.VMEM((d_model, total), BF16), pltpu.VMEM((NUM_DEV, HALVES, 8, LANES), F32)]
            + half_shapes() + half_shapes() + scatter_shapes(tok, d_model)
            + [pltpu.SemaphoreType.DMA((NUM_LINKS,)), pltpu.SemaphoreType.DMA((NUM_LINKS,)), pltpu.SemaphoreType.DMA((exp_loc, 3)),
               pltpu.SemaphoreType.DMA((5,)), pltpu.SemaphoreType.DMA((4,)), pltpu.SemaphoreType.DMA((3,)), pltpu.SemaphoreType.DMA((2 * HALVES, 3))],
            compiler_params=pltpu.CompilerParams(collective_id=0, has_side_effects=True, vmem_limit_bytes=67000000),
            name='layer',
        )(x_tokens, dy_tokens, x_attn.reshape(tok, d_model), table, expert_idx.T, w_gate, w_up, w_down, wq, wk, wv, wo)

        width, slots = 512, 4
        steps = d_model // width
        small = (y, dx, attn, dgt)
        dw_gate, dw_up, dw_down, y, dx, attn, dgt = pl.pallas_call(
            functools.partial(weight_grads, width, slots),
            out_shape=(shape((exp_loc, d_model, d_ff), F32), shape((exp_loc, d_model, d_ff), F32), shape((exp_loc, d_ff, d_model), F32)) + tuple(shape(v.shape, v.dtype) for v in small),
            in_specs=[any_spec] * 10,
            out_specs=(any_spec,) * 7,
            scratch_shapes=[pltpu.VMEM((d_model, total), BF16), pltpu.VMEM((total, d_model), BF16), pltpu.VMEM((total, LANES), F32),
                            pltpu.VMEM((exp_loc, total, d_ff), BF16), pltpu.VMEM((exp_loc, total, d_ff), BF16), pltpu.VMEM((exp_loc, d_ff, total), BF16),
                            pltpu.VMEM((slots, width, d_ff), F32), pltpu.VMEM((slots, width, d_ff), F32), pltpu.VMEM((slots, d_ff, width), F32)]
            + [pltpu.VMEM(v.shape, v.dtype) for v in small]
            + [pltpu.SemaphoreType.DMA((steps,)), pltpu.SemaphoreType.DMA((steps,)), pltpu.SemaphoreType.DMA(()), pltpu.SemaphoreType.DMA((exp_loc, 3)),
               pltpu.SemaphoreType.DMA((slots, 3)), pltpu.SemaphoreType.DMA((4, 2))],
            compiler_params=pltpu.CompilerParams(vmem_limit_bytes=66000000),
            name='weight_grads',
        )(xt, dy_all.reshape(total, d_model), gates.reshape(total, LANES), da, db, ht, y, dx, attn, dgt)
        return y, dx, dgt.T, dw_gate, dw_up, dw_down, attn.reshape(x_attn.shape)

    spec_rows = P(TOKEN_AXES, None)
    spec_seqs = P(TOKEN_AXES, None, None)
    spec_experts = P(GROUP_AXES, None, None)
    spec_heads = P(None, GROUP_AXES, None)
    return jax.shard_map(local_step, mesh=mesh,
                         in_specs=(spec_rows, spec_rows, spec_rows, spec_rows, spec_experts, spec_experts, spec_experts, spec_seqs, spec_heads, spec_heads, spec_heads, spec_experts),
                         out_specs=(spec_rows, spec_rows, spec_rows, spec_seqs, spec_seqs, spec_seqs, spec_seqs),
                         check_vma=False)
```

```python
import functools

import jax
import jax.numpy as jnp
from jax import lax
from jax.experimental import pallas as pl
from jax.experimental.pallas import tpu as pltpu
from jax.sharding import PartitionSpec as P

GROUP_AXES = ('ei', 'eo')
TOKEN_AXES = ('dp', 'ei', 'eo')
F32 = jnp.float32
BF16 = jnp.bfloat16
MESH_ID = pl.DeviceIdType.MESH
HALVES = 2
NUM_DEV = 8
LANES = 128


def dot_nn(lhs, rhs):
    return jnp.dot(lhs, rhs, preferred_element_type=F32)


def dot_nt(lhs, rhs):
    return lax.dot_general(lhs, rhs, (((1,), (1,)), ((), ())), preferred_element_type=F32)


def dot_tn(lhs, rhs):
    return lax.dot_general(lhs, rhs, (((0,), (0,)), ((), ())), preferred_element_type=F32)


class Place:
    def __init__(self):
        i = lax.axis_index('ei')
        o = lax.axis_index('eo')
        x = lax.div(o, 2)
        c = lax.rem(o, 2)
        self.core = c
        self.chip = i * 2 + x
        self.dev = {}
        self.block = {}
        self.flat = {}
        self.pair = {}
        self.chips = {}
        for flip_y in (0, 1):
            for flip_x in (0, 1):
                for flip_c in (0, 1):
                    yy = 1 - i if flip_y else i
                    xx = 1 - x if flip_x else x
                    cc = 1 - c if flip_c else c
                    name = ('y' if flip_y else '') + ('x' if flip_x else '') + ('c' if flip_c else '')
                    self.dev[name] = (0, yy, xx * 2 + cc)
                    self.block[name] = cc * 4 + yy * 2 + xx
                    self.flat[name] = yy * 4 + xx * 2 + cc
                    self.pair[name] = (yy * 2 + xx) * 2 + cc
                    self.chips[name] = yy * 2 + xx


class Link:
    def __init__(self, pool, src, dst, land, device):
        send, recv = pool.take()
        self.out = pltpu.make_async_remote_copy(src_ref=src, dst_ref=dst, send_sem=send, recv_sem=recv, device_id=device, device_id_type=MESH_ID)
        self.inn = pltpu.make_async_remote_copy(src_ref=land, dst_ref=land, send_sem=send, recv_sem=recv, device_id=device, device_id_type=MESH_ID)

    def start(self):
        self.out.start()

    def arrive(self):
        self.inn.wait_recv()

    def sent(self):
        self.out.wait_send()


class Pool:
    def __init__(self, sends, recvs):
        self.sends, self.recvs, self.used = sends, recvs, 0

    def take(self):
        k = self.used
        self.used += 1
        return self.sends.at[k], self.recvs.at[k]


class Gather:
    def __init__(self, pool, place, buf, rows, index):
        def at(name, lo=0, n=rows):
            return buf.at[pl.ds(pl.multiple_of(index[name] * rows + lo, 8), n), :]

        half = rows // 2
        own = at('')
        dev = place.dev
        self.to_x = Link(pool, own, own, at('x'), dev['x'])
        self.to_y = Link(pool, own, own, at('y'), dev['y'])
        self.to_c = Link(pool, own, own, at('c'), dev['c'])
        self.relay_x = Link(pool, at('y', 0, half), at('y', 0, half), at('yx', 0, half), dev['x'])
        self.relay_y = Link(pool, at('x', half, half), at('x', half, half), at('yx', half, half), dev['y'])
        self.core_x = Link(pool, at('x'), at('x'), at('xc'), dev['c'])
        self.core_y = Link(pool, at('y'), at('y'), at('yc'), dev['c'])
        self.core_d = Link(pool, at('yx'), at('yx'), at('yxc'), dev['c'])
        self.early = None
        self.links = (self.to_x, self.to_y, self.to_c, self.relay_x, self.relay_y, self.core_x, self.core_y, self.core_d)

    def begin(self):
        self.to_x.start()
        self.to_y.start()
        self.to_c.start()

    def after(self):
        self.early = True
        self.to_x.sent()
        self.to_y.sent()

    def relay(self):
        self.to_y.arrive()
        self.relay_x.start()
        self.to_x.arrive()
        self.relay_y.start()
        self.core_x.start()
        self.core_y.start()

    def last(self):
        self.relay_x.arrive()
        self.relay_y.arrive()
        self.core_d.start()

    def finish(self):
        self.to_c.arrive()
        self.core_x.arrive()
        self.core_y.arrive()
        self.core_d.arrive()

    def drain(self):
        for link in self.links[0 if self.early is None else 2:]:
            link.sent()


class Scatter:
    def __init__(self, pool, place, part, from_core, from_x, from_y, last_x, last_y, rows, first=0):
        half = rows // 2
        self.half, self.part, self.rows, self.place = half, part, rows, place
        self.from_core, self.from_x, self.from_y, self.last_x, self.last_y = from_core, from_x, from_y, last_x, last_y
        four = 4 * rows
        self.mine = pl.multiple_of(place.core * four, 8)
        self.cols = pl.ds(first, from_core.shape[-1])
        other = part.at[pl.ds(pl.multiple_of((1 - place.core) * four, 8), four), self.cols]
        dev = place.dev
        self.core = Link(pool, other, from_core, from_core, dev['c'])
        self.x0 = Link(pool, self.at('x', 0), from_x.at[0], from_x.at[0], dev['x'])
        self.x1 = Link(pool, self.at('yx', 0), from_x.at[1], from_x.at[1], dev['x'])
        self.y0 = Link(pool, self.at('y', half), from_y.at[0], from_y.at[0], dev['y'])
        self.y1 = Link(pool, self.at('yx', half), from_y.at[1], from_y.at[1], dev['y'])
        self.end_y = Link(pool, self.at('y', 0), last_y, last_y, dev['y'])
        self.end_x = Link(pool, self.at('x', half), last_x, last_x, dev['x'])
        self.links = (self.core, self.x0, self.x1, self.y0, self.y1, self.end_y, self.end_x)

    def at(self, name, lo):
        return self.part.at[pl.ds(pl.multiple_of(self.place.block[name] * self.rows + lo, 8), self.half), self.cols]

    def begin(self):
        self.core.start()

    def middle(self):
        self.core.arrive()
        mine = pl.ds(self.mine, 4 * self.rows)
        self.part[mine, self.cols] = self.part[mine, self.cols] + self.from_core[...]
        self.x1.start()
        self.y1.start()
        self.x0.start()
        self.y0.start()

    def late(self):
        self.x1.arrive()
        here = self.at('y', 0)
        here[...] = here[...] + self.from_x[1]
        self.end_y.start()
        self.y1.arrive()
        here = self.at('x', self.half)
        here[...] = here[...] + self.from_y[1]
        self.end_x.start()

    def finish(self, out, row=0):
        half = self.half
        self.x0.arrive()
        self.y0.arrive()
        self.end_y.arrive()
        self.end_x.arrive()
        out[row:row + half, self.cols] = (self.at('', 0)[...] + self.from_x[0] + self.last_y[...]).astype(BF16)
        out[row + half:row + 2 * half, self.cols] = (self.at('', half)[...] + self.from_y[0] + self.last_x[...]).astype(BF16)

    def drain(self):
        for link in self.links:
            link.sent()


def scatter_shapes(rows, width):
    half = rows // 2
    return [pltpu.VMEM((4 * rows, width), F32), pltpu.VMEM((2, half, width), F32), pltpu.VMEM((2, half, width), F32),
            pltpu.VMEM((half, width), F32), pltpu.VMEM((half, width), F32)]


NUM_LINKS = 7 + 14 + 8 * 5 + 7 * 13


def attention_qkv(xa, wqkv, qkv, chip, seq):
    pair = 2 * seq
    qkv[...] = dot_nt(xa[pl.ds(pl.multiple_of(chip * pair, pair), pair), :], wqkv[...]).astype(BF16)


def attention_out(qkv, wo, part, chip, chips, dims):
    seq, kv_dim, heads, head_dim = dims
    q_dim = heads * head_dim
    pair = 2 * seq
    row = lax.broadcasted_iota(jnp.int32, (pair, pair), 0)
    col = lax.broadcasted_iota(jnp.int32, (pair, pair), 1)
    causal = (row >= col) & ((row >= seq) == (col >= seq))
    keys = qkv[:, q_dim:q_dim + kv_dim]
    vals = qkv[:, q_dim + kv_dim:q_dim + 2 * kv_dim]
    outs = []
    for h in range(heads):
        scores = dot_nt(qkv[:, h * head_dim:(h + 1) * head_dim], keys) * head_dim ** -0.5
        scores = jnp.where(causal, scores, -1e30)
        top = jnp.max(scores, axis=1, keepdims=True)
        ex = jnp.exp(scores - top)
        probs = (ex / jnp.sum(ex, axis=1, keepdims=True)).astype(BF16)
        outs.append(dot_nn(probs, vals).astype(BF16))
    out = dot_nn(jnp.concatenate(outs, axis=1), wo[...])
    for c in range(2):
        part[pl.ds(pl.multiple_of((c * chips + chip) * seq, seq), seq), :] = out[c * seq:(c + 1) * seq, :]


def make_layer_kernel(tok, d_model, d_ff, exp_loc, attn_dims):
    r = tok // HALVES
    m = r * NUM_DEV
    tile = 512
    tiles = d_model // tile

    def kernel(x_in, dy_in, xa_in, idx_in, gate_in, wg_in, wu_in, wd_in, wq_in, wk_in, wv_in, wo_in,
               y_out, dx_out, attn_out, dg_out, xt_all, dy_all, da_all, db_all, ht_all, gates_out,
               xb, dyb, xab, gtb, gcol, wg, wu, wd, y_part, dx_part, at_part, wqkv, wo, qkv, s1, s2, d_o, dgc, dgt, da, db, hid, stage_t, xt, dgl, gtab, gfull,
               ry0, ry1, ry2, ry3, ry4, rd0, rd1, rd2, rd3, rd4, ra0, ra1, ra2, ra3, ra4,
               send_sems, recv_sems, w_sems, in_sems, aw_sems, out_sems, stage_sems, grad_sems):
        place = Place()
        pool = Pool(send_sems, recv_sems)
        dev, block = place.dev, place.block
        me = block['']

        def own_rows(buf, rows, index=me):
            return buf.at[pl.ds(pl.multiple_of(index * rows, 8), rows), :]

        loads = []
        for h in range(HALVES):
            loads.append(pltpu.make_async_copy(x_in.at[h * r:(h + 1) * r, :], own_rows(xb.at[h], r), in_sems.at[h]))
            loads.append(pltpu.make_async_copy(dy_in.at[h * r:(h + 1) * r, :], own_rows(dyb.at[h], r), in_sems.at[2 + h]))
        loads.append(pltpu.make_async_copy(xa_in, own_rows(xab, tok, place.pair['']), in_sems.at[4]))
        for load in loads:
            load.start()
        q_dim, kv_dim = wq_in.shape[0], wk_in.shape[0]
        attn_loads = [pltpu.make_async_copy(wq_in, wqkv.at[0:q_dim, :], aw_sems.at[0]), pltpu.make_async_copy(wk_in, wqkv.at[q_dim:q_dim + kv_dim, :], aw_sems.at[1]),
                      pltpu.make_async_copy(wv_in, wqkv.at[q_dim + kv_dim:q_dim + 2 * kv_dim, :], aw_sems.at[2]), pltpu.make_async_copy(wo_in, wo, aw_sems.at[3])]
        for load in attn_loads:
            load.start()
        weights = []
        for e in range(exp_loc):
            weights.append([pltpu.make_async_copy(src.at[e], dst.at[e], w_sems.at[e, k]) for k, (src, dst) in enumerate(((wg_in, wg), (wu_in, wu), (wd_in, wd)))])
        barrier = pltpu.get_barrier_semaphore()
        peers = [name for name in dev if name]
        for name in peers:
            pl.semaphore_signal(barrier, inc=1, device_id=dev[name], device_id_type=MESH_ID)
        gtab[...] = jnp.zeros_like(gtab)
        for g in range(NUM_DEV):
            for e in range(exp_loc):
                gtab[g, e:e + 1, 0:tok] = jnp.sum(jnp.where(idx_in[...] == g * exp_loc + e, gate_in[...], 0.0), axis=0, keepdims=True)
        pl.semaphore_wait(barrier, len(peers))

        routes = [Link(pool, gtab.at[place.flat[name]], gtb.at[me], gtb.at[block[name]], dev[name]) for name in peers]
        gx = [Gather(pool, place, xb.at[h], r, block) for h in range(HALVES)]
        gdy = [Gather(pool, place, dyb.at[h], r, block) for h in range(HALVES)]
        gxa = Gather(pool, place, xab, tok, place.pair)
        sy = [[Scatter(pool, place, y_part.at[h], ry0.at[h, n], ry1.at[h, n], ry2.at[h, n], ry3.at[h, n], ry4.at[h, n], r, n * tile) for n in range(tiles)] for h in range(HALVES)]
        sdx = [[Scatter(pool, place, dx_part.at[h], rd0.at[h, n], rd1.at[h, n], rd2.at[h, n], rd3.at[h, n], rd4.at[h, n], r, n * tile) for n in range(tiles)] for h in range(HALVES)]
        sat = Scatter(pool, place, at_part, ra0, ra1, ra2, ra3, ra4, tok)
        dg_links = [[Link(pool, dgt.at[h, 1 - place.core if 'c' in name else place.core], dgl.at[me, h], dgl.at[block[name], h], dev[name]) for name in peers] for h in range(HALVES)]

        for load in loads:
            load.wait()
        gxa.begin()
        for link in routes:
            link.start()
        gtb[me] = gtab[place.flat['']]
        for ws in weights:
            for w in ws:
                w.start()
        dgc[...] = jnp.zeros_like(dgc)
        gcol[...] = jnp.zeros_like(gcol)
        for load in attn_loads:
            load.wait()

        def pair(name, between=None):
            attention_qkv(xab, wqkv, qkv, place.chips[name], tok)
            if between is not None:
                between()
            attention_out(qkv, wo, at_part, place.chips[name], NUM_DEV // 2, attn_dims)

        gxa.to_c.arrive()
        pair('')
        gxa.after()
        gx[0].begin()
        gxa.relay()
        gdy[0].begin()
        gxa.core_x.arrive()
        pair('x')
        gxa.core_y.arrive()
        pair('y', gx[0].relay)
        gx[1].begin()
        gxa.last()
        gdy[0].relay()
        gxa.core_d.arrive()
        pair('yx', gx[0].last)
        sat.begin()
        for link in routes:
            link.arrive()
        wide = jnp.concatenate([gtb[...].reshape(NUM_DEV * 8, LANES), jnp.zeros((LANES - NUM_DEV * 8, LANES), F32)], axis=0).T
        for h in range(HALVES):
            for b in range(NUM_DEV):
                gcol[h, b * r:(b + 1) * r, 0:8] = wide[h * r:(h + 1) * r, b * 8:(b + 1) * 8]
            for e in range(exp_loc):
                gfull[h, e] = jnp.broadcast_to(gcol[h][:, e:e + 1], (m, LANES))
        gx[0].finish()

        def staged(h, e, k):
            part = pl.ds(h * m, m)
            if k == 2:
                slot = h * 2 + lax.rem(e, 2)
                return pltpu.make_async_copy(stage_t.at[slot], ht_all.at[e, :, part], stage_sems.at[slot])
            return pltpu.make_async_copy((da, db)[k].at[e], (da_all, db_all)[k].at[e, part, :], grad_sems.at[e, k])

        lane = lax.broadcasted_iota(jnp.int32, (m, LANES), 1)

        def gate_of(h, e):
            return jnp.concatenate([gfull[h, e]] * (tile // LANES), axis=1)

        def loop(count, events, body):
            def step(k, _):
                for at, event in events.items():
                    pl.when(k == at)(event)
                body(k)
                return 0

            lax.fori_loop(0, count, step, 0)

        def hidden(h):
            def body(e):
                if h == 0:
                    for k, (src, dst) in enumerate(((wg_in, wg), (wu_in, wu), (wd_in, wd))):
                        pltpu.make_async_copy(src.at[e], dst.at[e], w_sems.at[e, k]).wait()

                @pl.when(e >= 2)
                def _():
                    staged(h, e - 2, 2).wait()

                mask = gate_of(h, e) > 0.0
                a = jnp.where(mask, dot_nn(xb[h], wg[e]), 0.0)
                b = jnp.where(mask, dot_nn(xb[h], wu[e]), 0.0)
                sig = jax.nn.sigmoid(a)
                act = a * sig
                hid[e] = (act * b).astype(BF16)
                stage_t[h * 2 + lax.rem(e, 2)] = hid[e].T
                s1[e] = b * sig * (1.0 + a * (1.0 - sig))
                s2[e] = act
                staged(h, e, 2).start()

            return body

        def outputs(h):
            def body(n):
                cols = pl.ds(pl.multiple_of(n * tile, tile), tile)
                dy = dyb[h, :, cols].astype(F32)
                sums = dgc[h]
                for e in range(exp_loc):
                    o = dot_nn(hid[e], wd[e, :, cols]).astype(BF16).astype(F32)
                    y = gate_of(h, e) * o
                    y_part[h, :, cols] = y if e == 0 else y_part[h, :, cols] + y
                    prod = dy * o
                    dots = prod[:, 0:LANES]
                    for k in range(1, tile // LANES):
                        dots += prod[:, k * LANES:(k + 1) * LANES]
                    sums += jnp.where(lane == e, jnp.sum(dots, axis=1, keepdims=True), 0.0)
                dgc[h] = sums

            return body

        def hidden_grads(h):
            def body(e):
                if h:
                    for k in range(2):
                        staged(h - 1, e, k).wait()
                for n in range(tiles):
                    cols = pl.ds(n * tile, tile)
                    d_o[:, cols] = (gate_of(h, e) * dyb[h, :, cols].astype(F32)).astype(BF16)
                dh = dot_nt(d_o[...], wd[e]).astype(BF16).astype(F32)
                da[e] = (dh * s1[e]).astype(BF16)
                db[e] = (dh * s2[e]).astype(BF16)
                for k in range(2):
                    staged(h, e, k).start()

            return body

        def input_grads(h):
            def body(n):
                cols = pl.ds(pl.multiple_of(n * tile, tile), tile)
                for e in range(exp_loc):
                    dxe = (dot_nt(da[e], wg[e, cols, :]) + dot_nt(db[e], wu[e, cols, :])).astype(BF16).astype(F32)
                    dx_part[h, :, cols] = dxe if e == 0 else dx_part[h, :, cols] + dxe

            return body

        def send_dg(h):
            turned = dgc[h].T
            for c in range(2):
                dgt[h, c] = turned[0:8, c * LANES:(c + 1) * LANES]
            for link in dg_links[h]:
                link.start()
            dgl[me, h] = dgt[h, place.core]

        def seq(*calls):
            def run():
                for call in calls:
                    call()

            return run

        loop(exp_loc, {0: gdy[1].begin, 1: seq(gdy[0].last, gx[1].relay), 2: sat.middle, 4: seq(gdy[1].relay, gx[1].last)}, hidden(0))
        gdy[0].finish()
        loop(tiles, {1: sy[0][0].begin, 2: sy[0][1].begin}, outputs(0))
        sy[0][2].begin()
        send_dg(0)
        gx[1].finish()
        loop(exp_loc, {1: sy[0][0].middle, 3: sy[0][1].middle, 4: sy[0][2].middle}, hidden_grads(0))
        loop(tiles, {1: sdx[0][0].begin, 2: seq(sdx[0][1].begin, sat.late)}, input_grads(0))
        sdx[0][2].begin()
        loop(exp_loc, {0: gdy[1].last, 1: seq(sdx[0][0].middle, sdx[0][1].middle, sy[0][0].late), 2: seq(gdy[1].finish, sdx[0][2].middle, sy[0][1].late),
                       3: sy[0][2].late, 4: functools.partial(sat.finish, attn_out)}, hidden(1))
        loop(tiles, {1: sy[1][0].begin, 2: seq(sy[1][1].begin, sdx[0][0].late)}, outputs(1))
        sy[1][2].begin()
        send_dg(1)
        sdx[0][1].late()
        loop(exp_loc, {1: sy[1][0].middle, 2: sdx[0][2].late, 3: seq(sy[1][1].middle, sy[1][2].middle), 4: seq(*[functools.partial(s.finish, y_out) for s in sy[0]])}, hidden_grads(1))
        loop(tiles, {1: sdx[1][0].begin, 2: seq(sdx[1][1].begin, sdx[1][0].middle, sy[1][0].late)}, input_grads(1))
        sdx[1][2].begin()
        sdx[1][1].middle()
        sy[1][1].late()
        sy[1][2].late()
        sdx[1][2].middle()
        for h in range(HALVES):
            xt[:, h * m:(h + 1) * m] = xb[h].T
        saves = [pltpu.make_async_copy(xt, xt_all, out_sems.at[0]), pltpu.make_async_copy(dyb, dy_all, out_sems.at[1]), pltpu.make_async_copy(gcol, gates_out, out_sems.at[2])]
        for save in saves:
            save.start()
        for s in sdx[0]:
            s.finish(dx_out)
        for s in sdx[1]:
            s.late()
        for h in range(HALVES):
            for link in dg_links[h]:
                link.arrive()
        for h in range(HALVES):
            slots = idx_in[:, h * r:(h + 1) * r]
            total = jnp.zeros(slots.shape, F32)
            for b in range(NUM_DEV):
                first = ((b // 2) % 2 * 4 + b % 2 * 2 + b // 4) * exp_loc
                rows = dgl[b, h]
                mine = jnp.zeros((8, r), F32)
                for q in range(LANES // r):
                    mine = jnp.where(place.chip == q, rows[:, q * r:(q + 1) * r], mine)
                for e in range(exp_loc):
                    total = jnp.where(slots == first + e, mine[e:e + 1, :], total)
            dg_out[:, h * r:(h + 1) * r] = total
        for s in sy[1]:
            s.finish(y_out, r)
        for s in sdx[1]:
            s.finish(dx_out, r)
        for save in saves:
            save.wait()
        for e in range(exp_loc):
            for k in range(2):
                staged(HALVES - 1, jnp.int32(e), k).wait()
        for h in range(HALVES):
            for e in (exp_loc - 2, exp_loc - 1):
                staged(h, jnp.int32(e), 2).wait()
        for item in gx + gdy + [gxa, sat] + sum(sy + sdx, []):
            item.drain()
        for link in routes + dg_links[0] + dg_links[1]:
            link.sent()
        assert pool.used == NUM_LINKS

    return kernel, r, m


def weight_grads(width, slots, xt_in, dy_in, g_in, da_in, db_in, ht_in, y_in, dx_in, at_in, dg_in,
                 dwg, dwu, dwd, y_out, dx_out, at_out, dg_out,
                 xt, dy, g, da, db, ht, sg, su, sd, y, dx, at, dg, x_sems, d_sems, g_sem, e_sems, o_sems, p_sems):
    exp_loc = da.shape[0]
    steps = dy.shape[1] // width

    def load(e, k):
        src, dst = ((da_in, da), (db_in, db), (ht_in, ht))[k]
        return pltpu.make_async_copy(src.at[e], dst.at[e], e_sems.at[e, k])

    def x_load(n):
        rows = slice(n * width, (n + 1) * width)
        return pltpu.make_async_copy(xt_in.at[rows, :], xt.at[rows, :], x_sems.at[n])

    def dy_load(n):
        cols = slice(n * width, (n + 1) * width)
        return pltpu.make_async_copy(dy_in.at[:, cols], dy.at[:, cols], d_sems.at[n])

    g_load = pltpu.make_async_copy(g_in, g, g_sem)
    x_load(0).start()
    load(0, 0).start()
    load(0, 1).start()
    for n in range(1, steps):
        x_load(n).start()
    load(0, 2).start()
    g_load.start()
    for n in range(steps):
        dy_load(n).start()
    for e in range(1, exp_loc):
        for k in range(3):
            load(e, k).start()
    passing = ((y_in, y, y_out), (dx_in, dx, dx_out), (at_in, at, at_out), (dg_in, dg, dg_out))
    take = [pltpu.make_async_copy(src, mid, p_sems.at[k, 0]) for k, (src, mid, _) in enumerate(passing)]
    give = [pltpu.make_async_copy(mid, dst, p_sems.at[k, 1]) for k, (_, mid, dst) in enumerate(passing)]
    for copy in take:
        copy.start()

    def store(e, n, k):
        part = pl.ds(n * width, width)
        n = lax.rem(e, 2) * steps + n
        if k == 2:
            return pltpu.make_async_copy(sd.at[n], dwd.at[e, :, part], o_sems.at[n, k])
        return pltpu.make_async_copy((sg, su)[k].at[n], (dwg, dwu)[k].at[e, part, :], o_sems.at[n, k])

    lane = lax.broadcasted_iota(jnp.int32, g.shape, 1)

    def down(e):
        gate = jnp.sum(jnp.where(lane == e, g[...], 0.0), axis=1, keepdims=True)
        for n in range(steps):
            part = pl.ds(n * width, width)
            sd[lax.rem(e, 2) * steps + n] = dot_nn(ht[e], (gate * dy[:, part].astype(F32)).astype(BF16))
            store(e, n, 2).start()

    def step(e, _):
        @pl.when(e == 0)
        def _():
            load(e, 0).wait()
            load(e, 1).wait()
            for n in range(steps):
                x_load(n).wait()

        @pl.when(e > 0)
        def _():
            for k in range(3):
                load(e, k).wait()

        @pl.when(e > 1)
        def _():
            for n in range(steps):
                for k in range(2):
                    store(e - 2, n, k).wait()

        for n in range(steps):
            part = pl.ds(n * width, width)
            sg[lax.rem(e, 2) * steps + n] = dot_nn(xt[part, :], da[e])
            store(e, n, 0).start()
            su[lax.rem(e, 2) * steps + n] = dot_nn(xt[part, :], db[e])
            store(e, n, 1).start()

        @pl.when(e == 0)
        def _():
            load(e, 2).wait()
            g_load.wait()
            for n in range(steps):
                dy_load(n).wait()

        @pl.when(e > 1)
        def _():
            for n in range(steps):
                store(e - 2, n, 2).wait()

        @pl.when(e == 1)
        def _():
            for copy in take:
                copy.wait()
            for copy in give:
                copy.start()

        down(e)
        return 0

    lax.fori_loop(0, exp_loc, step, 0)
    for e in (exp_loc - 2, exp_loc - 1):
        for n in range(steps):
            for k in range(3):
                store(jnp.int32(e), n, k).wait()
    for copy in give:
        copy.wait()


def solution(mesh):
    num_dev = mesh.shape['ei'] * mesh.shape['eo']
    assert num_dev == NUM_DEV

    def local_step(x_tokens, expert_idx, gate_vals, dy_tokens, w_gate, w_up, w_down, x_attn, w_query, w_key, w_value, w_out):
        tok, d_model = x_tokens.shape
        top_k = expert_idx.shape[1]
        exp_loc, _, d_ff = w_gate.shape
        seq = x_attn.shape[1]
        heads, head_dim = w_query.shape[1], w_query.shape[2]
        kv_dim = w_key.shape[1] * head_dim
        q_dim = heads * head_dim
        wq = w_query.transpose(1, 2, 0).reshape(q_dim, d_model)
        wk = w_key.transpose(1, 2, 0).reshape(kv_dim, d_model)
        wv = w_value.transpose(1, 2, 0).reshape(kv_dim, d_model)
        wo = w_out.reshape(q_dim, d_model)
        kernel, r, m = make_layer_kernel(tok, d_model, d_ff, exp_loc, (seq, kv_dim, heads, head_dim))
        any_spec = pl.BlockSpec(memory_space=pl.ANY)
        vmem_spec = pl.BlockSpec(memory_space=pltpu.VMEM)
        shape = jax.ShapeDtypeStruct
        total = tok * NUM_DEV

        def half_shapes():
            return [pltpu.VMEM((HALVES, d_model // 512) + s.shape, s.dtype) for s in scatter_shapes(r, 512)]

        y, dx, attn, dgt, xt, dy_all, da, db, ht, gates = pl.pallas_call(
            kernel,
            out_shape=(shape((tok, d_model), BF16), shape((tok, d_model), BF16), shape((tok, d_model), BF16), shape((top_k, tok), F32),
                       shape((d_model, total), BF16), shape((HALVES, m, d_model), BF16),
                       shape((exp_loc, total, d_ff), BF16), shape((exp_loc, total, d_ff), BF16), shape((exp_loc, d_ff, total), BF16), shape((HALVES, m, LANES), F32)),
            in_specs=[any_spec, any_spec, any_spec, vmem_spec, vmem_spec] + [any_spec] * 7,
            out_specs=(vmem_spec,) * 4 + (any_spec,) * 6,
            scratch_shapes=[pltpu.VMEM((HALVES, m, d_model), BF16), pltpu.VMEM((HALVES, m, d_model), BF16), pltpu.VMEM((total, d_model), BF16),
                            pltpu.VMEM((NUM_DEV, 8, LANES), F32), pltpu.VMEM((HALVES, m, LANES), F32),
                            pltpu.VMEM((exp_loc, d_model, d_ff), BF16), pltpu.VMEM((exp_loc, d_model, d_ff), BF16), pltpu.VMEM((exp_loc, d_ff, d_model), BF16),
                            pltpu.VMEM((HALVES, m, d_model), F32), pltpu.VMEM((HALVES, m, d_model), F32), pltpu.VMEM((total, d_model), F32), pltpu.VMEM((q_dim + 2 * kv_dim, d_model), BF16), pltpu.VMEM((q_dim, d_model), BF16), pltpu.VMEM((2 * tok, q_dim + 2 * kv_dim), BF16),
                            pltpu.VMEM((exp_loc, m, d_ff), F32), pltpu.VMEM((exp_loc, m, d_ff), F32), pltpu.VMEM((m, d_model), BF16),
                            pltpu.VMEM((HALVES, m, LANES), F32), pltpu.VMEM((HALVES, 2, 8, LANES), F32), pltpu.VMEM((exp_loc, m, d_ff), BF16), pltpu.VMEM((exp_loc, m, d_ff), BF16),
                            pltpu.VMEM((exp_loc, m, d_ff), BF16), pltpu.VMEM((2 * HALVES, d_ff, m), BF16), pltpu.VMEM((d_model, total), BF16), pltpu.VMEM((NUM_DEV, HALVES, 8, LANES), F32), pltpu.VMEM((NUM_DEV, 8, LANES), F32), pltpu.VMEM((HALVES, exp_loc, m, LANES), F32)]
            + half_shapes() + half_shapes() + scatter_shapes(tok, d_model)
            + [pltpu.SemaphoreType.DMA((NUM_LINKS,)), pltpu.SemaphoreType.DMA((NUM_LINKS,)), pltpu.SemaphoreType.DMA((exp_loc, 3)),
               pltpu.SemaphoreType.DMA((5,)), pltpu.SemaphoreType.DMA((4,)), pltpu.SemaphoreType.DMA((3,)), pltpu.SemaphoreType.DMA((2 * HALVES,)), pltpu.SemaphoreType.DMA((exp_loc, 2))],
            compiler_params=pltpu.CompilerParams(collective_id=0, has_side_effects=True, vmem_limit_bytes=67000000),
            name='layer',
        )(x_tokens, dy_tokens, x_attn.reshape(tok, d_model), expert_idx.T, gate_vals.T, w_gate, w_up, w_down, wq, wk, wv, wo)

        width = 512
        steps = d_model // width
        slots = 2 * steps
        small = (y, dx, attn, dgt)
        dw_gate, dw_up, dw_down, y, dx, attn, dgt = pl.pallas_call(
            functools.partial(weight_grads, width, slots),
            out_shape=(shape((exp_loc, d_model, d_ff), F32), shape((exp_loc, d_model, d_ff), F32), shape((exp_loc, d_ff, d_model), F32)) + tuple(shape(v.shape, v.dtype) for v in small),
            in_specs=[any_spec] * 10,
            out_specs=(any_spec,) * 7,
            scratch_shapes=[pltpu.VMEM((d_model, total), BF16), pltpu.VMEM((total, d_model), BF16), pltpu.VMEM((total, LANES), F32),
                            pltpu.VMEM((exp_loc, total, d_ff), BF16), pltpu.VMEM((exp_loc, total, d_ff), BF16), pltpu.VMEM((exp_loc, d_ff, total), BF16),
                            pltpu.VMEM((slots, width, d_ff), F32), pltpu.VMEM((slots, width, d_ff), F32), pltpu.VMEM((slots, d_ff, width), F32)]
            + [pltpu.VMEM(v.shape, v.dtype) for v in small]
            + [pltpu.SemaphoreType.DMA((steps,)), pltpu.SemaphoreType.DMA((steps,)), pltpu.SemaphoreType.DMA(()), pltpu.SemaphoreType.DMA((exp_loc, 3)),
               pltpu.SemaphoreType.DMA((slots, 3)), pltpu.SemaphoreType.DMA((4, 2))],
            compiler_params=pltpu.CompilerParams(vmem_limit_bytes=66000000),
            name='weight_grads',
        )(xt, dy_all.reshape(total, d_model), gates.reshape(total, LANES), da, db, ht, y, dx, attn, dgt)
        return y, dx, dgt.T, dw_gate, dw_up, dw_down, attn.reshape(x_attn.shape)

    spec_rows = P(TOKEN_AXES, None)
    spec_seqs = P(TOKEN_AXES, None, None)
    spec_experts = P(GROUP_AXES, None, None)
    spec_heads = P(None, GROUP_AXES, None)
    return jax.shard_map(local_step, mesh=mesh,
                         in_specs=(spec_rows, spec_rows, spec_rows, spec_rows, spec_experts, spec_experts, spec_experts, spec_seqs, spec_heads, spec_heads, spec_heads, spec_experts),
                         out_specs=(spec_rows, spec_rows, spec_rows, spec_seqs, spec_seqs, spec_seqs, spec_seqs),
                         check_vma=False)
```

```python
import functools

import jax
import jax.numpy as jnp
from jax import lax
from jax.experimental import pallas as pl
from jax.experimental.pallas import tpu as pltpu
from jax.sharding import PartitionSpec as P

GROUP_AXES = ('ei', 'eo')
TOKEN_AXES = ('dp', 'ei', 'eo')
F32 = jnp.float32
BF16 = jnp.bfloat16
MESH_ID = pl.DeviceIdType.MESH
HALVES = 2
NUM_DEV = 8
LANES = 128


def dot_nn(lhs, rhs):
    return jnp.dot(lhs, rhs, preferred_element_type=F32)


def dot_nt(lhs, rhs):
    return lax.dot_general(lhs, rhs, (((1,), (1,)), ((), ())), preferred_element_type=F32)


def dot_tn(lhs, rhs):
    return lax.dot_general(lhs, rhs, (((0,), (0,)), ((), ())), preferred_element_type=F32)


class Place:
    def __init__(self):
        i = lax.axis_index('ei')
        o = lax.axis_index('eo')
        x = lax.div(o, 2)
        c = lax.rem(o, 2)
        self.core = c
        self.chip = i * 2 + x
        self.dev = {}
        self.block = {}
        self.flat = {}
        self.pair = {}
        self.chips = {}
        for flip_y in (0, 1):
            for flip_x in (0, 1):
                for flip_c in (0, 1):
                    yy = 1 - i if flip_y else i
                    xx = 1 - x if flip_x else x
                    cc = 1 - c if flip_c else c
                    name = ('y' if flip_y else '') + ('x' if flip_x else '') + ('c' if flip_c else '')
                    self.dev[name] = (0, yy, xx * 2 + cc)
                    self.block[name] = cc * 4 + yy * 2 + xx
                    self.flat[name] = yy * 4 + xx * 2 + cc
                    self.pair[name] = (yy * 2 + xx) * 2 + cc
                    self.chips[name] = yy * 2 + xx


class Link:
    def __init__(self, pool, src, dst, land, device):
        send, recv = pool.take()
        self.out = pltpu.make_async_remote_copy(src_ref=src, dst_ref=dst, send_sem=send, recv_sem=recv, device_id=device, device_id_type=MESH_ID)
        self.inn = pltpu.make_async_remote_copy(src_ref=land, dst_ref=land, send_sem=send, recv_sem=recv, device_id=device, device_id_type=MESH_ID)

    def start(self):
        self.out.start()

    def arrive(self):
        self.inn.wait_recv()

    def sent(self):
        self.out.wait_send()


class Pool:
    def __init__(self, sends, recvs):
        self.sends, self.recvs, self.used = sends, recvs, 0

    def take(self):
        k = self.used
        self.used += 1
        return self.sends.at[k], self.recvs.at[k]


class Gather:
    def __init__(self, pool, place, buf, rows, index):
        def at(name, lo=0, n=rows):
            return buf.at[pl.ds(pl.multiple_of(index[name] * rows + lo, 8), n), :]

        half = rows // 2
        own = at('')
        dev = place.dev
        self.to_x = Link(pool, own, own, at('x'), dev['x'])
        self.to_y = Link(pool, own, own, at('y'), dev['y'])
        self.to_c = Link(pool, own, own, at('c'), dev['c'])
        self.relay_x = Link(pool, at('y', 0, half), at('y', 0, half), at('yx', 0, half), dev['x'])
        self.relay_y = Link(pool, at('x', half, half), at('x', half, half), at('yx', half, half), dev['y'])
        self.core_x = Link(pool, at('x'), at('x'), at('xc'), dev['c'])
        self.core_y = Link(pool, at('y'), at('y'), at('yc'), dev['c'])
        self.core_d = Link(pool, at('yx'), at('yx'), at('yxc'), dev['c'])
        self.early = self.relayed = False
        self.links = (self.to_x, self.to_y, self.to_c, self.relay_x, self.relay_y, self.core_x, self.core_y, self.core_d)

    def begin_links(self):
        self.to_x.start()
        self.to_y.start()

    def begin_core(self):
        self.to_c.start()

    def begin(self):
        self.begin_links()
        self.begin_core()

    def after(self):
        self.early = True
        self.to_x.sent()
        self.to_y.sent()

    def relay(self):
        self.to_y.arrive()
        self.relay_x.start()
        self.to_x.arrive()
        self.relay_y.start()
        self.core_x.start()
        self.core_y.start()

    def relay_left(self):
        self.relayed = True
        self.relay_x.sent()
        self.relay_y.sent()

    def last(self):
        self.relay_x.arrive()
        self.relay_y.arrive()
        self.core_d.start()

    def finish(self):
        self.to_c.arrive()
        self.core_x.arrive()
        self.core_y.arrive()
        self.core_d.arrive()

    def drain(self):
        for link in self.links:
            if not (self.early and link in (self.to_x, self.to_y)) and not (self.relayed and link in (self.relay_x, self.relay_y)):
                link.sent()


class Scatter:
    def __init__(self, pool, place, part, from_core, from_x, from_y, last_x, last_y, rows, first=0):
        half = rows // 2
        self.half, self.part, self.rows, self.place = half, part, rows, place
        self.from_core, self.from_x, self.from_y, self.last_x, self.last_y = from_core, from_x, from_y, last_x, last_y
        four = 4 * rows
        self.mine = pl.multiple_of(place.core * four, 8)
        self.cols = pl.ds(first, from_core.shape[-1])
        other = part.at[pl.ds(pl.multiple_of((1 - place.core) * four, 8), four), self.cols]
        dev = place.dev
        self.core = Link(pool, other, from_core, from_core, dev['c'])
        self.x0 = Link(pool, self.at('x', 0), from_x.at[0], from_x.at[0], dev['x'])
        self.x1 = Link(pool, self.at('yx', 0), from_x.at[1], from_x.at[1], dev['x'])
        self.y0 = Link(pool, self.at('y', half), from_y.at[0], from_y.at[0], dev['y'])
        self.y1 = Link(pool, self.at('yx', half), from_y.at[1], from_y.at[1], dev['y'])
        self.end_y = Link(pool, self.at('y', 0), last_y, last_y, dev['y'])
        self.end_x = Link(pool, self.at('x', half), last_x, last_x, dev['x'])
        self.links = (self.core, self.x0, self.x1, self.y0, self.y1, self.end_y, self.end_x)

    def at(self, name, lo):
        return self.part.at[pl.ds(pl.multiple_of(self.place.block[name] * self.rows + lo, 8), self.half), self.cols]

    def begin(self):
        self.core.start()

    def middle(self):
        self.core.arrive()
        mine = pl.ds(self.mine, 4 * self.rows)
        self.part[mine, self.cols] = self.part[mine, self.cols] + self.from_core[...]
        self.x1.start()
        self.y1.start()
        self.x0.start()
        self.y0.start()

    def late(self):
        self.x1.arrive()
        here = self.at('y', 0)
        here[...] = here[...] + self.from_x[1]
        self.end_y.start()
        self.y1.arrive()
        here = self.at('x', self.half)
        here[...] = here[...] + self.from_y[1]
        self.end_x.start()

    def finish(self, out, row=0):
        half = self.half
        self.x0.arrive()
        self.y0.arrive()
        self.end_y.arrive()
        self.end_x.arrive()
        out[row:row + half, self.cols] = (self.at('', 0)[...] + self.from_x[0] + self.last_y[...]).astype(BF16)
        out[row + half:row + 2 * half, self.cols] = (self.at('', half)[...] + self.from_y[0] + self.last_x[...]).astype(BF16)

    def drain(self):
        for link in self.links:
            link.sent()


class ChipSum:
    def __init__(self, pool, place, part, from_core, rows, first, outs, sems):
        four = 4 * rows
        self.part, self.from_core = part, from_core
        self.mine = pl.multiple_of(place.core * four, 8)
        self.cols = pl.ds(first, from_core.shape[-1])
        other = part.at[pl.ds(pl.multiple_of((1 - place.core) * four, 8), four), self.cols]
        self.core = Link(pool, other, from_core, from_core, place.dev['c'])
        self.copies = [pltpu.make_async_copy(part.at[pl.ds(pl.multiple_of(place.block[name] * rows, 8), rows), self.cols], out.at[:, self.cols], sems.at[k])
                       for k, (name, out) in enumerate(outs)]

    def begin(self):
        self.core.start()

    def middle(self):
        self.core.arrive()
        mine = pl.ds(self.mine, self.from_core.shape[0])
        self.part[mine, self.cols] = self.part[mine, self.cols] + self.from_core[...]
        for copy in self.copies:
            copy.start()

    def drain(self):
        self.core.sent()
        for copy in self.copies:
            copy.wait()


def scatter_shapes(rows, width):
    half = rows // 2
    return [pltpu.VMEM((4 * rows, width), F32), pltpu.VMEM((2, half, width), F32), pltpu.VMEM((2, half, width), F32),
            pltpu.VMEM((half, width), F32), pltpu.VMEM((half, width), F32)]


NUM_LINKS = 7 + 14 + 8 * 5 + 7 * 7 + 6


def attention_qkv(xa, wqkv, qkv, chip, seq):
    pair = 2 * seq
    qkv[...] = dot_nt(xa[pl.ds(pl.multiple_of(chip * pair, pair), pair), :], wqkv[...]).astype(BF16)


def attention_out(qkv, wo, part, chip, chips, dims):
    seq, kv_dim, heads, head_dim = dims
    q_dim = heads * head_dim
    pair = 2 * seq
    row = lax.broadcasted_iota(jnp.int32, (pair, pair), 0)
    col = lax.broadcasted_iota(jnp.int32, (pair, pair), 1)
    causal = (row >= col) & ((row >= seq) == (col >= seq))
    keys = qkv[:, q_dim:q_dim + kv_dim]
    vals = qkv[:, q_dim + kv_dim:q_dim + 2 * kv_dim]
    outs = []
    for h in range(heads):
        scores = dot_nt(qkv[:, h * head_dim:(h + 1) * head_dim], keys) * head_dim ** -0.5
        scores = jnp.where(causal, scores, -1e30)
        top = jnp.max(scores, axis=1, keepdims=True)
        ex = jnp.exp(scores - top)
        probs = (ex / jnp.sum(ex, axis=1, keepdims=True)).astype(BF16)
        outs.append(dot_nn(probs, vals).astype(BF16))
    out = dot_nn(jnp.concatenate(outs, axis=1), wo[...])
    for c in range(2):
        part[pl.ds(pl.multiple_of((c * chips + chip) * seq, seq), seq), :] = out[c * seq:(c + 1) * seq, :]


def make_layer_kernel(tok, d_model, d_ff, exp_loc, attn_dims):
    r = tok // HALVES
    m = r * NUM_DEV
    tile = 512
    tiles = d_model // tile

    def kernel(x_in, dy_in, xa_in, idx_in, gate_in, wg_in, wu_in, wd_in, wq_in, wk_in, wv_in, wo_in,
               y_out, dx_out, attn_out, dg_out, xt_all, dy_all, da_all, db_all, ht_all, gates_out, own_out, to_x_out, to_y_out, to_d_out,
               xb, dyb, xab, gtb, gcol, wg, wu, wd, y_part, dx_part, at_part, wqkv, wo, qkv, s1, s2, d_o, dgc, dgt, da, db, hid, stage_t, xt, dgl, gtab, gfull,
               ryc, rdc, ry0, ry1, ry2, ry3, ry4, rd0, rd1, rd2, rd3, rd4, ra0, ra1, ra2, ra3, ra4,
               send_sems, recv_sems, w_sems, in_sems, aw_sems, out_sems, stage_sems, grad_sems, sum_sems, res_sems, y_res, dx_res, attn_res, dg_res):
        place = Place()
        pool = Pool(send_sems, recv_sems)
        dev, block = place.dev, place.block
        me = block['']

        def own_rows(buf, rows, index=me):
            return buf.at[pl.ds(pl.multiple_of(index * rows, 8), rows), :]

        loads = []
        for h in range(HALVES):
            loads.append(pltpu.make_async_copy(x_in.at[h * r:(h + 1) * r, :], own_rows(xb.at[h], r), in_sems.at[h]))
            loads.append(pltpu.make_async_copy(dy_in.at[h * r:(h + 1) * r, :], own_rows(dyb.at[h], r), in_sems.at[2 + h]))
        loads.append(pltpu.make_async_copy(xa_in, own_rows(xab, tok, place.pair['']), in_sems.at[4]))
        for load in loads:
            load.start()
        q_dim, kv_dim = wq_in.shape[0], wk_in.shape[0]
        attn_loads = [pltpu.make_async_copy(wq_in, wqkv.at[0:q_dim, :], aw_sems.at[0]), pltpu.make_async_copy(wk_in, wqkv.at[q_dim:q_dim + kv_dim, :], aw_sems.at[1]),
                      pltpu.make_async_copy(wv_in, wqkv.at[q_dim + kv_dim:q_dim + 2 * kv_dim, :], aw_sems.at[2]), pltpu.make_async_copy(wo_in, wo, aw_sems.at[3])]
        for load in attn_loads:
            load.start()
        weights = []
        for e in range(exp_loc):
            weights.append([pltpu.make_async_copy(src.at[e], dst.at[e], w_sems.at[e, k]) for k, (src, dst) in enumerate(((wg_in, wg), (wu_in, wu), (wd_in, wd)))])
        barrier = pltpu.get_barrier_semaphore()
        peers = [name for name in dev if name]
        for name in peers:
            pl.semaphore_signal(barrier, inc=1, device_id=dev[name], device_id_type=MESH_ID)
        gtab[...] = jnp.zeros_like(gtab)
        for g in range(NUM_DEV):
            for e in range(exp_loc):
                gtab[g, e:e + 1, 0:tok] = jnp.sum(jnp.where(idx_in[...] == g * exp_loc + e, gate_in[...], 0.0), axis=0, keepdims=True)
        pl.semaphore_wait(barrier, len(peers))

        routes = [Link(pool, gtab.at[place.flat[name]], gtb.at[me], gtb.at[block[name]], dev[name]) for name in peers]
        gx = [Gather(pool, place, xb.at[h], r, block) for h in range(HALVES)]
        gdy = [Gather(pool, place, dyb.at[h], r, block) for h in range(HALVES)]
        gxa = Gather(pool, place, xab, tok, place.pair)
        def passed(t):
            return [(name, out.at[t]) for name, out in (('', own_out), ('x', to_x_out), ('y', to_y_out), ('yx', to_d_out))]

        sy = [[Scatter(pool, place, y_part.at[0], ry0.at[n], ry1.at[n], ry2.at[n], ry3.at[n], ry4.at[n], r, n * tile) for n in range(tiles)],
              [ChipSum(pool, place, y_part.at[1], ryc.at[n], r, n * tile, passed(0), sum_sems.at[0, n]) for n in range(tiles)]]
        sdx = [[Scatter(pool, place, dx_part.at[0], rd0.at[n], rd1.at[n], rd2.at[n], rd3.at[n], rd4.at[n], r, n * tile) for n in range(tiles)],
               [ChipSum(pool, place, dx_part.at[1], rdc.at[n], r, n * tile, passed(1), sum_sems.at[1, n]) for n in range(tiles)]]
        sat = Scatter(pool, place, at_part, ra0, ra1, ra2, ra3, ra4, tok)
        dg_links = [[Link(pool, dgt.at[h, 1 - place.core if 'c' in name else place.core], dgl.at[me, h], dgl.at[block[name], h], dev[name]) for name in peers] for h in range(HALVES)]

        for load in loads:
            load.wait()
        gx[0].begin()
        gxa.begin_core()
        for link in routes:
            link.start()
        gtb[me] = gtab[place.flat['']]
        for ws in weights:
            for w in ws:
                w.start()
        dgc[...] = jnp.zeros_like(dgc)
        gcol[...] = jnp.zeros_like(gcol)
        for load in attn_loads:
            load.wait()

        def pairs(names, between=None):
            for k, name in enumerate(names):
                attention_qkv(xab, wqkv, qkv.at[k], place.chips[name], tok)
            if between is not None:
                between()
            for k, name in enumerate(names):
                attention_out(qkv.at[k], wo, at_part, place.chips[name], NUM_DEV // 2, attn_dims)

        gxa.to_c.arrive()
        pairs(('',))
        gx[0].relay()
        for link in routes:
            link.arrive()
        wide = jnp.concatenate([gtb[...].reshape(NUM_DEV * 8, LANES), jnp.zeros((LANES - NUM_DEV * 8, LANES), F32)], axis=0).T
        for h in range(HALVES):
            for b in range(NUM_DEV):
                gcol[h, b * r:(b + 1) * r, 0:8] = wide[h * r:(h + 1) * r, b * 8:(b + 1) * 8]
            for e in range(exp_loc):
                gfull[h, e] = jnp.broadcast_to(gcol[h][:, e:e + 1], (m, LANES))
        gx[0].relay_left()
        gxa.begin_links()
        gx[0].last()
        gx[0].finish()

        def staged(h, e, k):
            part = pl.ds(h * m, m)
            if k == 2:
                slot = h * 2 + lax.rem(e, 2)
                return pltpu.make_async_copy(stage_t.at[slot], ht_all.at[e, :, part], stage_sems.at[slot])
            return pltpu.make_async_copy((da, db)[k].at[e], (da_all, db_all)[k].at[e, part, :], grad_sems.at[e, k])

        lane = lax.broadcasted_iota(jnp.int32, (m, LANES), 1)

        def gate_of(h, e):
            return jnp.concatenate([gfull[h, e]] * (tile // LANES), axis=1)

        def loop(count, events, body):
            def step(k, _):
                for at, event in events.items():
                    pl.when(k == at)(event)
                body(k)
                return 0

            lax.fori_loop(0, count, step, 0)

        def hidden(h):
            def body(e):
                if h == 0:
                    for k, (src, dst) in enumerate(((wg_in, wg), (wu_in, wu), (wd_in, wd))):
                        pltpu.make_async_copy(src.at[e], dst.at[e], w_sems.at[e, k]).wait()

                @pl.when(e >= 2)
                def _():
                    staged(h, e - 2, 2).wait()

                mask = gate_of(h, e) > 0.0
                a = jnp.where(mask, dot_nn(xb[h], wg[e]), 0.0)
                b = jnp.where(mask, dot_nn(xb[h], wu[e]), 0.0)
                sig = jax.nn.sigmoid(a)
                act = a * sig
                hid[e] = (act * b).astype(BF16)
                stage_t[h * 2 + lax.rem(e, 2)] = hid[e].T
                s1[e] = b * sig * (1.0 + a * (1.0 - sig))
                s2[e] = act
                staged(h, e, 2).start()

            return body

        def outputs(h):
            def body(n):
                cols = pl.ds(pl.multiple_of(n * tile, tile), tile)
                dy = dyb[h, :, cols].astype(F32)
                sums = dgc[h]
                for e in range(exp_loc):
                    o = dot_nn(hid[e], wd[e, :, cols]).astype(BF16).astype(F32)
                    y = gate_of(h, e) * o
                    y_part[h, :, cols] = y if e == 0 else y_part[h, :, cols] + y
                    prod = dy * o
                    dots = prod[:, 0:LANES]
                    for k in range(1, tile // LANES):
                        dots += prod[:, k * LANES:(k + 1) * LANES]
                    sums += jnp.where(lane == e, jnp.sum(dots, axis=1, keepdims=True), 0.0)
                dgc[h] = sums

            return body

        def hidden_grads(h):
            def body(e):
                if h:
                    for k in range(2):
                        staged(h - 1, e, k).wait()
                for n in range(tiles):
                    cols = pl.ds(n * tile, tile)
                    d_o[:, cols] = (gate_of(h, e) * dyb[h, :, cols].astype(F32)).astype(BF16)
                dh = dot_nt(d_o[...], wd[e]).astype(BF16).astype(F32)
                da[e] = (dh * s1[e]).astype(BF16)
                db[e] = (dh * s2[e]).astype(BF16)
                for k in range(2):
                    staged(h, e, k).start()

            return body

        def input_grads(h):
            def body(n):
                cols = pl.ds(pl.multiple_of(n * tile, tile), tile)
                for e in range(exp_loc):
                    dxe = (dot_nt(da[e], wg[e, cols, :]) + dot_nt(db[e], wu[e, cols, :])).astype(BF16).astype(F32)
                    dx_part[h, :, cols] = dxe if e == 0 else dx_part[h, :, cols] + dxe

            return body

        def send_dg(h):
            turned = dgc[h].T
            for c in range(2):
                dgt[h, c] = turned[0:8, c * LANES:(c + 1) * LANES]
            for link in dg_links[h]:
                link.start()
            dgl[me, h] = dgt[h, place.core]

        def dg_read():
            for h in range(HALVES):
                for link in dg_links[h]:
                    link.arrive()
            for h in range(HALVES):
                slots = idx_in[:, h * r:(h + 1) * r]
                total = jnp.zeros(slots.shape, F32)
                for b in range(NUM_DEV):
                    first = ((b // 2) % 2 * 4 + b % 2 * 2 + b // 4) * exp_loc
                    rows = dgl[b, h]
                    mine = jnp.zeros((8, r), F32)
                    for q in range(LANES // r):
                        mine = jnp.where(place.chip == q, rows[:, q * r:(q + 1) * r], mine)
                    for e in range(exp_loc):
                        total = jnp.where(slots == first + e, mine[e:e + 1, :], total)
                dg_res[:, h * r:(h + 1) * r] = total

        def seq(*calls):
            def run():
                for call in calls:
                    call()

            return run

        loop(exp_loc, {2: gdy[0].begin, 3: gxa.relay}, hidden(0))
        gxa.core_x.arrive()
        gxa.core_y.arrive()
        pairs(('x', 'y'), gdy[0].relay)
        gx[1].begin()
        gxa.last()
        gdy[1].begin()
        gxa.core_d.arrive()
        pairs(('yx',), gdy[0].last)
        sat.begin()
        gdy[0].finish()
        loop(tiles, {1: seq(gx[1].relay, sy[0][0].begin), 2: seq(gdy[1].relay, sat.middle, sy[0][1].begin)}, outputs(0))
        sy[0][2].begin()
        send_dg(0)
        loop(exp_loc, {1: sy[0][0].middle, 2: gx[1].last, 3: sy[0][1].middle, 4: sy[0][2].middle}, hidden_grads(0))
        loop(tiles, {1: seq(gx[1].finish, sdx[0][0].begin), 2: seq(gdy[1].last, sdx[0][1].begin)}, input_grads(0))
        sdx[0][2].begin()
        loop(exp_loc, {1: seq(sdx[0][0].middle, sdx[0][1].middle), 2: seq(gdy[1].finish, sdx[0][2].middle)}, hidden(1))
        sat.late()
        loop(tiles, {1: seq(sy[0][0].late, sy[1][0].begin), 2: seq(sy[0][1].late, sy[0][2].late, sy[1][1].begin)}, outputs(1))
        sy[1][2].begin()
        send_dg(1)
        for h in range(HALVES):
            xt[:, h * m:(h + 1) * m] = xb[h].T
        saves = [pltpu.make_async_copy(xt, xt_all, out_sems.at[0]), pltpu.make_async_copy(dyb, dy_all, out_sems.at[1]), pltpu.make_async_copy(gcol, gates_out, out_sems.at[2])]
        for save in saves:
            save.start()
        loop(exp_loc, {1: sy[1][0].middle, 2: sdx[0][0].late, 3: seq(sy[1][1].middle, sy[1][2].middle), 4: sdx[0][1].late}, hidden_grads(1))
        loop(tiles, {1: seq(sdx[1][0].begin, sdx[0][2].late), 2: seq(sdx[1][1].begin, sdx[1][0].middle)}, input_grads(1))
        sdx[1][2].begin()
        sdx[1][1].middle()
        for s in sy[0]:
            s.finish(y_res)
        sat.finish(attn_res)
        for s in sdx[0]:
            s.finish(dx_res)
        dg_read()
        results = [pltpu.make_async_copy(src, dst, res_sems.at[k]) for k, (src, dst) in enumerate(((y_res, y_out), (dx_res, dx_out), (attn_res, attn_out), (dg_res, dg_out)))]
        for result in results:
            result.start()
        sdx[1][2].middle()
        for save in saves + results:
            save.wait()
        for e in range(exp_loc):
            for k in range(2):
                staged(HALVES - 1, jnp.int32(e), k).wait()
        for h in range(HALVES):
            for e in (exp_loc - 2, exp_loc - 1):
                staged(h, jnp.int32(e), 2).wait()
        for item in gx + gdy + [gxa, sat] + sum(sy + sdx, []):
            item.drain()
        for link in routes + dg_links[0] + dg_links[1]:
            link.sent()
        assert pool.used == NUM_LINKS

    return kernel, r, m


def weight_grads(width, slots, xt_in, dy_in, g_in, da_in, db_in, ht_in, at_in, dg_in, y_in, dx_in,
                 dwg, dwu, dwd, at_out, dg_out, y_out, dx_out,
                 xt, dy, g, da, db, ht, sg, su, sd, at, dg, y, dx, x_sems, d_sems, g_sem, e_sems, o_sems, p_sems):
    exp_loc = da.shape[0]
    steps = dy.shape[1] // width

    def load(e, k):
        src, dst = ((da_in, da), (db_in, db), (ht_in, ht))[k]
        return pltpu.make_async_copy(src.at[e], dst.at[e], e_sems.at[e, k])

    def x_load(n):
        rows = slice(n * width, (n + 1) * width)
        return pltpu.make_async_copy(xt_in.at[rows, :], xt.at[rows, :], x_sems.at[n])

    def dy_load(n):
        cols = slice(n * width, (n + 1) * width)
        return pltpu.make_async_copy(dy_in.at[:, cols], dy.at[:, cols], d_sems.at[n])

    g_load = pltpu.make_async_copy(g_in, g, g_sem)
    x_load(0).start()
    load(0, 0).start()
    load(0, 1).start()
    for n in range(1, steps):
        x_load(n).start()
    load(0, 2).start()
    g_load.start()
    for n in range(steps):
        dy_load(n).start()
    for e in range(1, exp_loc):
        for k in range(3):
            load(e, k).start()
    rows = slice(0, y.shape[0])
    passing = ((at_in, at, at_out), (dg_in, dg, dg_out), (y_in, y, y_out.at[rows, :]), (dx_in, dx, dx_out.at[rows, :]))
    take = [pltpu.make_async_copy(src, mid, p_sems.at[k, 0]) for k, (src, mid, _) in enumerate(passing)]
    give = [pltpu.make_async_copy(mid, dst, p_sems.at[k, 1]) for k, (_, mid, dst) in enumerate(passing)]
    for copy in take:
        copy.start()

    def store(e, n, k):
        part = pl.ds(n * width, width)
        n = lax.rem(e, 2) * steps + n
        if k == 2:
            return pltpu.make_async_copy(sd.at[n], dwd.at[e, :, part], o_sems.at[n, k])
        return pltpu.make_async_copy((sg, su)[k].at[n], (dwg, dwu)[k].at[e, part, :], o_sems.at[n, k])

    lane = lax.broadcasted_iota(jnp.int32, g.shape, 1)

    def down(e):
        gate = jnp.sum(jnp.where(lane == e, g[...], 0.0), axis=1, keepdims=True)
        for n in range(steps):
            part = pl.ds(n * width, width)
            sd[lax.rem(e, 2) * steps + n] = dot_nn(ht[e], (gate * dy[:, part].astype(F32)).astype(BF16))
            store(e, n, 2).start()

    def step(e, _):
        @pl.when(e == 0)
        def _():
            load(e, 0).wait()
            load(e, 1).wait()
            for n in range(steps):
                x_load(n).wait()

        @pl.when(e > 0)
        def _():
            for k in range(3):
                load(e, k).wait()

        @pl.when(e > 1)
        def _():
            for n in range(steps):
                for k in range(2):
                    store(e - 2, n, k).wait()

        for n in range(steps):
            part = pl.ds(n * width, width)
            sg[lax.rem(e, 2) * steps + n] = dot_nn(xt[part, :], da[e])
            store(e, n, 0).start()
            su[lax.rem(e, 2) * steps + n] = dot_nn(xt[part, :], db[e])
            store(e, n, 1).start()

        @pl.when(e == 0)
        def _():
            load(e, 2).wait()
            g_load.wait()
            for n in range(steps):
                dy_load(n).wait()

        @pl.when(e > 1)
        def _():
            for n in range(steps):
                store(e - 2, n, 2).wait()

        @pl.when(e == 1)
        def _():
            for copy in take:
                copy.wait()
            for copy in give:
                copy.start()

        down(e)
        return 0

    lax.fori_loop(0, exp_loc, step, 0)
    for e in (exp_loc - 2, exp_loc - 1):
        for n in range(steps):
            for k in range(3):
                store(jnp.int32(e), n, k).wait()
    for copy in give:
        copy.wait()


def solution(mesh):
    num_dev = mesh.shape['ei'] * mesh.shape['eo']
    assert num_dev == NUM_DEV

    def local_step(x_tokens, expert_idx, gate_vals, dy_tokens, w_gate, w_up, w_down, x_attn, w_query, w_key, w_value, w_out):
        tok, d_model = x_tokens.shape
        top_k = expert_idx.shape[1]
        exp_loc, _, d_ff = w_gate.shape
        seq = x_attn.shape[1]
        heads, head_dim = w_query.shape[1], w_query.shape[2]
        kv_dim = w_key.shape[1] * head_dim
        q_dim = heads * head_dim
        wq = w_query.transpose(1, 2, 0).reshape(q_dim, d_model)
        wk = w_key.transpose(1, 2, 0).reshape(kv_dim, d_model)
        wv = w_value.transpose(1, 2, 0).reshape(kv_dim, d_model)
        wo = w_out.reshape(q_dim, d_model)
        kernel, r, m = make_layer_kernel(tok, d_model, d_ff, exp_loc, (seq, kv_dim, heads, head_dim))
        any_spec = pl.BlockSpec(memory_space=pl.ANY)
        vmem_spec = pl.BlockSpec(memory_space=pltpu.VMEM)
        shape = jax.ShapeDtypeStruct
        total = tok * NUM_DEV

        def half_shapes():
            return [pltpu.VMEM((d_model // 512,) + s.shape, s.dtype) for s in scatter_shapes(r, 512)]

        y0, dx0, attn, dgt, xt, dy_all, da, db, ht, gates, own, to_x, to_y, to_d = pl.pallas_call(
            kernel,
            out_shape=(shape((r, d_model), BF16), shape((r, d_model), BF16), shape((tok, d_model), BF16), shape((top_k, tok), F32),
                       shape((d_model, total), BF16), shape((HALVES, m, d_model), BF16),
                       shape((exp_loc, total, d_ff), BF16), shape((exp_loc, total, d_ff), BF16), shape((exp_loc, d_ff, total), BF16), shape((HALVES, m, LANES), F32)) + (shape((2, r, d_model), F32),) * 4,
            in_specs=[any_spec, any_spec, any_spec, vmem_spec, vmem_spec] + [any_spec] * 7,
            out_specs=(any_spec,) * 14,
            scratch_shapes=[pltpu.VMEM((HALVES, m, d_model), BF16), pltpu.VMEM((HALVES, m, d_model), BF16), pltpu.VMEM((total, d_model), BF16),
                            pltpu.VMEM((NUM_DEV, 8, LANES), F32), pltpu.VMEM((HALVES, m, LANES), F32),
                            pltpu.VMEM((exp_loc, d_model, d_ff), BF16), pltpu.VMEM((exp_loc, d_model, d_ff), BF16), pltpu.VMEM((exp_loc, d_ff, d_model), BF16),
                            pltpu.VMEM((HALVES, m, d_model), F32), pltpu.VMEM((HALVES, m, d_model), F32), pltpu.VMEM((total, d_model), F32), pltpu.VMEM((q_dim + 2 * kv_dim, d_model), BF16), pltpu.VMEM((q_dim, d_model), BF16), pltpu.VMEM((2, 2 * tok, q_dim + 2 * kv_dim), BF16),
                            pltpu.VMEM((exp_loc, m, d_ff), F32), pltpu.VMEM((exp_loc, m, d_ff), F32), pltpu.VMEM((m, d_model), BF16),
                            pltpu.VMEM((HALVES, m, LANES), F32), pltpu.VMEM((HALVES, 2, 8, LANES), F32), pltpu.VMEM((exp_loc, m, d_ff), BF16), pltpu.VMEM((exp_loc, m, d_ff), BF16),
                            pltpu.VMEM((exp_loc, m, d_ff), BF16), pltpu.VMEM((2 * HALVES, d_ff, m), BF16), pltpu.VMEM((d_model, total), BF16), pltpu.VMEM((NUM_DEV, HALVES, 8, LANES), F32), pltpu.VMEM((NUM_DEV, 8, LANES), F32), pltpu.VMEM((HALVES, exp_loc, m, LANES), F32)]
            + [pltpu.VMEM((d_model // 512, 4 * r, 512), F32)] * 2 + half_shapes() + half_shapes() + scatter_shapes(tok, d_model)
            + [pltpu.SemaphoreType.DMA((NUM_LINKS,)), pltpu.SemaphoreType.DMA((NUM_LINKS,)), pltpu.SemaphoreType.DMA((exp_loc, 3)),
               pltpu.SemaphoreType.DMA((5,)), pltpu.SemaphoreType.DMA((4,)), pltpu.SemaphoreType.DMA((3,)), pltpu.SemaphoreType.DMA((2 * HALVES,)), pltpu.SemaphoreType.DMA((exp_loc, 2)), pltpu.SemaphoreType.DMA((2, d_model // 512, 4)), pltpu.SemaphoreType.DMA((4,)),
               pltpu.VMEM((r, d_model), BF16), pltpu.VMEM((r, d_model), BF16), pltpu.VMEM((tok, d_model), BF16), pltpu.VMEM((top_k, tok), F32)],
            compiler_params=pltpu.CompilerParams(collective_id=0, has_side_effects=True, vmem_limit_bytes=67000000),
            name='layer',
        )(x_tokens, dy_tokens, x_attn.reshape(tok, d_model), expert_idx.T, gate_vals.T, w_gate, w_up, w_down, wq, wk, wv, wo)

        width = 512
        steps = d_model // width
        slots = 2 * steps
        small = (attn, dgt, y0, dx0)

        def swap(value, flip_y, flip_x):
            eo_size = mesh.shape['eo']
            pairs = [(g, (g // eo_size ^ flip_y) * eo_size + (g % eo_size ^ 2 * flip_x)) for g in range(NUM_DEV)]
            return lax.ppermute(value, GROUP_AXES, pairs)

        from_x, from_y, from_d = swap(to_x, 0, 1), swap(to_y, 1, 0), swap(to_d, 1, 1)
        dw_gate, dw_up, dw_down, attn, dgt, y, dx = pl.pallas_call(
            functools.partial(weight_grads, width, slots),
            out_shape=(shape((exp_loc, d_model, d_ff), F32), shape((exp_loc, d_model, d_ff), F32), shape((exp_loc, d_ff, d_model), F32)) + tuple(shape((tok, d_model) if v is y0 or v is dx0 else v.shape, v.dtype) for v in small),
            in_specs=[any_spec] * 10,
            out_specs=(any_spec,) * 7,
            scratch_shapes=[pltpu.VMEM((d_model, total), BF16), pltpu.VMEM((total, d_model), BF16), pltpu.VMEM((total, LANES), F32),
                            pltpu.VMEM((exp_loc, total, d_ff), BF16), pltpu.VMEM((exp_loc, total, d_ff), BF16), pltpu.VMEM((exp_loc, d_ff, total), BF16),
                            pltpu.VMEM((slots, width, d_ff), F32), pltpu.VMEM((slots, width, d_ff), F32), pltpu.VMEM((slots, d_ff, width), F32)]
            + [pltpu.VMEM(v.shape, v.dtype) for v in small]
            + [pltpu.SemaphoreType.DMA((steps,)), pltpu.SemaphoreType.DMA((steps,)), pltpu.SemaphoreType.DMA(()), pltpu.SemaphoreType.DMA((exp_loc, 3)),
               pltpu.SemaphoreType.DMA((slots, 3)), pltpu.SemaphoreType.DMA((4, 2))],
            compiler_params=pltpu.CompilerParams(vmem_limit_bytes=64500000),
            cost_estimate=pl.CostEstimate(flops=3 * 2 * total * d_model * d_ff * exp_loc, bytes_accessed=3 * 4 * exp_loc * d_model * d_ff, transcendentals=0),
            name='weight_grads',
        )(xt, dy_all.reshape(total, d_model), gates.reshape(total, LANES), da, db, ht, attn, dgt, y0, dx0)
        y, dx = (lax.dynamic_update_slice(whole, (own[t] + from_x[t] + from_y[t] + from_d[t]).astype(BF16), (r, 0)) for t, whole in enumerate((y, dx)))
        return y, dx, dgt.T, dw_gate, dw_up, dw_down, attn.reshape(x_attn.shape)

    spec_rows = P(TOKEN_AXES, None)
    spec_seqs = P(TOKEN_AXES, None, None)
    spec_experts = P(GROUP_AXES, None, None)
    spec_heads = P(None, GROUP_AXES, None)
    return jax.shard_map(local_step, mesh=mesh,
                         in_specs=(spec_rows, spec_rows, spec_rows, spec_rows, spec_experts, spec_experts, spec_experts, spec_seqs, spec_heads, spec_heads, spec_heads, spec_experts),
                         out_specs=(spec_rows, spec_rows, spec_rows, spec_seqs, spec_seqs, spec_seqs, spec_seqs),
                         check_vma=False)
```

```python
import functools

import jax
import jax.numpy as jnp
from jax import lax
from jax.experimental import pallas as pl
from jax.experimental.pallas import tpu as pltpu
from jax.sharding import PartitionSpec as P

GROUP_AXES = ('ei', 'eo')
TOKEN_AXES = ('dp', 'ei', 'eo')
F32 = jnp.float32
BF16 = jnp.bfloat16
MESH_ID = pl.DeviceIdType.MESH
HALVES = 2
NUM_DEV = 8
LANES = 128


def dot_nn(lhs, rhs):
    return jnp.dot(lhs, rhs, preferred_element_type=F32)


def dot_nt(lhs, rhs):
    return lax.dot_general(lhs, rhs, (((1,), (1,)), ((), ())), preferred_element_type=F32)


def dot_tn(lhs, rhs):
    return lax.dot_general(lhs, rhs, (((0,), (0,)), ((), ())), preferred_element_type=F32)


class Place:
    def __init__(self):
        i = lax.axis_index('ei')
        o = lax.axis_index('eo')
        x = lax.div(o, 2)
        c = lax.rem(o, 2)
        self.core = c
        self.chip = i * 2 + x
        self.dev = {}
        self.block = {}
        self.flat = {}
        self.pair = {}
        self.chips = {}
        for flip_y in (0, 1):
            for flip_x in (0, 1):
                for flip_c in (0, 1):
                    yy = 1 - i if flip_y else i
                    xx = 1 - x if flip_x else x
                    cc = 1 - c if flip_c else c
                    name = ('y' if flip_y else '') + ('x' if flip_x else '') + ('c' if flip_c else '')
                    self.dev[name] = (0, yy, xx * 2 + cc)
                    self.block[name] = cc * 4 + yy * 2 + xx
                    self.flat[name] = yy * 4 + xx * 2 + cc
                    self.pair[name] = (yy * 2 + xx) * 2 + cc
                    self.chips[name] = yy * 2 + xx


class Pool:
    def __init__(self, sems):
        self.sems, self.used = sems, 0

    def take(self):
        self.used += 1
        return self.sems.at[self.used - 1]


def send(src, dst, device, sent, landed):
    return pltpu.make_async_remote_copy(src_ref=src, dst_ref=dst, send_sem=sent, recv_sem=landed, device_id=device, device_id_type=MESH_ID)


def wait_for(ref, sem):
    pltpu.make_async_copy(ref, ref, sem).wait()


class Gather:
    def __init__(self, pool, place, buf, rows, index, split=False):
        def at(name, lo=0, n=rows):
            return buf.at[pl.ds(pl.multiple_of(index[name] * rows + lo, 8), n), :]

        half = rows // 2
        own = at('')
        dev = place.dev
        self.buf, self.rows, self.relayed = buf, rows, False
        self.sent, self.relays_sent, self.near, self.relays = (pool.take() for _ in range(4))
        self.over = [pool.take() for _ in range(4)] if split else [pool.take()] * 4
        self.to_x = send(own, own, dev['x'], self.sent, self.near)
        self.to_y = send(own, own, dev['y'], self.sent, self.near)
        self.to_c = send(own, own, dev['c'], self.sent, self.over[0])
        self.relay_x = send(at('y', 0, half), at('y', 0, half), dev['x'], self.relays_sent, self.relays)
        self.relay_y = send(at('x', half, half), at('x', half, half), dev['y'], self.relays_sent, self.relays)
        self.core_x = send(at('x'), at('x'), dev['c'], self.sent, self.over[1])
        self.core_y = send(at('y'), at('y'), dev['c'], self.sent, self.over[2])
        self.core_d = send(at('yx'), at('yx'), dev['c'], self.sent, self.over[3])

    def blocks(self, count):
        return self.buf.at[0:count * self.rows, :]

    def begin_links(self):
        self.to_x.start()
        self.to_y.start()

    def begin_core(self):
        self.to_c.start()

    def begin(self):
        self.begin_links()
        self.begin_core()

    def relay(self):
        wait_for(self.blocks(2), self.near)
        self.relay_x.start()
        self.relay_y.start()
        self.core_x.start()
        self.core_y.start()

    def relay_left(self):
        self.relayed = True
        wait_for(self.blocks(1), self.relays_sent)

    def last(self):
        wait_for(self.blocks(1), self.relays)
        self.core_d.start()

    def crossed(self, k):
        wait_for(self.blocks(1), self.over[k])

    def finish(self):
        wait_for(self.blocks(4), self.over[0])

    def drain(self):
        wait_for(self.blocks(6), self.sent)
        if not self.relayed:
            wait_for(self.blocks(1), self.relays_sent)


class Scatter:
    def __init__(self, pool, place, part, from_core, from_x, from_y, last_x, last_y, rows, first=0):
        half = rows // 2
        self.half, self.part, self.rows, self.place = half, part, rows, place
        self.from_core, self.from_x, self.from_y, self.last_x, self.last_y = from_core, from_x, from_y, last_x, last_y
        four = 4 * rows
        self.mine = pl.multiple_of(place.core * four, 8)
        self.cols = pl.ds(first, from_core.shape[-1])
        other = part.at[pl.ds(pl.multiple_of((1 - place.core) * four, 8), four), self.cols]
        dev = place.dev
        self.sent, self.crossed, self.first_x, self.first_y, self.rest = (pool.take() for _ in range(5))
        self.core = send(other, from_core, dev['c'], self.sent, self.crossed)
        self.x0 = send(self.at('x', 0), from_x.at[0], dev['x'], self.sent, self.rest)
        self.x1 = send(self.at('yx', 0), from_x.at[1], dev['x'], self.sent, self.first_x)
        self.y0 = send(self.at('y', half), from_y.at[0], dev['y'], self.sent, self.rest)
        self.y1 = send(self.at('yx', half), from_y.at[1], dev['y'], self.sent, self.first_y)
        self.end_y = send(self.at('y', 0), last_y, dev['y'], self.sent, self.rest)
        self.end_x = send(self.at('x', half), last_x, dev['x'], self.sent, self.rest)

    def at(self, name, lo):
        return self.part.at[pl.ds(pl.multiple_of(self.place.block[name] * self.rows + lo, 8), self.half), self.cols]

    def begin(self):
        self.core.start()

    def middle(self):
        wait_for(self.from_core, self.crossed)
        mine = pl.ds(self.mine, 4 * self.rows)
        self.part[mine, self.cols] = self.part[mine, self.cols] + self.from_core[...]
        self.x1.start()
        self.y1.start()
        self.x0.start()
        self.y0.start()

    def late(self):
        wait_for(self.from_x.at[1], self.first_x)
        here = self.at('y', 0)
        here[...] = here[...] + self.from_x[1]
        self.end_y.start()
        wait_for(self.from_y.at[1], self.first_y)
        here = self.at('x', self.half)
        here[...] = here[...] + self.from_y[1]
        self.end_x.start()

    def finish(self, out, row=0):
        half = self.half
        wait_for(self.part.at[0:4 * half, self.cols], self.rest)
        out[row:row + half, self.cols] = (self.at('', 0)[...] + self.from_x[0] + self.last_y[...]).astype(BF16)
        out[row + half:row + 2 * half, self.cols] = (self.at('', half)[...] + self.from_y[0] + self.last_x[...]).astype(BF16)

    def drain(self):
        wait_for(self.part.at[0:7 * self.rows, self.cols], self.sent)


class ChipSum:
    def __init__(self, pool, place, part, from_core, rows, first, outs, sem):
        four = 4 * rows
        self.part, self.from_core, self.sem = part, from_core, sem
        self.mine = pl.multiple_of(place.core * four, 8)
        self.cols = pl.ds(first, from_core.shape[-1])
        other = part.at[pl.ds(pl.multiple_of((1 - place.core) * four, 8), four), self.cols]
        self.sent, self.crossed = pool.take(), pool.take()
        self.core = send(other, from_core, place.dev['c'], self.sent, self.crossed)
        self.copies = [pltpu.make_async_copy(part.at[pl.ds(pl.multiple_of(place.block[name] * rows, 8), rows), self.cols], out.at[:, self.cols], sem)
                       for name, out in outs]

    def begin(self):
        self.core.start()

    def middle(self):
        wait_for(self.from_core, self.crossed)
        mine = pl.ds(self.mine, self.from_core.shape[0])
        self.part[mine, self.cols] = self.part[mine, self.cols] + self.from_core[...]
        for copy in self.copies:
            copy.start()

    def drain(self):
        wait_for(self.from_core, self.sent)
        wait_for(self.from_core, self.sem)


def scatter_shapes(rows, width):
    half = rows // 2
    return [pltpu.VMEM((4 * rows, width), F32), pltpu.VMEM((2, half, width), F32), pltpu.VMEM((2, half, width), F32),
            pltpu.VMEM((half, width), F32), pltpu.VMEM((half, width), F32)]


NUM_SEMS = 2 + 4 + 5 * 4 + 8 + 5 * 7 + 2 * 6


def attention_qkv(xa, wqkv, qkv, chip, seq):
    pair = 2 * seq
    qkv[...] = dot_nt(xa[pl.ds(pl.multiple_of(chip * pair, pair), pair), :], wqkv[...]).astype(BF16)


def attention_out(qkv, wo, part, chip, chips, dims):
    seq, kv_dim, heads, head_dim = dims
    q_dim = heads * head_dim
    pair = 2 * seq
    row = lax.broadcasted_iota(jnp.int32, (pair, pair), 0)
    col = lax.broadcasted_iota(jnp.int32, (pair, pair), 1)
    causal = (row >= col) & ((row >= seq) == (col >= seq))
    keys = qkv[:, q_dim:q_dim + kv_dim]
    vals = qkv[:, q_dim + kv_dim:q_dim + 2 * kv_dim]
    outs = []
    for h in range(heads):
        scores = dot_nt(qkv[:, h * head_dim:(h + 1) * head_dim], keys) * head_dim ** -0.5
        scores = jnp.where(causal, scores, -1e30)
        top = jnp.max(scores, axis=1, keepdims=True)
        ex = jnp.exp(scores - top)
        probs = (ex / jnp.sum(ex, axis=1, keepdims=True)).astype(BF16)
        outs.append(dot_nn(probs, vals).astype(BF16))
    out = dot_nn(jnp.concatenate(outs, axis=1), wo[...])
    for c in range(2):
        part[pl.ds(pl.multiple_of((c * chips + chip) * seq, seq), seq), :] = out[c * seq:(c + 1) * seq, :]


def make_layer_kernel(tok, d_model, d_ff, exp_loc, attn_dims):
    r = tok // HALVES
    m = r * NUM_DEV
    tile = 512
    tiles = d_model // tile

    def kernel(x_in, dy_in, xa_in, idx_in, gate_in, wg_in, wu_in, wd_in, wq_in, wk_in, wv_in, wo_in,
               y_out, dx_out, attn_out, dg_out, xt_all, dy_all, da_all, db_all, ht_all, gates_out, own_out, to_x_out, to_y_out, to_d_out,
               xb, dyb, xab, gtb, gcol, wg, wu, wd, y_part, dx_part, at_part, wqkv, wo, qkv, s1, s2, d_o, dgc, dgt, da, db, hid, stage_t, xt, dgl, gtab, gfull,
               ryc, rdc, ry0, ry1, ry2, ry3, ry4, rd0, rd1, rd2, rd3, rd4, ra0, ra1, ra2, ra3, ra4,
               sems, w_sems, in_sems, aw_sems, out_sems, stage_sems, grad_sems, sum_sems, res_sems, y_res, dx_res, attn_res, dg_res):
        place = Place()
        pool = Pool(sems)
        dev, block = place.dev, place.block
        me = block['']

        def own_rows(buf, rows, index=me):
            return buf.at[pl.ds(pl.multiple_of(index * rows, 8), rows), :]

        loads = []
        for h in range(HALVES):
            loads.append(pltpu.make_async_copy(x_in.at[h * r:(h + 1) * r, :], own_rows(xb.at[h], r), in_sems))
            loads.append(pltpu.make_async_copy(dy_in.at[h * r:(h + 1) * r, :], own_rows(dyb.at[h], r), in_sems))
        loads.append(pltpu.make_async_copy(xa_in, own_rows(xab, tok, place.pair['']), in_sems))
        for load in loads:
            load.start()
        q_dim, kv_dim = wq_in.shape[0], wk_in.shape[0]
        attn_loads = [pltpu.make_async_copy(wq_in, wqkv.at[0:q_dim, :], aw_sems), pltpu.make_async_copy(wk_in, wqkv.at[q_dim:q_dim + kv_dim, :], aw_sems),
                      pltpu.make_async_copy(wv_in, wqkv.at[q_dim + kv_dim:q_dim + 2 * kv_dim, :], aw_sems), pltpu.make_async_copy(wo_in, wo, aw_sems)]
        for load in attn_loads:
            load.start()
        weights = []
        for e in range(exp_loc):
            weights.append([pltpu.make_async_copy(src.at[e], dst.at[e], w_sems.at[e]) for src, dst in ((wg_in, wg), (wu_in, wu), (wd_in, wd))])
        barrier = pltpu.get_barrier_semaphore()
        peers = [name for name in dev if name]
        for name in peers:
            pl.semaphore_signal(barrier, inc=1, device_id=dev[name], device_id_type=MESH_ID)
        gtab[...] = jnp.zeros_like(gtab)
        for g in range(NUM_DEV):
            for e in range(exp_loc):
                gtab[g, e:e + 1, 0:tok] = jnp.sum(jnp.where(idx_in[...] == g * exp_loc + e, gate_in[...], 0.0), axis=0, keepdims=True)
        pl.semaphore_wait(barrier, len(peers))

        routes_sent, routes_in = pool.take(), pool.take()
        routes = [send(gtab.at[place.flat[name]], gtb.at[me], dev[name], routes_sent, routes_in) for name in peers]
        gx = [Gather(pool, place, xb.at[h], r, block) for h in range(HALVES)]
        gdy = [Gather(pool, place, dyb.at[h], r, block) for h in range(HALVES)]
        gxa = Gather(pool, place, xab, tok, place.pair, split=True)
        def passed(t):
            return [(name, out.at[t]) for name, out in (('', own_out), ('x', to_x_out), ('y', to_y_out), ('yx', to_d_out))]

        sy = [[Scatter(pool, place, y_part.at[0], ry0.at[n], ry1.at[n], ry2.at[n], ry3.at[n], ry4.at[n], r, n * tile) for n in range(tiles)],
              [ChipSum(pool, place, y_part.at[1], ryc.at[n], r, n * tile, passed(0), sum_sems.at[0, n]) for n in range(tiles)]]
        sdx = [[Scatter(pool, place, dx_part.at[0], rd0.at[n], rd1.at[n], rd2.at[n], rd3.at[n], rd4.at[n], r, n * tile) for n in range(tiles)],
               [ChipSum(pool, place, dx_part.at[1], rdc.at[n], r, n * tile, passed(1), sum_sems.at[1, n]) for n in range(tiles)]]
        sat = Scatter(pool, place, at_part, ra0, ra1, ra2, ra3, ra4, tok)
        dg_sems = [(pool.take(), pool.take()) for _ in range(HALVES)]
        dg_links = [[send(dgt.at[h, 1 - place.core if 'c' in name else place.core], dgl.at[me, h], dev[name], *dg_sems[h]) for name in peers] for h in range(HALVES)]

        wait_for(xab.at[0:3 * tok, :], in_sems)
        gx[0].begin()
        gxa.begin_core()
        for link in routes:
            link.start()
        gtb[me] = gtab[place.flat['']]
        for ws in weights:
            for w in ws:
                w.start()
        dgc[...] = jnp.zeros_like(dgc)
        gcol[...] = jnp.zeros_like(gcol)
        wait_for(xab, aw_sems)

        def pairs(names, between=None):
            for k, name in enumerate(names):
                attention_qkv(xab, wqkv, qkv.at[k], place.chips[name], tok)
            if between is not None:
                between()
            for k, name in enumerate(names):
                attention_out(qkv.at[k], wo, at_part, place.chips[name], NUM_DEV // 2, attn_dims)

        gxa.crossed(0)
        pairs(('',))
        gx[0].relay()
        wait_for(gtb.at[0:7], routes_in)
        wide = jnp.concatenate([gtb[...].reshape(NUM_DEV * 8, LANES), jnp.zeros((LANES - NUM_DEV * 8, LANES), F32)], axis=0).T
        for h in range(HALVES):
            for b in range(NUM_DEV):
                gcol[h, b * r:(b + 1) * r, 0:8] = wide[h * r:(h + 1) * r, b * 8:(b + 1) * 8]
            for e in range(exp_loc):
                gfull[h, e] = jnp.broadcast_to(gcol[h][:, e:e + 1], (m, LANES))
        gx[0].relay_left()
        gxa.begin_links()
        gx[0].last()
        gx[0].finish()

        def staged(h, e, k):
            part = pl.ds(h * m, m)
            if k == 2:
                slot = h * 2 + lax.rem(e, 2)
                return pltpu.make_async_copy(stage_t.at[slot], ht_all.at[e, :, part], stage_sems.at[slot])
            return pltpu.make_async_copy((da, db)[k].at[e], (da_all, db_all)[k].at[e, part, :], grad_sems.at[e])

        lane = lax.broadcasted_iota(jnp.int32, (m, LANES), 1)

        def gate_of(h, e):
            return jnp.concatenate([gfull[h, e]] * (tile // LANES), axis=1)

        def loop(count, events, body):
            def step(k, _):
                for at, event in events.items():
                    pl.when(k == at)(event)
                body(k)
                return 0

            lax.fori_loop(0, count, step, 0)

        def hidden(h):
            def body(e):
                if h == 0:
                    wait_for(wg.at[0:3], w_sems.at[e])

                @pl.when(e >= 2)
                def _():
                    staged(h, e - 2, 2).wait()

                mask = gate_of(h, e) > 0.0
                a = jnp.where(mask, dot_nn(xb[h], wg[e]), 0.0)
                b = jnp.where(mask, dot_nn(xb[h], wu[e]), 0.0)
                sig = jax.nn.sigmoid(a)
                act = a * sig
                hid[e] = (act * b).astype(BF16)
                stage_t[h * 2 + lax.rem(e, 2)] = hid[e].T
                s1[e] = b * sig * (1.0 + a * (1.0 - sig))
                s2[e] = act
                staged(h, e, 2).start()

            return body

        def outputs(h):
            def body(n):
                cols = pl.ds(pl.multiple_of(n * tile, tile), tile)
                dy = dyb[h, :, cols].astype(F32)
                sums = dgc[h]
                for e in range(exp_loc):
                    o = dot_nn(hid[e], wd[e, :, cols]).astype(BF16).astype(F32)
                    y = gate_of(h, e) * o
                    y_part[h, :, cols] = y if e == 0 else y_part[h, :, cols] + y
                    prod = dy * o
                    dots = prod[:, 0:LANES]
                    for k in range(1, tile // LANES):
                        dots += prod[:, k * LANES:(k + 1) * LANES]
                    sums += jnp.where(lane == e, jnp.sum(dots, axis=1, keepdims=True), 0.0)
                dgc[h] = sums

            return body

        def hidden_grads(h):
            def body(e):
                if h:
                    wait_for(da.at[0:2], grad_sems.at[e])
                for n in range(tiles):
                    cols = pl.ds(n * tile, tile)
                    d_o[:, cols] = (gate_of(h, e) * dyb[h, :, cols].astype(F32)).astype(BF16)
                dh = dot_nt(d_o[...], wd[e]).astype(BF16).astype(F32)
                da[e] = (dh * s1[e]).astype(BF16)
                db[e] = (dh * s2[e]).astype(BF16)
                for k in range(2):
                    staged(h, e, k).start()

            return body

        def input_grads(h):
            def body(n):
                cols = pl.ds(pl.multiple_of(n * tile, tile), tile)
                for e in range(exp_loc):
                    dxe = (dot_nt(da[e], wg[e, cols, :]) + dot_nt(db[e], wu[e, cols, :])).astype(BF16).astype(F32)
                    dx_part[h, :, cols] = dxe if e == 0 else dx_part[h, :, cols] + dxe

            return body

        def send_dg(h):
            turned = dgc[h].T
            for c in range(2):
                dgt[h, c] = turned[0:8, c * LANES:(c + 1) * LANES]
            for link in dg_links[h]:
                link.start()
            dgl[me, h] = dgt[h, place.core]

        def dg_read():
            for h in range(HALVES):
                wait_for(gtb.at[0:7], dg_sems[h][1])
            for h in range(HALVES):
                slots = idx_in[:, h * r:(h + 1) * r]
                total = jnp.zeros(slots.shape, F32)
                for b in range(NUM_DEV):
                    first = ((b // 2) % 2 * 4 + b % 2 * 2 + b // 4) * exp_loc
                    rows = dgl[b, h]
                    mine = jnp.zeros((8, r), F32)
                    for q in range(LANES // r):
                        mine = jnp.where(place.chip == q, rows[:, q * r:(q + 1) * r], mine)
                    for e in range(exp_loc):
                        total = jnp.where(slots == first + e, mine[e:e + 1, :], total)
                dg_res[:, h * r:(h + 1) * r] = total

        def seq(*calls):
            def run():
                for call in calls:
                    call()

            return run

        loop(exp_loc, {2: gdy[0].begin, 3: gxa.relay}, hidden(0))
        gxa.crossed(1)
        gxa.crossed(2)
        pairs(('x', 'y'), gdy[0].relay)
        gx[1].begin()
        gxa.last()
        gdy[1].begin()
        gxa.crossed(3)
        pairs(('yx',), gdy[0].last)
        sat.begin()
        gdy[0].finish()
        loop(tiles, {1: seq(gx[1].relay, sy[0][0].begin), 2: seq(gdy[1].relay, sat.middle, sy[0][1].begin)}, outputs(0))
        sy[0][2].begin()
        send_dg(0)
        loop(exp_loc, {1: sy[0][0].middle, 2: gx[1].last, 3: sy[0][1].middle, 4: sy[0][2].middle}, hidden_grads(0))
        loop(tiles, {1: seq(gx[1].finish, sdx[0][0].begin), 2: seq(gdy[1].last, sdx[0][1].begin)}, input_grads(0))
        sdx[0][2].begin()
        loop(exp_loc, {1: seq(sdx[0][0].middle, sdx[0][1].middle), 2: seq(gdy[1].finish, sdx[0][2].middle)}, hidden(1))
        sat.late()
        loop(tiles, {1: seq(sy[0][0].late, sy[1][0].begin), 2: seq(sy[0][1].late, sy[0][2].late, sy[1][1].begin)}, outputs(1))
        sy[1][2].begin()
        send_dg(1)
        for h in range(HALVES):
            xt[:, h * m:(h + 1) * m] = xb[h].T
        saves = [pltpu.make_async_copy(xt, xt_all, out_sems.at[0]), pltpu.make_async_copy(dyb, dy_all, out_sems.at[1]), pltpu.make_async_copy(gcol, gates_out, out_sems.at[2])]
        for save in saves:
            save.start()
        loop(exp_loc, {0: sdx[0][0].late, 1: seq(sy[1][0].middle, sdx[0][1].late), 3: seq(sy[1][1].middle, sy[1][2].middle, sdx[0][2].late)}, hidden_grads(1))
        loop(tiles, {1: sdx[1][0].begin, 2: seq(sdx[1][1].begin, sdx[1][0].middle)}, input_grads(1))
        sdx[1][2].begin()
        sdx[1][1].middle()
        for s in sy[0]:
            s.finish(y_res)
        sat.finish(attn_res)
        for s in sdx[0]:
            s.finish(dx_res)
        dg_read()
        results = [pltpu.make_async_copy(src, dst, res_sems.at[k]) for k, (src, dst) in enumerate(((y_res, y_out), (dx_res, dx_out), (attn_res, attn_out), (dg_res, dg_out)))]
        for result in results:
            result.start()
        sdx[1][2].middle()
        for save in saves + results:
            save.wait()
        for e in range(exp_loc):
            wait_for(da.at[0:2], grad_sems.at[e])
        for h in range(HALVES):
            for e in (exp_loc - 2, exp_loc - 1):
                staged(h, jnp.int32(e), 2).wait()
        for item in gx + gdy + [gxa, sat] + sum(sy + sdx, []):
            item.drain()
        for sem in (routes_sent, dg_sems[0][0], dg_sems[1][0]):
            wait_for(gtb.at[0:7], sem)
        assert pool.used == NUM_SEMS, pool.used

    return kernel, r, m


def weight_grads(width, slots, xt_in, dy_in, g_in, da_in, db_in, ht_in, at_in, dg_in, y_in, dx_in,
                 dwg, dwu, dwd, at_out, dg_out, y_out, dx_out,
                 xt, dy, g, da, db, ht, sg, su, sd, at, dg, y, dx, x_sems, d_sems, g_sem, e_sems, o_sems, p_sems):
    exp_loc = da.shape[0]
    steps = dy.shape[1] // width

    def load(e, k):
        src, dst = ((da_in, da), (db_in, db), (ht_in, ht))[k]
        return pltpu.make_async_copy(src.at[e], dst.at[e], e_sems.at[e, k])

    def x_load(n):
        rows = slice(n * width, (n + 1) * width)
        return pltpu.make_async_copy(xt_in.at[rows, :], xt.at[rows, :], x_sems.at[n])

    def dy_load(n):
        cols = slice(n * width, (n + 1) * width)
        return pltpu.make_async_copy(dy_in.at[:, cols], dy.at[:, cols], d_sems.at[n])

    g_load = pltpu.make_async_copy(g_in, g, g_sem)
    x_load(0).start()
    load(0, 0).start()
    load(0, 1).start()
    for n in range(1, steps):
        x_load(n).start()
    load(0, 2).start()
    g_load.start()
    for n in range(steps):
        dy_load(n).start()
    for e in range(1, exp_loc):
        for k in range(3):
            load(e, k).start()
    rows = slice(0, y.shape[0])
    passing = ((at_in, at, at_out), (dg_in, dg, dg_out), (y_in, y, y_out.at[rows, :]), (dx_in, dx, dx_out.at[rows, :]))
    take = [pltpu.make_async_copy(src, mid, p_sems.at[k, 0]) for k, (src, mid, _) in enumerate(passing)]
    give = [pltpu.make_async_copy(mid, dst, p_sems.at[k, 1]) for k, (_, mid, dst) in enumerate(passing)]
    for copy in take:
        copy.start()

    def store(e, n, k):
        part = pl.ds(n * width, width)
        n = lax.rem(e, 2) * steps + n
        if k == 2:
            return pltpu.make_async_copy(sd.at[n], dwd.at[e, :, part], o_sems.at[n, k])
        return pltpu.make_async_copy((sg, su)[k].at[n], (dwg, dwu)[k].at[e, part, :], o_sems.at[n, k])

    lane = lax.broadcasted_iota(jnp.int32, g.shape, 1)

    def down(e):
        gate = jnp.sum(jnp.where(lane == e, g[...], 0.0), axis=1, keepdims=True)
        for n in range(steps):
            part = pl.ds(n * width, width)
            sd[lax.rem(e, 2) * steps + n] = dot_nn(ht[e], (gate * dy[:, part].astype(F32)).astype(BF16))
            store(e, n, 2).start()

    def step(e, _):
        @pl.when(e == 0)
        def _():
            load(e, 0).wait()
            load(e, 1).wait()
            for n in range(steps):
                x_load(n).wait()

        @pl.when(e > 0)
        def _():
            for k in range(3):
                load(e, k).wait()

        @pl.when(e > 1)
        def _():
            for n in range(steps):
                for k in range(2):
                    store(e - 2, n, k).wait()

        for n in range(steps):
            part = pl.ds(n * width, width)
            sg[lax.rem(e, 2) * steps + n] = dot_nn(xt[part, :], da[e])
            store(e, n, 0).start()
            su[lax.rem(e, 2) * steps + n] = dot_nn(xt[part, :], db[e])
            store(e, n, 1).start()

        @pl.when(e == 0)
        def _():
            load(e, 2).wait()
            g_load.wait()
            for n in range(steps):
                dy_load(n).wait()

        @pl.when(e > 1)
        def _():
            for n in range(steps):
                store(e - 2, n, 2).wait()

        @pl.when(e == 1)
        def _():
            for copy in take:
                copy.wait()
            for copy in give:
                copy.start()

        down(e)
        return 0

    lax.fori_loop(0, exp_loc, step, 0)
    for e in (exp_loc - 2, exp_loc - 1):
        for n in range(steps):
            for k in range(3):
                store(jnp.int32(e), n, k).wait()
    for copy in give:
        copy.wait()


def solution(mesh):
    num_dev = mesh.shape['ei'] * mesh.shape['eo']
    assert num_dev == NUM_DEV

    def local_step(x_tokens, expert_idx, gate_vals, dy_tokens, w_gate, w_up, w_down, x_attn, w_query, w_key, w_value, w_out):
        tok, d_model = x_tokens.shape
        top_k = expert_idx.shape[1]
        exp_loc, _, d_ff = w_gate.shape
        seq = x_attn.shape[1]
        heads, head_dim = w_query.shape[1], w_query.shape[2]
        kv_dim = w_key.shape[1] * head_dim
        q_dim = heads * head_dim
        wq = w_query.transpose(1, 2, 0).reshape(q_dim, d_model)
        wk = w_key.transpose(1, 2, 0).reshape(kv_dim, d_model)
        wv = w_value.transpose(1, 2, 0).reshape(kv_dim, d_model)
        wo = w_out.reshape(q_dim, d_model)
        kernel, r, m = make_layer_kernel(tok, d_model, d_ff, exp_loc, (seq, kv_dim, heads, head_dim))
        any_spec = pl.BlockSpec(memory_space=pl.ANY)
        vmem_spec = pl.BlockSpec(memory_space=pltpu.VMEM)
        shape = jax.ShapeDtypeStruct
        total = tok * NUM_DEV

        def half_shapes():
            return [pltpu.VMEM((d_model // 512,) + s.shape, s.dtype) for s in scatter_shapes(r, 512)]

        y0, dx0, attn, dgt, xt, dy_all, da, db, ht, gates, own, to_x, to_y, to_d = pl.pallas_call(
            kernel,
            out_shape=(shape((r, d_model), BF16), shape((r, d_model), BF16), shape((tok, d_model), BF16), shape((top_k, tok), F32),
                       shape((d_model, total), BF16), shape((HALVES, m, d_model), BF16),
                       shape((exp_loc, total, d_ff), BF16), shape((exp_loc, total, d_ff), BF16), shape((exp_loc, d_ff, total), BF16), shape((HALVES, m, LANES), F32)) + (shape((2, r, d_model), F32),) * 4,
            in_specs=[any_spec, any_spec, any_spec, vmem_spec, vmem_spec] + [any_spec] * 7,
            out_specs=(any_spec,) * 14,
            scratch_shapes=[pltpu.VMEM((HALVES, m, d_model), BF16), pltpu.VMEM((HALVES, m, d_model), BF16), pltpu.VMEM((total, d_model), BF16),
                            pltpu.VMEM((NUM_DEV, 8, LANES), F32), pltpu.VMEM((HALVES, m, LANES), F32),
                            pltpu.VMEM((exp_loc, d_model, d_ff), BF16), pltpu.VMEM((exp_loc, d_model, d_ff), BF16), pltpu.VMEM((exp_loc, d_ff, d_model), BF16),
                            pltpu.VMEM((HALVES, m, d_model), F32), pltpu.VMEM((HALVES, m, d_model), F32), pltpu.VMEM((total, d_model), F32), pltpu.VMEM((q_dim + 2 * kv_dim, d_model), BF16), pltpu.VMEM((q_dim, d_model), BF16), pltpu.VMEM((2, 2 * tok, q_dim + 2 * kv_dim), BF16),
                            pltpu.VMEM((exp_loc, m, d_ff), F32), pltpu.VMEM((exp_loc, m, d_ff), F32), pltpu.VMEM((m, d_model), BF16),
                            pltpu.VMEM((HALVES, m, LANES), F32), pltpu.VMEM((HALVES, 2, 8, LANES), F32), pltpu.VMEM((exp_loc, m, d_ff), BF16), pltpu.VMEM((exp_loc, m, d_ff), BF16),
                            pltpu.VMEM((exp_loc, m, d_ff), BF16), pltpu.VMEM((2 * HALVES, d_ff, m), BF16), pltpu.VMEM((d_model, total), BF16), pltpu.VMEM((NUM_DEV, HALVES, 8, LANES), F32), pltpu.VMEM((NUM_DEV, 8, LANES), F32), pltpu.VMEM((HALVES, exp_loc, m, LANES), F32)]
            + [pltpu.VMEM((d_model // 512, 4 * r, 512), F32)] * 2 + half_shapes() + half_shapes() + scatter_shapes(tok, d_model)
            + [pltpu.SemaphoreType.DMA((NUM_SEMS,)), pltpu.SemaphoreType.DMA((exp_loc,)),
               pltpu.SemaphoreType.DMA(()), pltpu.SemaphoreType.DMA(()), pltpu.SemaphoreType.DMA((3,)), pltpu.SemaphoreType.DMA((2 * HALVES,)), pltpu.SemaphoreType.DMA((exp_loc,)), pltpu.SemaphoreType.DMA((2, d_model // 512)), pltpu.SemaphoreType.DMA((4,)),
               pltpu.VMEM((r, d_model), BF16), pltpu.VMEM((r, d_model), BF16), pltpu.VMEM((tok, d_model), BF16), pltpu.VMEM((top_k, tok), F32)],
            compiler_params=pltpu.CompilerParams(collective_id=0, has_side_effects=True, vmem_limit_bytes=67000000),
            name='layer',
        )(x_tokens, dy_tokens, x_attn.reshape(tok, d_model), expert_idx.T, gate_vals.T, w_gate, w_up, w_down, wq, wk, wv, wo)

        width = 512
        steps = d_model // width
        slots = 2 * steps
        small = (attn, dgt, y0, dx0)

        def swap(value, flip_y, flip_x):
            eo_size = mesh.shape['eo']
            pairs = [(g, (g // eo_size ^ flip_y) * eo_size + (g % eo_size ^ 2 * flip_x)) for g in range(NUM_DEV)]
            return lax.ppermute(value, GROUP_AXES, pairs)

        from_x, from_y, from_d = swap(to_x, 0, 1), swap(to_y, 1, 0), swap(to_d, 1, 1)
        dw_gate, dw_up, dw_down, attn, dgt, y, dx = pl.pallas_call(
            functools.partial(weight_grads, width, slots),
            out_shape=(shape((exp_loc, d_model, d_ff), F32), shape((exp_loc, d_model, d_ff), F32), shape((exp_loc, d_ff, d_model), F32)) + tuple(shape((tok, d_model) if v is y0 or v is dx0 else v.shape, v.dtype) for v in small),
            in_specs=[any_spec] * 10,
            out_specs=(any_spec,) * 7,
            scratch_shapes=[pltpu.VMEM((d_model, total), BF16), pltpu.VMEM((total, d_model), BF16), pltpu.VMEM((total, LANES), F32),
                            pltpu.VMEM((exp_loc, total, d_ff), BF16), pltpu.VMEM((exp_loc, total, d_ff), BF16), pltpu.VMEM((exp_loc, d_ff, total), BF16),
                            pltpu.VMEM((slots, width, d_ff), F32), pltpu.VMEM((slots, width, d_ff), F32), pltpu.VMEM((slots, d_ff, width), F32)]
            + [pltpu.VMEM(v.shape, v.dtype) for v in small]
            + [pltpu.SemaphoreType.DMA((steps,)), pltpu.SemaphoreType.DMA((steps,)), pltpu.SemaphoreType.DMA(()), pltpu.SemaphoreType.DMA((exp_loc, 3)),
               pltpu.SemaphoreType.DMA((slots, 3)), pltpu.SemaphoreType.DMA((4, 2))],
            compiler_params=pltpu.CompilerParams(vmem_limit_bytes=64500000),
            cost_estimate=pl.CostEstimate(flops=3 * 2 * total * d_model * d_ff * exp_loc, bytes_accessed=3 * 4 * exp_loc * d_model * d_ff, transcendentals=0),
            name='weight_grads',
        )(xt, dy_all.reshape(total, d_model), gates.reshape(total, LANES), da, db, ht, attn, dgt, y0, dx0)
        y, dx = (lax.dynamic_update_slice(whole, (own[t] + from_x[t] + from_y[t] + from_d[t]).astype(BF16), (r, 0)) for t, whole in enumerate((y, dx)))
        return y, dx, dgt.T, dw_gate, dw_up, dw_down, attn.reshape(x_attn.shape)

    spec_rows = P(TOKEN_AXES, None)
    spec_seqs = P(TOKEN_AXES, None, None)
    spec_experts = P(GROUP_AXES, None, None)
    spec_heads = P(None, GROUP_AXES, None)
    return jax.shard_map(local_step, mesh=mesh,
                         in_specs=(spec_rows, spec_rows, spec_rows, spec_rows, spec_experts, spec_experts, spec_experts, spec_seqs, spec_heads, spec_heads, spec_heads, spec_experts),
                         out_specs=(spec_rows, spec_rows, spec_rows, spec_seqs, spec_seqs, spec_seqs, spec_seqs),
                         check_vma=False)
```

```python
import functools

import jax
import jax.numpy as jnp
from jax import lax
from jax.experimental import pallas as pl
from jax.experimental.pallas import tpu as pltpu
from jax.sharding import PartitionSpec as P

GROUP_AXES = ('ei', 'eo')
TOKEN_AXES = ('dp', 'ei', 'eo')
F32 = jnp.float32
BF16 = jnp.bfloat16
MESH_ID = pl.DeviceIdType.MESH
HALVES = 2
NUM_DEV = 8
LANES = 128


def dot_nn(lhs, rhs):
    return jnp.dot(lhs, rhs, preferred_element_type=F32)


def dot_nt(lhs, rhs):
    return lax.dot_general(lhs, rhs, (((1,), (1,)), ((), ())), preferred_element_type=F32)


def dot_tn(lhs, rhs):
    return lax.dot_general(lhs, rhs, (((0,), (0,)), ((), ())), preferred_element_type=F32)


class Place:
    def __init__(self):
        i = lax.axis_index('ei')
        o = lax.axis_index('eo')
        x = lax.div(o, 2)
        c = lax.rem(o, 2)
        self.core = c
        self.chip = i * 2 + x
        self.dev = {}
        self.block = {}
        self.flat = {}
        self.pair = {}
        self.chips = {}
        for flip_y in (0, 1):
            for flip_x in (0, 1):
                for flip_c in (0, 1):
                    yy = 1 - i if flip_y else i
                    xx = 1 - x if flip_x else x
                    cc = 1 - c if flip_c else c
                    name = ('y' if flip_y else '') + ('x' if flip_x else '') + ('c' if flip_c else '')
                    self.dev[name] = (0, yy, xx * 2 + cc)
                    self.block[name] = cc * 4 + yy * 2 + xx
                    self.flat[name] = yy * 4 + xx * 2 + cc
                    self.pair[name] = (yy * 2 + xx) * 2 + cc
                    self.chips[name] = yy * 2 + xx


class Pool:
    def __init__(self, sems):
        self.sems, self.used = sems, 0

    def take(self):
        self.used += 1
        return self.sems.at[self.used - 1]


def send(src, dst, device, sent, landed):
    return pltpu.make_async_remote_copy(src_ref=src, dst_ref=dst, send_sem=sent, recv_sem=landed, device_id=device, device_id_type=MESH_ID)


def wait_for(ref, sem):
    pltpu.make_async_copy(ref, ref, sem).wait()


class Gather:
    def __init__(self, pool, place, buf, rows, index, split=False):
        def at(name, lo=0, n=rows):
            return buf.at[pl.ds(pl.multiple_of(index[name] * rows + lo, 8), n), :]

        half = rows // 2
        own = at('')
        dev = place.dev
        self.buf, self.rows, self.relayed = buf, rows, False
        self.sent, self.relays_sent, self.near, self.relays = (pool.take() for _ in range(4))
        self.over = [pool.take() for _ in range(4)] if split else [pool.take()] * 4
        self.to_x = send(own, own, dev['x'], self.sent, self.near)
        self.to_y = send(own, own, dev['y'], self.sent, self.near)
        self.to_c = send(own, own, dev['c'], self.sent, self.over[0])
        self.relay_x = send(at('y', 0, half), at('y', 0, half), dev['x'], self.relays_sent, self.relays)
        self.relay_y = send(at('x', half, half), at('x', half, half), dev['y'], self.relays_sent, self.relays)
        self.core_x = send(at('x'), at('x'), dev['c'], self.sent, self.over[1])
        self.core_y = send(at('y'), at('y'), dev['c'], self.sent, self.over[2])
        self.core_d = send(at('yx'), at('yx'), dev['c'], self.sent, self.over[3])

    def blocks(self, count):
        return self.buf.at[0:count * self.rows, :]

    def begin_links(self):
        self.to_x.start()
        self.to_y.start()

    def begin_core(self):
        self.to_c.start()

    def begin(self):
        self.begin_links()
        self.begin_core()

    def relay(self):
        wait_for(self.blocks(2), self.near)
        self.relay_x.start()
        self.relay_y.start()
        self.core_x.start()
        self.core_y.start()

    def relay_left(self):
        self.relayed = True
        wait_for(self.blocks(1), self.relays_sent)

    def last(self):
        wait_for(self.blocks(1), self.relays)
        self.core_d.start()

    def crossed(self, k):
        wait_for(self.blocks(1), self.over[k])

    def finish(self):
        wait_for(self.blocks(4), self.over[0])

    def drain(self):
        wait_for(self.blocks(6), self.sent)
        if not self.relayed:
            wait_for(self.blocks(1), self.relays_sent)


class Scatter:
    def __init__(self, pool, place, part, from_core, from_x, from_y, last_x, last_y, rows, first=0):
        half = rows // 2
        self.half, self.part, self.rows, self.place = half, part, rows, place
        self.from_core, self.from_x, self.from_y, self.last_x, self.last_y = from_core, from_x, from_y, last_x, last_y
        four = 4 * rows
        self.mine = pl.multiple_of(place.core * four, 8)
        self.cols = pl.ds(first, from_core.shape[-1])
        other = part.at[pl.ds(pl.multiple_of((1 - place.core) * four, 8), four), self.cols]
        dev = place.dev
        self.sent, self.crossed, self.first_x, self.first_y, self.rest = (pool.take() for _ in range(5))
        self.core = send(other, from_core, dev['c'], self.sent, self.crossed)
        self.x0 = send(self.at('x', 0), from_x.at[0], dev['x'], self.sent, self.rest)
        self.x1 = send(self.at('yx', 0), from_x.at[1], dev['x'], self.sent, self.first_x)
        self.y0 = send(self.at('y', half), from_y.at[0], dev['y'], self.sent, self.rest)
        self.y1 = send(self.at('yx', half), from_y.at[1], dev['y'], self.sent, self.first_y)
        self.end_y = send(self.at('y', 0), last_y, dev['y'], self.sent, self.rest)
        self.end_x = send(self.at('x', half), last_x, dev['x'], self.sent, self.rest)

    def at(self, name, lo):
        return self.part.at[pl.ds(pl.multiple_of(self.place.block[name] * self.rows + lo, 8), self.half), self.cols]

    def begin(self):
        self.core.start()

    def middle(self):
        wait_for(self.from_core, self.crossed)
        mine = pl.ds(self.mine, 4 * self.rows)
        self.part[mine, self.cols] = self.part[mine, self.cols] + self.from_core[...]
        self.x1.start()
        self.y1.start()
        self.x0.start()
        self.y0.start()

    def late(self):
        wait_for(self.from_x.at[1], self.first_x)
        here = self.at('y', 0)
        here[...] = here[...] + self.from_x[1]
        self.end_y.start()
        wait_for(self.from_y.at[1], self.first_y)
        here = self.at('x', self.half)
        here[...] = here[...] + self.from_y[1]
        self.end_x.start()

    def finish(self, out, row=0):
        half = self.half
        wait_for(self.part.at[0:4 * half, self.cols], self.rest)
        out[row:row + half, self.cols] = (self.at('', 0)[...] + self.from_x[0] + self.last_y[...]).astype(BF16)
        out[row + half:row + 2 * half, self.cols] = (self.at('', half)[...] + self.from_y[0] + self.last_x[...]).astype(BF16)

    def drain(self):
        wait_for(self.part.at[0:7 * self.rows, self.cols], self.sent)


class ChipSum:
    def __init__(self, pool, place, part, from_core, rows, first, outs, sem):
        four = 4 * rows
        self.part, self.from_core, self.sem = part, from_core, sem
        self.mine = pl.multiple_of(place.core * four, 8)
        self.cols = pl.ds(first, from_core.shape[-1])
        other = part.at[pl.ds(pl.multiple_of((1 - place.core) * four, 8), four), self.cols]
        self.sent, self.crossed = pool.take(), pool.take()
        self.core = send(other, from_core, place.dev['c'], self.sent, self.crossed)
        self.copies = [pltpu.make_async_copy(part.at[pl.ds(pl.multiple_of(place.block[name] * rows, 8), rows), self.cols], out, sem)
                       for name, out in outs]

    def begin(self):
        self.core.start()

    def middle(self):
        wait_for(self.from_core, self.crossed)
        mine = pl.ds(self.mine, self.from_core.shape[0])
        self.part[mine, self.cols] = self.part[mine, self.cols] + self.from_core[...]
        for copy in self.copies:
            copy.start()

    def drain(self):
        wait_for(self.from_core, self.sent)
        wait_for(self.from_core, self.sem)


def scatter_shapes(rows, width):
    half = rows // 2
    return [pltpu.VMEM((4 * rows, width), F32), pltpu.VMEM((2, half, width), F32), pltpu.VMEM((2, half, width), F32),
            pltpu.VMEM((half, width), F32), pltpu.VMEM((half, width), F32)]


NUM_SEMS = 2 + 4 + 5 * 4 + 8 + 5 * 6 + 2 * 7


def attention_qkv(xa, wqkv, qkv, chip, seq):
    pair = 2 * seq
    qkv[...] = dot_nt(xa[pl.ds(pl.multiple_of(chip * pair, pair), pair), :], wqkv[...]).astype(BF16)


def attention_out(qkv, wo, part, chip, chips, dims):
    seq, kv_dim, heads, head_dim = dims
    q_dim = heads * head_dim
    pair = 2 * seq
    row = lax.broadcasted_iota(jnp.int32, (pair, pair), 0)
    col = lax.broadcasted_iota(jnp.int32, (pair, pair), 1)
    causal = (row >= col) & ((row >= seq) == (col >= seq))
    keys = qkv[:, q_dim:q_dim + kv_dim]
    vals = qkv[:, q_dim + kv_dim:q_dim + 2 * kv_dim]
    outs = []
    for h in range(heads):
        scores = dot_nt(qkv[:, h * head_dim:(h + 1) * head_dim], keys) * head_dim ** -0.5
        scores = jnp.where(causal, scores, -1e30)
        top = jnp.max(scores, axis=1, keepdims=True)
        ex = jnp.exp(scores - top)
        probs = (ex / jnp.sum(ex, axis=1, keepdims=True)).astype(BF16)
        outs.append(dot_nn(probs, vals).astype(BF16))
    out = dot_nn(jnp.concatenate(outs, axis=1), wo[...])
    for c in range(2):
        part[pl.ds(pl.multiple_of((c * chips + chip) * seq, seq), seq), :] = out[c * seq:(c + 1) * seq, :]


def make_layer_kernel(tok, d_model, d_ff, exp_loc, attn_dims):
    r = tok // HALVES
    m = r * NUM_DEV
    tile = 512
    tiles = d_model // tile

    def kernel(x_in, dy_in, xa_in, idx_in, gate_in, wg_in, wu_in, wd_in, wq_in, wk_in, wv_in, wo_in,
               y_out, dx_out, attn_out, dg_out, xt_all, dy_all, da_all, db_all, ht_all, gates_out, own_out, to_x_out, to_y_out, to_d_out,
               xb, dyb, xab, gtb, gcol, wg, wu, wd, y_part, dx_part, at_part, wqkv, wo, qkv, s1, s2, d_o, dgc, dgt, da, db, hid, stage_t, xt, dgl, gtab, gfull,
               ryc, rdc, ry0, ry1, ry2, ry3, ry4, rd0, rd1, rd2, rd3, rd4, ra0, ra1, ra2, ra3, ra4,
               sems, w_sems, in_sems, aw_sems, out_sems, stage_sems, grad_sems, sum_sems, res_sems, y_res, dx_res, attn_res, dg_res):
        place = Place()
        pool = Pool(sems)
        dev, block = place.dev, place.block
        me = block['']

        def own_rows(buf, rows, index=me):
            return buf.at[pl.ds(pl.multiple_of(index * rows, 8), rows), :]

        loads = []
        for h in range(HALVES):
            loads.append(pltpu.make_async_copy(x_in.at[h * r:(h + 1) * r, :], own_rows(xb.at[h], r), in_sems))
            loads.append(pltpu.make_async_copy(dy_in.at[h * r:(h + 1) * r, :], own_rows(dyb.at[h], r), in_sems))
        loads.append(pltpu.make_async_copy(xa_in, own_rows(xab, tok, place.pair['']), in_sems))
        for load in loads:
            load.start()
        q_dim, kv_dim = wq_in.shape[0], wk_in.shape[0]
        attn_loads = [pltpu.make_async_copy(wq_in, wqkv.at[0:q_dim, :], aw_sems), pltpu.make_async_copy(wk_in, wqkv.at[q_dim:q_dim + kv_dim, :], aw_sems),
                      pltpu.make_async_copy(wv_in, wqkv.at[q_dim + kv_dim:q_dim + 2 * kv_dim, :], aw_sems), pltpu.make_async_copy(wo_in, wo, aw_sems)]
        for load in attn_loads:
            load.start()
        weights = []
        for e in range(exp_loc):
            weights.append([pltpu.make_async_copy(src.at[e], dst.at[e], w_sems.at[e]) for src, dst in ((wg_in, wg), (wu_in, wu), (wd_in, wd))])
        barrier = pltpu.get_barrier_semaphore()
        peers = [name for name in dev if name]
        for name in peers:
            pl.semaphore_signal(barrier, inc=1, device_id=dev[name], device_id_type=MESH_ID)
        gtab[...] = jnp.zeros_like(gtab)
        for g in range(NUM_DEV):
            for e in range(exp_loc):
                gtab[g, e:e + 1, 0:tok] = jnp.sum(jnp.where(idx_in[...] == g * exp_loc + e, gate_in[...], 0.0), axis=0, keepdims=True)
        pl.semaphore_wait(barrier, len(peers))

        routes_sent, routes_in = pool.take(), pool.take()
        routes = [send(gtab.at[place.flat[name]], gtb.at[me], dev[name], routes_sent, routes_in) for name in peers]
        gx = [Gather(pool, place, xb.at[h], r, block) for h in range(HALVES)]
        gdy = [Gather(pool, place, dyb.at[h], r, block) for h in range(HALVES)]
        gxa = Gather(pool, place, xab, tok, place.pair, split=True)
        def passed(k):
            return [(name, out.at[:, k * tile:(k + 1) * tile]) for name, out in (('', own_out), ('x', to_x_out), ('y', to_y_out), ('yx', to_d_out))]

        def chip_sum(part, from_core, n, k):
            return ChipSum(pool, place, part, from_core, r, n * tile, passed(k), sum_sems.at[k])

        sy = [[Scatter(pool, place, y_part.at[0], ry0.at[n], ry1.at[n], ry2.at[n], ry3.at[n], ry4.at[n], r, n * tile) for n in range(tiles)],
              [chip_sum(y_part.at[1], ryc.at[n], n, n) for n in range(tiles)]]
        sdx = [[Scatter(pool, place, dx_part.at[0], rd0.at[n], rd1.at[n], rd2.at[n], rd3.at[n], rd4.at[n], r, n * tile) for n in range(tiles - 1)]
               + [chip_sum(dx_part.at[0], rd0.at[tiles - 1], tiles - 1, 2 * tiles)],
               [chip_sum(dx_part.at[1], rdc.at[n], n, tiles + n) for n in range(tiles)]]
        sat = Scatter(pool, place, at_part, ra0, ra1, ra2, ra3, ra4, tok)
        dg_sems = [(pool.take(), pool.take()) for _ in range(HALVES)]
        dg_links = [[send(dgt.at[h, 1 - place.core if 'c' in name else place.core], dgl.at[me, h], dev[name], *dg_sems[h]) for name in peers] for h in range(HALVES)]

        wait_for(xab.at[0:3 * tok, :], in_sems)
        gx[0].begin()
        gxa.begin_core()
        for link in routes:
            link.start()
        gtb[me] = gtab[place.flat['']]
        for ws in weights:
            for w in ws:
                w.start()
        dgc[...] = jnp.zeros_like(dgc)
        gcol[...] = jnp.zeros_like(gcol)
        wait_for(xab, aw_sems)

        def pairs(names, between=None):
            for k, name in enumerate(names):
                attention_qkv(xab, wqkv, qkv.at[k], place.chips[name], tok)
            if between is not None:
                between()
            for k, name in enumerate(names):
                attention_out(qkv.at[k], wo, at_part, place.chips[name], NUM_DEV // 2, attn_dims)

        gxa.crossed(0)
        pairs(('',))
        gx[0].relay()
        wait_for(gtb.at[0:7], routes_in)
        wide = jnp.concatenate([gtb[...].reshape(NUM_DEV * 8, LANES), jnp.zeros((LANES - NUM_DEV * 8, LANES), F32)], axis=0).T
        for h in range(HALVES):
            for b in range(NUM_DEV):
                gcol[h, b * r:(b + 1) * r, 0:8] = wide[h * r:(h + 1) * r, b * 8:(b + 1) * 8]
            for e in range(exp_loc):
                gfull[h, e] = jnp.broadcast_to(gcol[h][:, e:e + 1], (m, LANES))
        gx[0].relay_left()
        gxa.begin_links()
        gx[0].last()
        gx[0].finish()

        def staged(h, e, k):
            part = pl.ds(h * m, m)
            if k == 2:
                slot = h * 2 + lax.rem(e, 2)
                return pltpu.make_async_copy(stage_t.at[slot], ht_all.at[e, :, part], stage_sems.at[slot])
            return pltpu.make_async_copy((da, db)[k].at[e], (da_all, db_all)[k].at[e, part, :], grad_sems.at[e])

        lane = lax.broadcasted_iota(jnp.int32, (m, LANES), 1)

        def gate_of(h, e):
            return jnp.concatenate([gfull[h, e]] * (tile // LANES), axis=1)

        def loop(count, events, body):
            def step(k, _):
                for at, event in events.items():
                    pl.when(k == at)(event)
                body(k)
                return 0

            lax.fori_loop(0, count, step, 0)

        def hidden(h):
            def body(e):
                if h == 0:
                    wait_for(wg.at[0:3], w_sems.at[e])

                @pl.when(e >= 2)
                def _():
                    staged(h, e - 2, 2).wait()

                mask = gate_of(h, e) > 0.0
                a = jnp.where(mask, dot_nn(xb[h], wg[e]), 0.0)
                b = jnp.where(mask, dot_nn(xb[h], wu[e]), 0.0)
                sig = jax.nn.sigmoid(a)
                act = a * sig
                hid[e] = (act * b).astype(BF16)
                stage_t[h * 2 + lax.rem(e, 2)] = hid[e].T
                s1[e] = b * sig * (1.0 + a * (1.0 - sig))
                s2[e] = act
                staged(h, e, 2).start()

            return body

        def outputs(h):
            def body(n):
                cols = pl.ds(pl.multiple_of(n * tile, tile), tile)
                dy = dyb[h, :, cols].astype(F32)
                sums = dgc[h]
                for e in range(exp_loc):
                    o = dot_nn(hid[e], wd[e, :, cols]).astype(BF16).astype(F32)
                    y = gate_of(h, e) * o
                    y_part[h, :, cols] = y if e == 0 else y_part[h, :, cols] + y
                    prod = dy * o
                    dots = prod[:, 0:LANES]
                    for k in range(1, tile // LANES):
                        dots += prod[:, k * LANES:(k + 1) * LANES]
                    sums += jnp.where(lane == e, jnp.sum(dots, axis=1, keepdims=True), 0.0)
                dgc[h] = sums

            return body

        def hidden_grads(h):
            def body(e):
                if h:
                    wait_for(da.at[0:2], grad_sems.at[e])
                for n in range(tiles):
                    cols = pl.ds(n * tile, tile)
                    d_o[:, cols] = (gate_of(h, e) * dyb[h, :, cols].astype(F32)).astype(BF16)
                dh = dot_nt(d_o[...], wd[e]).astype(BF16).astype(F32)
                da[e] = (dh * s1[e]).astype(BF16)
                db[e] = (dh * s2[e]).astype(BF16)
                for k in range(2):
                    staged(h, e, k).start()

            return body

        def input_grads(h):
            def body(n):
                cols = pl.ds(pl.multiple_of(n * tile, tile), tile)
                for e in range(exp_loc):
                    dxe = (dot_nt(da[e], wg[e, cols, :]) + dot_nt(db[e], wu[e, cols, :])).astype(BF16).astype(F32)
                    dx_part[h, :, cols] = dxe if e == 0 else dx_part[h, :, cols] + dxe

            return body

        def send_dg(h):
            turned = dgc[h].T
            for c in range(2):
                dgt[h, c] = turned[0:8, c * LANES:(c + 1) * LANES]
            for link in dg_links[h]:
                link.start()
            dgl[me, h] = dgt[h, place.core]

        def dg_read():
            for h in range(HALVES):
                wait_for(gtb.at[0:7], dg_sems[h][1])
            for h in range(HALVES):
                slots = idx_in[:, h * r:(h + 1) * r]
                total = jnp.zeros(slots.shape, F32)
                for b in range(NUM_DEV):
                    first = ((b // 2) % 2 * 4 + b % 2 * 2 + b // 4) * exp_loc
                    rows = dgl[b, h]
                    mine = jnp.zeros((8, r), F32)
                    for q in range(LANES // r):
                        mine = jnp.where(place.chip == q, rows[:, q * r:(q + 1) * r], mine)
                    for e in range(exp_loc):
                        total = jnp.where(slots == first + e, mine[e:e + 1, :], total)
                dg_res[:, h * r:(h + 1) * r] = total

        def seq(*calls):
            def run():
                for call in calls:
                    call()

            return run

        loop(exp_loc, {0: gdy[0].begin, 3: gxa.relay}, hidden(0))
        gxa.crossed(1)
        gxa.crossed(2)
        pairs(('x', 'y'), seq(gdy[0].relay, gxa.last))
        gx[1].begin()
        gdy[1].begin()
        gxa.crossed(3)
        pairs(('yx',), gdy[0].last)
        sat.begin()
        gdy[0].finish()
        loop(tiles, {1: seq(gx[1].relay, sy[0][0].begin), 2: seq(gdy[1].relay, sat.middle, sy[0][1].begin)}, outputs(0))
        sy[0][2].begin()
        send_dg(0)
        loop(exp_loc, {1: sy[0][0].middle, 2: gx[1].last, 3: sy[0][1].middle, 4: sy[0][2].middle}, hidden_grads(0))
        loop(tiles, {1: seq(gx[1].finish, sdx[0][0].begin), 2: seq(gdy[1].last, sdx[0][1].begin)}, input_grads(0))
        sdx[0][2].begin()
        loop(exp_loc, {1: seq(sdx[0][0].middle, sdx[0][1].middle), 2: seq(gdy[1].finish, sdx[0][2].middle)}, hidden(1))
        sat.late()
        loop(tiles, {1: seq(sy[0][0].late, sy[1][0].begin), 2: seq(sy[0][1].late, sy[0][2].late, sy[1][1].begin)}, outputs(1))
        sy[1][2].begin()
        send_dg(1)
        for h in range(HALVES):
            xt[:, h * m:(h + 1) * m] = xb[h].T
        saves = [pltpu.make_async_copy(xt, xt_all, out_sems.at[0]), pltpu.make_async_copy(dyb, dy_all, out_sems.at[1]), pltpu.make_async_copy(gcol, gates_out, out_sems.at[2])]
        for save in saves:
            save.start()
        loop(exp_loc, {0: sdx[0][0].late, 1: seq(sy[1][0].middle, sdx[0][1].late), 3: seq(sy[1][1].middle, sy[1][2].middle)}, hidden_grads(1))
        loop(tiles, {1: sdx[1][0].begin, 2: seq(sdx[1][1].begin, sdx[1][0].middle)}, input_grads(1))
        sdx[1][2].begin()
        sdx[1][1].middle()
        for s in sy[0]:
            s.finish(y_res)
        sat.finish(attn_res)
        for s in sdx[0][:-1]:
            s.finish(dx_res)
        dx_res[:, (tiles - 1) * tile:] = jnp.zeros((r, tile), BF16)
        dg_read()
        results = [pltpu.make_async_copy(src, dst, res_sems.at[k]) for k, (src, dst) in enumerate(((y_res, y_out), (dx_res, dx_out), (attn_res, attn_out), (dg_res, dg_out)))]
        for result in results:
            result.start()
        sdx[1][2].middle()
        for save in saves + results:
            save.wait()
        for e in range(exp_loc):
            wait_for(da.at[0:2], grad_sems.at[e])
        for h in range(HALVES):
            for e in (exp_loc - 2, exp_loc - 1):
                staged(h, jnp.int32(e), 2).wait()
        for item in gx + gdy + [gxa, sat] + sum(sy + sdx, []):
            item.drain()
        for sem in (routes_sent, dg_sems[0][0], dg_sems[1][0]):
            wait_for(gtb.at[0:7], sem)
        assert pool.used == NUM_SEMS, pool.used

    return kernel, r, m


def weight_grads(width, slots, xt_in, dy_in, g_in, da_in, db_in, ht_in, at_in, dg_in,
                 dwg, dwu, dwd, at_out, dg_out,
                 xt, dy, g, da, db, ht, sg, su, sd, at, dg, x_sems, d_sems, g_sem, e_sems, o_sems, p_sems):
    exp_loc = da.shape[0]
    steps = dy.shape[1] // width

    def load(e, k):
        src, dst = ((da_in, da), (db_in, db), (ht_in, ht))[k]
        return pltpu.make_async_copy(src.at[e], dst.at[e], e_sems.at[e, k])

    def x_load(n):
        rows = slice(n * width, (n + 1) * width)
        return pltpu.make_async_copy(xt_in.at[rows, :], xt.at[rows, :], x_sems.at[n])

    def dy_load(n):
        cols = slice(n * width, (n + 1) * width)
        return pltpu.make_async_copy(dy_in.at[:, cols], dy.at[:, cols], d_sems.at[n])

    g_load = pltpu.make_async_copy(g_in, g, g_sem)
    x_load(0).start()
    load(0, 0).start()
    load(0, 1).start()
    for n in range(1, steps):
        x_load(n).start()
    load(0, 2).start()
    g_load.start()
    for n in range(steps):
        dy_load(n).start()
    for e in range(1, exp_loc):
        for k in range(3):
            load(e, k).start()
    passing = ((at_in, at, at_out), (dg_in, dg, dg_out))
    take = [pltpu.make_async_copy(src, mid, p_sems.at[k, 0]) for k, (src, mid, _) in enumerate(passing)]
    give = [pltpu.make_async_copy(mid, dst, p_sems.at[k, 1]) for k, (_, mid, dst) in enumerate(passing)]
    for copy in take:
        copy.start()

    def store(e, n, k):
        part = pl.ds(n * width, width)
        n = lax.rem(e, 2) * steps + n
        if k == 2:
            return pltpu.make_async_copy(sd.at[n], dwd.at[e, :, part], o_sems.at[n, k])
        return pltpu.make_async_copy((sg, su)[k].at[n], (dwg, dwu)[k].at[e, part, :], o_sems.at[n, k])

    lane = lax.broadcasted_iota(jnp.int32, g.shape, 1)

    def down(e):
        gate = jnp.sum(jnp.where(lane == e, g[...], 0.0), axis=1, keepdims=True)
        for n in range(steps):
            part = pl.ds(n * width, width)
            sd[lax.rem(e, 2) * steps + n] = dot_nn(ht[e], (gate * dy[:, part].astype(F32)).astype(BF16))
            store(e, n, 2).start()

    def step(e, _):
        @pl.when(e == 0)
        def _():
            load(e, 0).wait()
            load(e, 1).wait()
            for n in range(steps):
                x_load(n).wait()

        @pl.when(e > 0)
        def _():
            for k in range(3):
                load(e, k).wait()

        @pl.when(e > 1)
        def _():
            for n in range(steps):
                for k in range(2):
                    store(e - 2, n, k).wait()

        for n in range(steps):
            part = pl.ds(n * width, width)
            sg[lax.rem(e, 2) * steps + n] = dot_nn(xt[part, :], da[e])
            store(e, n, 0).start()
            su[lax.rem(e, 2) * steps + n] = dot_nn(xt[part, :], db[e])
            store(e, n, 1).start()

        @pl.when(e == 0)
        def _():
            load(e, 2).wait()
            g_load.wait()
            for n in range(steps):
                dy_load(n).wait()

        @pl.when(e > 1)
        def _():
            for n in range(steps):
                store(e - 2, n, 2).wait()

        @pl.when(e == 1)
        def _():
            for copy in take:
                copy.wait()
            for copy in give:
                copy.start()

        down(e)
        return 0

    lax.fori_loop(0, exp_loc, step, 0)
    for e in (exp_loc - 2, exp_loc - 1):
        for n in range(steps):
            for k in range(3):
                store(jnp.int32(e), n, k).wait()
    for copy in give:
        copy.wait()


def solution(mesh):
    num_dev = mesh.shape['ei'] * mesh.shape['eo']
    assert num_dev == NUM_DEV

    def local_step(x_tokens, expert_idx, gate_vals, dy_tokens, w_gate, w_up, w_down, x_attn, w_query, w_key, w_value, w_out):
        tok, d_model = x_tokens.shape
        top_k = expert_idx.shape[1]
        exp_loc, _, d_ff = w_gate.shape
        seq = x_attn.shape[1]
        heads, head_dim = w_query.shape[1], w_query.shape[2]
        kv_dim = w_key.shape[1] * head_dim
        q_dim = heads * head_dim
        wq = w_query.transpose(1, 2, 0).reshape(q_dim, d_model)
        wk = w_key.transpose(1, 2, 0).reshape(kv_dim, d_model)
        wv = w_value.transpose(1, 2, 0).reshape(kv_dim, d_model)
        wo = w_out.reshape(q_dim, d_model)
        kernel, r, m = make_layer_kernel(tok, d_model, d_ff, exp_loc, (seq, kv_dim, heads, head_dim))
        any_spec = pl.BlockSpec(memory_space=pl.ANY)
        vmem_spec = pl.BlockSpec(memory_space=pltpu.VMEM)
        shape = jax.ShapeDtypeStruct
        total = tok * NUM_DEV

        def half_shapes():
            return [pltpu.VMEM((d_model // 512,) + s.shape, s.dtype) for s in scatter_shapes(r, 512)]

        y0, dx0, attn, dgt, xt, dy_all, da, db, ht, gates, own, to_x, to_y, to_d = pl.pallas_call(
            kernel,
            out_shape=(shape((r, d_model), BF16), shape((r, d_model), BF16), shape((tok, d_model), BF16), shape((top_k, tok), F32),
                       shape((d_model, total), BF16), shape((HALVES, m, d_model), BF16),
                       shape((exp_loc, total, d_ff), BF16), shape((exp_loc, total, d_ff), BF16), shape((exp_loc, d_ff, total), BF16), shape((HALVES, m, LANES), F32)) + (shape((r, 2 * d_model + 512), F32),) * 4,
            in_specs=[any_spec, any_spec, any_spec, vmem_spec, vmem_spec] + [any_spec] * 7,
            out_specs=(any_spec,) * 14,
            scratch_shapes=[pltpu.VMEM((HALVES, m, d_model), BF16), pltpu.VMEM((HALVES, m, d_model), BF16), pltpu.VMEM((total, d_model), BF16),
                            pltpu.VMEM((NUM_DEV, 8, LANES), F32), pltpu.VMEM((HALVES, m, LANES), F32),
                            pltpu.VMEM((exp_loc, d_model, d_ff), BF16), pltpu.VMEM((exp_loc, d_model, d_ff), BF16), pltpu.VMEM((exp_loc, d_ff, d_model), BF16),
                            pltpu.VMEM((HALVES, m, d_model), F32), pltpu.VMEM((HALVES, m, d_model), F32), pltpu.VMEM((total, d_model), F32), pltpu.VMEM((q_dim + 2 * kv_dim, d_model), BF16), pltpu.VMEM((q_dim, d_model), BF16), pltpu.VMEM((2, 2 * tok, q_dim + 2 * kv_dim), BF16),
                            pltpu.VMEM((exp_loc, m, d_ff), F32), pltpu.VMEM((exp_loc, m, d_ff), F32), pltpu.VMEM((m, d_model), BF16),
                            pltpu.VMEM((HALVES, m, LANES), F32), pltpu.VMEM((HALVES, 2, 8, LANES), F32), pltpu.VMEM((exp_loc, m, d_ff), BF16), pltpu.VMEM((exp_loc, m, d_ff), BF16),
                            pltpu.VMEM((exp_loc, m, d_ff), BF16), pltpu.VMEM((2 * HALVES, d_ff, m), BF16), pltpu.VMEM((d_model, total), BF16), pltpu.VMEM((NUM_DEV, HALVES, 8, LANES), F32), pltpu.VMEM((NUM_DEV, 8, LANES), F32), pltpu.VMEM((HALVES, exp_loc, m, LANES), F32)]
            + [pltpu.VMEM((d_model // 512, 4 * r, 512), F32)] * 2 + half_shapes() + half_shapes() + scatter_shapes(tok, d_model)
            + [pltpu.SemaphoreType.DMA((NUM_SEMS,)), pltpu.SemaphoreType.DMA((exp_loc,)),
               pltpu.SemaphoreType.DMA(()), pltpu.SemaphoreType.DMA(()), pltpu.SemaphoreType.DMA((3,)), pltpu.SemaphoreType.DMA((2 * HALVES,)), pltpu.SemaphoreType.DMA((exp_loc,)), pltpu.SemaphoreType.DMA((2 * (d_model // 512) + 1,)), pltpu.SemaphoreType.DMA((4,)),
               pltpu.VMEM((r, d_model), BF16), pltpu.VMEM((r, d_model), BF16), pltpu.VMEM((tok, d_model), BF16), pltpu.VMEM((top_k, tok), F32)],
            compiler_params=pltpu.CompilerParams(collective_id=0, has_side_effects=True, vmem_limit_bytes=67000000),
            name='layer',
        )(x_tokens, dy_tokens, x_attn.reshape(tok, d_model), expert_idx.T, gate_vals.T, w_gate, w_up, w_down, wq, wk, wv, wo)

        width = 512
        steps = d_model // width
        slots = 2 * steps
        small = (attn, dgt)

        def swap(value, flip_y, flip_x):
            eo_size = mesh.shape['eo']
            pairs = [(g, (g // eo_size ^ flip_y) * eo_size + (g % eo_size ^ 2 * flip_x)) for g in range(NUM_DEV)]
            return lax.ppermute(value, GROUP_AXES, pairs)

        from_x, from_y, from_d = swap(to_x, 0, 1), swap(to_y, 1, 0), swap(to_d, 1, 1)
        dw_gate, dw_up, dw_down, attn, dgt = pl.pallas_call(
            functools.partial(weight_grads, width, slots),
            out_shape=(shape((exp_loc, d_model, d_ff), F32), shape((exp_loc, d_model, d_ff), F32), shape((exp_loc, d_ff, d_model), F32)) + tuple(shape(v.shape, v.dtype) for v in small),
            in_specs=[any_spec] * 8,
            out_specs=(any_spec,) * 5,
            scratch_shapes=[pltpu.VMEM((d_model, total), BF16), pltpu.VMEM((total, d_model), BF16), pltpu.VMEM((total, LANES), F32),
                            pltpu.VMEM((exp_loc, total, d_ff), BF16), pltpu.VMEM((exp_loc, total, d_ff), BF16), pltpu.VMEM((exp_loc, d_ff, total), BF16),
                            pltpu.VMEM((slots, width, d_ff), F32), pltpu.VMEM((slots, width, d_ff), F32), pltpu.VMEM((slots, d_ff, width), F32)]
            + [pltpu.VMEM(v.shape, v.dtype) for v in small]
            + [pltpu.SemaphoreType.DMA((steps,)), pltpu.SemaphoreType.DMA((steps,)), pltpu.SemaphoreType.DMA(()), pltpu.SemaphoreType.DMA((exp_loc, 3)),
               pltpu.SemaphoreType.DMA((slots, 3)), pltpu.SemaphoreType.DMA((2, 2))],
            compiler_params=pltpu.CompilerParams(vmem_limit_bytes=64500000),
            cost_estimate=pl.CostEstimate(flops=3 * 2 * total * d_model * d_ff * exp_loc, bytes_accessed=3 * 4 * exp_loc * d_model * d_ff, transcendentals=0),
            name='weight_grads',
        )(xt, dy_all.reshape(total, d_model), gates.reshape(total, LANES), da, db, ht, attn, dgt)
        def summed(first, width):
            cols = slice(first, first + width)
            return (own[:, cols] + from_x[:, cols] + from_y[:, cols] + from_d[:, cols]).astype(BF16)

        y = jnp.concatenate([y0, summed(0, d_model)], axis=0)
        dx = jnp.concatenate([jnp.concatenate([dx0[:, :d_model - 512], summed(2 * d_model, 512)], axis=1), summed(d_model, d_model)], axis=0)
        return y, dx, dgt.T, dw_gate, dw_up, dw_down, attn.reshape(x_attn.shape)

    spec_rows = P(TOKEN_AXES, None)
    spec_seqs = P(TOKEN_AXES, None, None)
    spec_experts = P(GROUP_AXES, None, None)
    spec_heads = P(None, GROUP_AXES, None)
    return jax.shard_map(local_step, mesh=mesh,
                         in_specs=(spec_rows, spec_rows, spec_rows, spec_rows, spec_experts, spec_experts, spec_experts, spec_seqs, spec_heads, spec_heads, spec_heads, spec_experts),
                         out_specs=(spec_rows, spec_rows, spec_rows, spec_seqs, spec_seqs, spec_seqs, spec_seqs),
                         check_vma=False)
```

```python
import functools

import jax
import jax.numpy as jnp
from jax import lax
from jax.experimental import pallas as pl
from jax.experimental.pallas import tpu as pltpu
from jax.sharding import PartitionSpec as P

GROUP_AXES = ('ei', 'eo')
TOKEN_AXES = ('dp', 'ei', 'eo')
F32 = jnp.float32
BF16 = jnp.bfloat16
MESH_ID = pl.DeviceIdType.MESH
HALVES = 2
NUM_DEV = 8
LANES = 128


def dot_nn(lhs, rhs):
    return jnp.dot(lhs, rhs, preferred_element_type=F32)


def dot_nt(lhs, rhs):
    return lax.dot_general(lhs, rhs, (((1,), (1,)), ((), ())), preferred_element_type=F32)


def dot_tn(lhs, rhs):
    return lax.dot_general(lhs, rhs, (((0,), (0,)), ((), ())), preferred_element_type=F32)


class Place:
    def __init__(self):
        i = lax.axis_index('ei')
        o = lax.axis_index('eo')
        x = lax.div(o, 2)
        c = lax.rem(o, 2)
        self.core = c
        self.chip = i * 2 + x
        self.dev = {}
        self.block = {}
        self.flat = {}
        self.pair = {}
        self.chips = {}
        for flip_y in (0, 1):
            for flip_x in (0, 1):
                for flip_c in (0, 1):
                    yy = 1 - i if flip_y else i
                    xx = 1 - x if flip_x else x
                    cc = 1 - c if flip_c else c
                    name = ('y' if flip_y else '') + ('x' if flip_x else '') + ('c' if flip_c else '')
                    self.dev[name] = (0, yy, xx * 2 + cc)
                    self.block[name] = cc * 4 + yy * 2 + xx
                    self.flat[name] = yy * 4 + xx * 2 + cc
                    self.pair[name] = (yy * 2 + xx) * 2 + cc
                    self.chips[name] = yy * 2 + xx


class Pool:
    def __init__(self, sems):
        self.sems, self.used = sems, 0

    def take(self):
        self.used += 1
        return self.sems.at[self.used - 1]


def send(src, dst, device, sent, landed):
    return pltpu.make_async_remote_copy(src_ref=src, dst_ref=dst, send_sem=sent, recv_sem=landed, device_id=device, device_id_type=MESH_ID)


def wait_for(ref, sem):
    pltpu.make_async_copy(ref, ref, sem).wait()


class Gather:
    def __init__(self, pool, place, buf, rows, index, split=False):
        def at(name, lo=0, n=rows):
            return buf.at[pl.ds(pl.multiple_of(index[name] * rows + lo, 8), n), :]

        half = rows // 2
        own = at('')
        dev = place.dev
        self.buf, self.rows, self.relayed = buf, rows, False
        self.sent, self.relays_sent, self.near, self.relays = (pool.take() for _ in range(4))
        self.over = [pool.take() for _ in range(4)] if split else [pool.take()] * 4
        self.to_x = send(own, own, dev['x'], self.sent, self.near)
        self.to_y = send(own, own, dev['y'], self.sent, self.near)
        self.to_c = send(own, own, dev['c'], self.sent, self.over[0])
        self.relay_x = send(at('y', 0, half), at('y', 0, half), dev['x'], self.relays_sent, self.relays)
        self.relay_y = send(at('x', half, half), at('x', half, half), dev['y'], self.relays_sent, self.relays)
        self.core_x = send(at('x'), at('x'), dev['c'], self.sent, self.over[1])
        self.core_y = send(at('y'), at('y'), dev['c'], self.sent, self.over[2])
        self.core_d = send(at('yx'), at('yx'), dev['c'], self.sent, self.over[3])

    def blocks(self, count):
        return self.buf.at[0:count * self.rows, :]

    def begin_links(self):
        self.to_x.start()
        self.to_y.start()

    def begin_core(self):
        self.to_c.start()

    def begin(self):
        self.begin_links()
        self.begin_core()

    def relay(self):
        wait_for(self.blocks(2), self.near)
        self.relay_x.start()
        self.relay_y.start()
        self.core_x.start()
        self.core_y.start()

    def relay_left(self):
        self.relayed = True
        wait_for(self.blocks(1), self.relays_sent)

    def last(self):
        wait_for(self.blocks(1), self.relays)
        self.core_d.start()

    def crossed(self, k):
        wait_for(self.blocks(1), self.over[k])

    def finish(self):
        wait_for(self.blocks(4), self.over[0])

    def drain(self):
        wait_for(self.blocks(6), self.sent)
        if not self.relayed:
            wait_for(self.blocks(1), self.relays_sent)


class Scatter:
    def __init__(self, pool, place, part, from_core, from_x, from_y, last_x, last_y, rows, first=0):
        half = rows // 2
        self.half, self.part, self.rows, self.place = half, part, rows, place
        self.from_core, self.from_x, self.from_y, self.last_x, self.last_y = from_core, from_x, from_y, last_x, last_y
        four = 4 * rows
        self.mine = pl.multiple_of(place.core * four, 8)
        self.cols = pl.ds(first, from_core.shape[-1])
        other = part.at[pl.ds(pl.multiple_of((1 - place.core) * four, 8), four), self.cols]
        dev = place.dev
        self.sent, self.crossed, self.first_x, self.first_y, self.rest = (pool.take() for _ in range(5))
        self.core = send(other, from_core, dev['c'], self.sent, self.crossed)
        self.x0 = send(self.at('x', 0), from_x.at[0], dev['x'], self.sent, self.rest)
        self.x1 = send(self.at('yx', 0), from_x.at[1], dev['x'], self.sent, self.first_x)
        self.y0 = send(self.at('y', half), from_y.at[0], dev['y'], self.sent, self.rest)
        self.y1 = send(self.at('yx', half), from_y.at[1], dev['y'], self.sent, self.first_y)
        self.end_y = send(self.at('y', 0), last_y, dev['y'], self.sent, self.rest)
        self.end_x = send(self.at('x', half), last_x, dev['x'], self.sent, self.rest)

    def at(self, name, lo):
        return self.part.at[pl.ds(pl.multiple_of(self.place.block[name] * self.rows + lo, 8), self.half), self.cols]

    def begin(self):
        self.core.start()

    def middle(self):
        wait_for(self.from_core, self.crossed)
        mine = pl.ds(self.mine, 4 * self.rows)
        self.part[mine, self.cols] = self.part[mine, self.cols] + self.from_core[...]
        self.x1.start()
        self.y1.start()
        self.x0.start()
        self.y0.start()

    def late(self):
        wait_for(self.from_x.at[1], self.first_x)
        here = self.at('y', 0)
        here[...] = here[...] + self.from_x[1]
        self.end_y.start()
        wait_for(self.from_y.at[1], self.first_y)
        here = self.at('x', self.half)
        here[...] = here[...] + self.from_y[1]
        self.end_x.start()

    def finish(self, out, row=0):
        half = self.half
        wait_for(self.part.at[0:4 * half, self.cols], self.rest)
        out[row:row + half, self.cols] = (self.at('', 0)[...] + self.from_x[0] + self.last_y[...]).astype(BF16)
        out[row + half:row + 2 * half, self.cols] = (self.at('', half)[...] + self.from_y[0] + self.last_x[...]).astype(BF16)

    def drain(self):
        wait_for(self.part.at[0:7 * self.rows, self.cols], self.sent)


class ChipSum:
    def __init__(self, pool, place, part, from_core, rows, first, outs, sem):
        four = 4 * rows
        self.part, self.from_core, self.sem = part, from_core, sem
        self.mine = pl.multiple_of(place.core * four, 8)
        self.cols = pl.ds(first, from_core.shape[-1])
        other = part.at[pl.ds(pl.multiple_of((1 - place.core) * four, 8), four), self.cols]
        self.sent, self.crossed = pool.take(), pool.take()
        self.core = send(other, from_core, place.dev['c'], self.sent, self.crossed)
        self.copies = [pltpu.make_async_copy(part.at[pl.ds(pl.multiple_of(place.block[name] * rows, 8), rows), self.cols], out, sem)
                       for name, out in outs]

    def begin(self):
        self.core.start()

    def middle(self):
        wait_for(self.from_core, self.crossed)
        mine = pl.ds(self.mine, self.from_core.shape[0])
        self.part[mine, self.cols] = self.part[mine, self.cols] + self.from_core[...]
        for copy in self.copies:
            copy.start()

    def drain(self):
        wait_for(self.from_core, self.sent)
        wait_for(self.from_core, self.sem)


def scatter_shapes(rows, width):
    half = rows // 2
    return [pltpu.VMEM((4 * rows, width), F32), pltpu.VMEM((2, half, width), F32), pltpu.VMEM((2, half, width), F32),
            pltpu.VMEM((half, width), F32), pltpu.VMEM((half, width), F32)]


NUM_SEMS = 2 + 4 + 5 * 4 + 8 + 5 * 6 + 2 * 7


def attention_qkv(xa, wqkv, qkv, chip, seq):
    pair = 2 * seq
    qkv[...] = dot_nt(xa[pl.ds(pl.multiple_of(chip * pair, pair), pair), :], wqkv[...]).astype(BF16)


def attention_out(qkv, wo, part, chip, chips, dims):
    seq, kv_dim, heads, head_dim = dims
    q_dim = heads * head_dim
    pair = 2 * seq
    row = lax.broadcasted_iota(jnp.int32, (pair, pair), 0)
    col = lax.broadcasted_iota(jnp.int32, (pair, pair), 1)
    causal = (row >= col) & ((row >= seq) == (col >= seq))
    keys = qkv[:, q_dim:q_dim + kv_dim]
    vals = qkv[:, q_dim + kv_dim:q_dim + 2 * kv_dim]
    outs = []
    for h in range(heads):
        scores = dot_nt(qkv[:, h * head_dim:(h + 1) * head_dim], keys) * head_dim ** -0.5
        scores = jnp.where(causal, scores, -1e30)
        top = jnp.max(scores, axis=1, keepdims=True)
        ex = jnp.exp(scores - top)
        probs = (ex / jnp.sum(ex, axis=1, keepdims=True)).astype(BF16)
        outs.append(dot_nn(probs, vals).astype(BF16))
    out = dot_nn(jnp.concatenate(outs, axis=1), wo[...])
    for c in range(2):
        part[pl.ds(pl.multiple_of((c * chips + chip) * seq, seq), seq), :] = out[c * seq:(c + 1) * seq, :]


def make_layer_kernel(tok, d_model, d_ff, exp_loc, attn_dims):
    r = tok // HALVES
    m = r * NUM_DEV
    tile = 512
    tiles = d_model // tile

    def kernel(x_in, dy_in, xa_in, idx_in, gate_in, wg_in, wu_in, wd_in, wq_in, wk_in, wv_in, wo_in,
               y_out, dx_out, attn_out, dg_out, xt_all, dy_all, da_all, db_all, ht_all, gates_out, own_out, to_x_out, to_y_out, to_d_out,
               xb, dyb, xab, gtb, gcol, wg, wu, wd, y_part, dx_part, at_part, wqkv, wo, qkv, s1, s2, d_o, dgc, dgt, da, db, hid, stage_t, xt, dgl, gtab, gfull,
               ryc, rdc, ry0, ry1, ry2, ry3, ry4, rd0, rd1, rd2, rd3, rd4, ra0, ra1, ra2, ra3, ra4,
               sems, w_sems, in_sems, aw_sems, out_sems, stage_sems, grad_sems, sum_sems, res_sems, y_res, dx_res, attn_res, dg_res):
        place = Place()
        pool = Pool(sems)
        dev, block = place.dev, place.block
        me = block['']

        def own_rows(buf, rows, index=me):
            return buf.at[pl.ds(pl.multiple_of(index * rows, 8), rows), :]

        loads = []
        for h in range(HALVES):
            loads.append(pltpu.make_async_copy(x_in.at[h * r:(h + 1) * r, :], own_rows(xb.at[h], r), in_sems))
            loads.append(pltpu.make_async_copy(dy_in.at[h * r:(h + 1) * r, :], own_rows(dyb.at[h], r), in_sems))
        loads.append(pltpu.make_async_copy(xa_in, own_rows(xab, tok, place.pair['']), in_sems))
        for load in loads:
            load.start()
        q_dim, kv_dim = wq_in.shape[0], wk_in.shape[0]
        attn_loads = [pltpu.make_async_copy(wq_in, wqkv.at[0:q_dim, :], aw_sems), pltpu.make_async_copy(wk_in, wqkv.at[q_dim:q_dim + kv_dim, :], aw_sems),
                      pltpu.make_async_copy(wv_in, wqkv.at[q_dim + kv_dim:q_dim + 2 * kv_dim, :], aw_sems), pltpu.make_async_copy(wo_in, wo, aw_sems)]
        for load in attn_loads:
            load.start()
        weights = []
        for e in range(exp_loc):
            weights.append([pltpu.make_async_copy(src.at[e], dst.at[e], w_sems.at[e]) for src, dst in ((wg_in, wg), (wu_in, wu), (wd_in, wd))])
        barrier = pltpu.get_barrier_semaphore()
        peers = [name for name in dev if name]
        for name in peers:
            pl.semaphore_signal(barrier, inc=1, device_id=dev[name], device_id_type=MESH_ID)
        gtab[...] = jnp.zeros_like(gtab)
        for g in range(NUM_DEV):
            for e in range(exp_loc):
                gtab[g, e:e + 1, 0:tok] = jnp.max(jnp.where(idx_in[...] == g * exp_loc + e, gate_in[...], -1.0), axis=0, keepdims=True)
        pl.semaphore_wait(barrier, len(peers))

        routes_sent, routes_in = pool.take(), pool.take()
        routes = [send(gtab.at[place.flat[name]], gtb.at[me], dev[name], routes_sent, routes_in) for name in peers]
        gx = [Gather(pool, place, xb.at[h], r, block) for h in range(HALVES)]
        gdy = [Gather(pool, place, dyb.at[h], r, block) for h in range(HALVES)]
        gxa = Gather(pool, place, xab, tok, place.pair, split=True)
        def passed(k):
            return [(name, out.at[:, k * tile:(k + 1) * tile]) for name, out in (('', own_out), ('x', to_x_out), ('y', to_y_out), ('yx', to_d_out))]

        def chip_sum(part, from_core, n, k):
            return ChipSum(pool, place, part, from_core, r, n * tile, passed(k), sum_sems.at[k])

        sy = [[Scatter(pool, place, y_part.at[0], ry0.at[n], ry1.at[n], ry2.at[n], ry3.at[n], ry4.at[n], r, n * tile) for n in range(tiles)],
              [chip_sum(y_part.at[1], ryc.at[n], n, n) for n in range(tiles)]]
        sdx = [[Scatter(pool, place, dx_part.at[0], rd0.at[n], rd1.at[n], rd2.at[n], rd3.at[n], rd4.at[n], r, n * tile) for n in range(tiles - 1)]
               + [chip_sum(dx_part.at[0], rd0.at[tiles - 1], tiles - 1, 2 * tiles)],
               [chip_sum(dx_part.at[1], rdc.at[n], n, tiles + n) for n in range(tiles)]]
        sat = Scatter(pool, place, at_part, ra0, ra1, ra2, ra3, ra4, tok)
        dg_sems = [(pool.take(), pool.take()) for _ in range(HALVES)]
        dg_links = [[send(dgt.at[h, 1 - place.core if 'c' in name else place.core], dgl.at[me, h], dev[name], *dg_sems[h]) for name in peers] for h in range(HALVES)]

        wait_for(xab.at[0:3 * tok, :], in_sems)
        gx[0].begin()
        gxa.begin_core()
        for link in routes:
            link.start()
        gtb[me] = gtab[place.flat['']]
        for ws in weights:
            for w in ws:
                w.start()
        dgc[...] = jnp.zeros_like(dgc)
        gcol[...] = jnp.zeros_like(gcol)
        wait_for(xab, aw_sems)

        def pairs(names, between=None):
            for k, name in enumerate(names):
                attention_qkv(xab, wqkv, qkv.at[k], place.chips[name], tok)
            if between is not None:
                between()
            for k, name in enumerate(names):
                attention_out(qkv.at[k], wo, at_part, place.chips[name], NUM_DEV // 2, attn_dims)

        gxa.crossed(0)
        pairs(('',))
        gx[0].relay()
        wait_for(gtb.at[0:7], routes_in)
        wide = jnp.concatenate([gtb[...].reshape(NUM_DEV * 8, LANES), jnp.zeros((LANES - NUM_DEV * 8, LANES), F32)], axis=0).T
        for h in range(HALVES):
            for b in range(NUM_DEV):
                gcol[h, b * r:(b + 1) * r, 0:8] = wide[h * r:(h + 1) * r, b * 8:(b + 1) * 8]
            for e in range(exp_loc):
                gfull[h, e] = jnp.broadcast_to(gcol[h][:, e:e + 1], (m, LANES))
        gx[0].relay_left()
        gxa.begin_links()
        gx[0].last()
        gx[0].finish()

        def staged(h, e, k):
            part = pl.ds(h * m, m)
            if k == 2:
                slot = h * 2 + lax.rem(e, 2)
                return pltpu.make_async_copy(stage_t.at[slot], ht_all.at[e, :, part], stage_sems.at[slot])
            return pltpu.make_async_copy((da, db)[k].at[e], (da_all, db_all)[k].at[e, part, :], grad_sems.at[e])

        lane = lax.broadcasted_iota(jnp.int32, (m, LANES), 1)

        def gate_of(h, e):
            return jnp.concatenate([jnp.maximum(gfull[h, e], 0.0)] * (tile // LANES), axis=1)

        def loop(count, events, body):
            def step(k, _):
                for at, event in events.items():
                    pl.when(k == at)(event)
                body(k)
                return 0

            lax.fori_loop(0, count, step, 0)

        def hidden(h):
            def body(e):
                if h == 0:
                    wait_for(wg.at[0:3], w_sems.at[e])

                @pl.when(e >= 2)
                def _():
                    staged(h, e - 2, 2).wait()

                mask = jnp.concatenate([gfull[h, e]] * (tile // LANES), axis=1) >= 0.0
                a = jnp.where(mask, dot_nn(xb[h], wg[e]), 0.0)
                b = jnp.where(mask, dot_nn(xb[h], wu[e]), 0.0)
                sig = jax.nn.sigmoid(a)
                act = a * sig
                hid[e] = (act * b).astype(BF16)
                stage_t[h * 2 + lax.rem(e, 2)] = hid[e].T
                s1[e] = b * sig * (1.0 + a * (1.0 - sig))
                s2[e] = act
                staged(h, e, 2).start()

            return body

        def outputs(h):
            def body(n):
                cols = pl.ds(pl.multiple_of(n * tile, tile), tile)
                dy = dyb[h, :, cols].astype(F32)
                sums = dgc[h]
                for e in range(exp_loc):
                    o = dot_nn(hid[e], wd[e, :, cols]).astype(BF16).astype(F32)
                    y = gate_of(h, e) * o
                    y_part[h, :, cols] = y if e == 0 else y_part[h, :, cols] + y
                    prod = dy * o
                    dots = prod[:, 0:LANES]
                    for k in range(1, tile // LANES):
                        dots += prod[:, k * LANES:(k + 1) * LANES]
                    sums += jnp.where(lane == e, jnp.sum(dots, axis=1, keepdims=True), 0.0)
                dgc[h] = sums

            return body

        def hidden_grads(h):
            def body(e):
                if h:
                    wait_for(da.at[0:2], grad_sems.at[e])
                for n in range(tiles):
                    cols = pl.ds(n * tile, tile)
                    d_o[:, cols] = (gate_of(h, e) * dyb[h, :, cols].astype(F32)).astype(BF16)
                dh = dot_nt(d_o[...], wd[e]).astype(BF16).astype(F32)
                da[e] = (dh * s1[e]).astype(BF16)
                db[e] = (dh * s2[e]).astype(BF16)
                for k in range(2):
                    staged(h, e, k).start()

            return body

        def input_grads(h):
            def body(n):
                cols = pl.ds(pl.multiple_of(n * tile, tile), tile)
                for e in range(exp_loc):
                    dxe = (dot_nt(da[e], wg[e, cols, :]) + dot_nt(db[e], wu[e, cols, :])).astype(BF16).astype(F32)
                    dx_part[h, :, cols] = dxe if e == 0 else dx_part[h, :, cols] + dxe

            return body

        def send_dg(h):
            turned = dgc[h].T
            for c in range(2):
                dgt[h, c] = turned[0:8, c * LANES:(c + 1) * LANES]
            for link in dg_links[h]:
                link.start()
            dgl[me, h] = dgt[h, place.core]

        def dg_read():
            for h in range(HALVES):
                wait_for(gtb.at[0:7], dg_sems[h][1])
            for h in range(HALVES):
                slots = idx_in[:, h * r:(h + 1) * r]
                total = jnp.zeros(slots.shape, F32)
                for b in range(NUM_DEV):
                    first = ((b // 2) % 2 * 4 + b % 2 * 2 + b // 4) * exp_loc
                    rows = dgl[b, h]
                    mine = jnp.zeros((8, r), F32)
                    for q in range(LANES // r):
                        mine = jnp.where(place.chip == q, rows[:, q * r:(q + 1) * r], mine)
                    for e in range(exp_loc):
                        total = jnp.where(slots == first + e, mine[e:e + 1, :], total)
                dg_res[:, h * r:(h + 1) * r] = total

        def seq(*calls):
            def run():
                for call in calls:
                    call()

            return run

        loop(exp_loc, {0: gdy[0].begin, 3: gxa.relay}, hidden(0))
        gxa.crossed(1)
        gxa.crossed(2)
        pairs(('x', 'y'), seq(gdy[0].relay, gxa.last))
        gx[1].begin()
        gdy[1].begin()
        gxa.crossed(3)
        pairs(('yx',), gdy[0].last)
        sat.begin()
        gdy[0].finish()
        loop(tiles, {1: seq(gx[1].relay, sy[0][0].begin), 2: seq(gdy[1].relay, sat.middle, sy[0][1].begin)}, outputs(0))
        sy[0][2].begin()
        send_dg(0)
        loop(exp_loc, {1: sy[0][0].middle, 2: gx[1].last, 3: sy[0][1].middle, 4: sy[0][2].middle}, hidden_grads(0))
        loop(tiles, {1: seq(gx[1].finish, sdx[0][0].begin), 2: seq(gdy[1].last, sdx[0][1].begin)}, input_grads(0))
        sdx[0][2].begin()
        loop(exp_loc, {1: seq(sdx[0][0].middle, sdx[0][1].middle), 2: seq(gdy[1].finish, sdx[0][2].middle)}, hidden(1))
        sat.late()
        loop(tiles, {1: seq(sy[0][0].late, sy[1][0].begin), 2: seq(sy[0][1].late, sy[0][2].late, sy[1][1].begin)}, outputs(1))
        sy[1][2].begin()
        send_dg(1)
        for h in range(HALVES):
            xt[:, h * m:(h + 1) * m] = xb[h].T
        saves = [pltpu.make_async_copy(xt, xt_all, out_sems.at[0]), pltpu.make_async_copy(dyb, dy_all, out_sems.at[1]), pltpu.make_async_copy(gcol, gates_out, out_sems.at[2])]
        for save in saves:
            save.start()
        loop(exp_loc, {0: sdx[0][0].late, 1: seq(sy[1][0].middle, sdx[0][1].late), 3: seq(sy[1][1].middle, sy[1][2].middle)}, hidden_grads(1))
        loop(tiles, {1: sdx[1][0].begin, 2: seq(sdx[1][1].begin, sdx[1][0].middle)}, input_grads(1))
        sdx[1][2].begin()
        sdx[1][1].middle()
        for s in sy[0]:
            s.finish(y_res)
        sat.finish(attn_res)
        for s in sdx[0][:-1]:
            s.finish(dx_res)
        dx_res[:, (tiles - 1) * tile:] = jnp.zeros((r, tile), BF16)
        dg_read()
        results = [pltpu.make_async_copy(src, dst, res_sems.at[k]) for k, (src, dst) in enumerate(((y_res, y_out), (dx_res, dx_out), (attn_res, attn_out), (dg_res, dg_out)))]
        for result in results:
            result.start()
        sdx[1][2].middle()
        for save in saves + results:
            save.wait()
        for e in range(exp_loc):
            wait_for(da.at[0:2], grad_sems.at[e])
        for h in range(HALVES):
            for e in (exp_loc - 2, exp_loc - 1):
                staged(h, jnp.int32(e), 2).wait()
        for item in gx + gdy + [gxa, sat] + sum(sy + sdx, []):
            item.drain()
        for sem in (routes_sent, dg_sems[0][0], dg_sems[1][0]):
            wait_for(gtb.at[0:7], sem)
        assert pool.used == NUM_SEMS, pool.used

    return kernel, r, m


def weight_grads(width, slots, xt_in, dy_in, g_in, da_in, db_in, ht_in, at_in, dg_in,
                 dwg, dwu, dwd, at_out, dg_out,
                 xt, dy, g, da, db, ht, sg, su, sd, at, dg, x_sems, d_sems, g_sem, e_sems, o_sems, p_sems):
    exp_loc = da.shape[0]
    steps = dy.shape[1] // width

    def load(e, k):
        src, dst = ((da_in, da), (db_in, db), (ht_in, ht))[k]
        return pltpu.make_async_copy(src.at[e], dst.at[e], e_sems.at[e, k])

    def x_load(n):
        rows = slice(n * width, (n + 1) * width)
        return pltpu.make_async_copy(xt_in.at[rows, :], xt.at[rows, :], x_sems.at[n])

    def dy_load(n):
        cols = slice(n * width, (n + 1) * width)
        return pltpu.make_async_copy(dy_in.at[:, cols], dy.at[:, cols], d_sems.at[n])

    g_load = pltpu.make_async_copy(g_in, g, g_sem)
    x_load(0).start()
    load(0, 0).start()
    load(0, 1).start()
    for n in range(1, steps):
        x_load(n).start()
    load(0, 2).start()
    g_load.start()
    for n in range(steps):
        dy_load(n).start()
    for e in range(1, exp_loc):
        for k in range(3):
            load(e, k).start()
    passing = ((at_in, at, at_out), (dg_in, dg, dg_out))
    take = [pltpu.make_async_copy(src, mid, p_sems.at[k, 0]) for k, (src, mid, _) in enumerate(passing)]
    give = [pltpu.make_async_copy(mid, dst, p_sems.at[k, 1]) for k, (_, mid, dst) in enumerate(passing)]
    for copy in take:
        copy.start()

    def store(e, n, k):
        part = pl.ds(n * width, width)
        n = lax.rem(e, 2) * steps + n
        if k == 2:
            return pltpu.make_async_copy(sd.at[n], dwd.at[e, :, part], o_sems.at[n, k])
        return pltpu.make_async_copy((sg, su)[k].at[n], (dwg, dwu)[k].at[e, part, :], o_sems.at[n, k])

    lane = lax.broadcasted_iota(jnp.int32, g.shape, 1)

    def down(e):
        gate = jnp.maximum(jnp.sum(jnp.where(lane == e, g[...], 0.0), axis=1, keepdims=True), 0.0)
        for n in range(steps):
            part = pl.ds(n * width, width)
            sd[lax.rem(e, 2) * steps + n] = dot_nn(ht[e], (gate * dy[:, part].astype(F32)).astype(BF16))
            store(e, n, 2).start()

    def step(e, _):
        @pl.when(e == 0)
        def _():
            load(e, 0).wait()
            load(e, 1).wait()
            for n in range(steps):
                x_load(n).wait()

        @pl.when(e > 0)
        def _():
            for k in range(3):
                load(e, k).wait()

        @pl.when(e > 1)
        def _():
            for n in range(steps):
                for k in range(2):
                    store(e - 2, n, k).wait()

        for n in range(steps):
            part = pl.ds(n * width, width)
            sg[lax.rem(e, 2) * steps + n] = dot_nn(xt[part, :], da[e])
            store(e, n, 0).start()
            su[lax.rem(e, 2) * steps + n] = dot_nn(xt[part, :], db[e])
            store(e, n, 1).start()

        @pl.when(e == 0)
        def _():
            load(e, 2).wait()
            g_load.wait()
            for n in range(steps):
                dy_load(n).wait()

        @pl.when(e > 1)
        def _():
            for n in range(steps):
                store(e - 2, n, 2).wait()

        @pl.when(e == 1)
        def _():
            for copy in take:
                copy.wait()
            for copy in give:
                copy.start()

        down(e)
        return 0

    lax.fori_loop(0, exp_loc, step, 0)
    for e in (exp_loc - 2, exp_loc - 1):
        for n in range(steps):
            for k in range(3):
                store(jnp.int32(e), n, k).wait()
    for copy in give:
        copy.wait()


def solution(mesh):
    num_dev = mesh.shape['ei'] * mesh.shape['eo']
    assert num_dev == NUM_DEV

    def local_step(x_tokens, expert_idx, gate_vals, dy_tokens, w_gate, w_up, w_down, x_attn, w_query, w_key, w_value, w_out):
        tok, d_model = x_tokens.shape
        top_k = expert_idx.shape[1]
        exp_loc, _, d_ff = w_gate.shape
        seq = x_attn.shape[1]
        heads, head_dim = w_query.shape[1], w_query.shape[2]
        kv_dim = w_key.shape[1] * head_dim
        q_dim = heads * head_dim
        wq = w_query.transpose(1, 2, 0).reshape(q_dim, d_model)
        wk = w_key.transpose(1, 2, 0).reshape(kv_dim, d_model)
        wv = w_value.transpose(1, 2, 0).reshape(kv_dim, d_model)
        wo = w_out.reshape(q_dim, d_model)
        kernel, r, m = make_layer_kernel(tok, d_model, d_ff, exp_loc, (seq, kv_dim, heads, head_dim))
        any_spec = pl.BlockSpec(memory_space=pl.ANY)
        vmem_spec = pl.BlockSpec(memory_space=pltpu.VMEM)
        shape = jax.ShapeDtypeStruct
        total = tok * NUM_DEV

        def half_shapes():
            return [pltpu.VMEM((d_model // 512,) + s.shape, s.dtype) for s in scatter_shapes(r, 512)]

        y0, dx0, attn, dgt, xt, dy_all, da, db, ht, gates, own, to_x, to_y, to_d = pl.pallas_call(
            kernel,
            out_shape=(shape((r, d_model), BF16), shape((r, d_model), BF16), shape((tok, d_model), BF16), shape((top_k, tok), F32),
                       shape((d_model, total), BF16), shape((HALVES, m, d_model), BF16),
                       shape((exp_loc, total, d_ff), BF16), shape((exp_loc, total, d_ff), BF16), shape((exp_loc, d_ff, total), BF16), shape((HALVES, m, LANES), F32)) + (shape((r, 2 * d_model + 512), F32),) * 4,
            in_specs=[any_spec, any_spec, any_spec, vmem_spec, vmem_spec] + [any_spec] * 7,
            out_specs=(any_spec,) * 14,
            scratch_shapes=[pltpu.VMEM((HALVES, m, d_model), BF16), pltpu.VMEM((HALVES, m, d_model), BF16), pltpu.VMEM((total, d_model), BF16),
                            pltpu.VMEM((NUM_DEV, 8, LANES), F32), pltpu.VMEM((HALVES, m, LANES), F32),
                            pltpu.VMEM((exp_loc, d_model, d_ff), BF16), pltpu.VMEM((exp_loc, d_model, d_ff), BF16), pltpu.VMEM((exp_loc, d_ff, d_model), BF16),
                            pltpu.VMEM((HALVES, m, d_model), F32), pltpu.VMEM((HALVES, m, d_model), F32), pltpu.VMEM((total, d_model), F32), pltpu.VMEM((q_dim + 2 * kv_dim, d_model), BF16), pltpu.VMEM((q_dim, d_model), BF16), pltpu.VMEM((2, 2 * tok, q_dim + 2 * kv_dim), BF16),
                            pltpu.VMEM((exp_loc, m, d_ff), F32), pltpu.VMEM((exp_loc, m, d_ff), F32), pltpu.VMEM((m, d_model), BF16),
                            pltpu.VMEM((HALVES, m, LANES), F32), pltpu.VMEM((HALVES, 2, 8, LANES), F32), pltpu.VMEM((exp_loc, m, d_ff), BF16), pltpu.VMEM((exp_loc, m, d_ff), BF16),
                            pltpu.VMEM((exp_loc, m, d_ff), BF16), pltpu.VMEM((2 * HALVES, d_ff, m), BF16), pltpu.VMEM((d_model, total), BF16), pltpu.VMEM((NUM_DEV, HALVES, 8, LANES), F32), pltpu.VMEM((NUM_DEV, 8, LANES), F32), pltpu.VMEM((HALVES, exp_loc, m, LANES), F32)]
            + [pltpu.VMEM((d_model // 512, 4 * r, 512), F32)] * 2 + half_shapes() + half_shapes() + scatter_shapes(tok, d_model)
            + [pltpu.SemaphoreType.DMA((NUM_SEMS,)), pltpu.SemaphoreType.DMA((exp_loc,)),
               pltpu.SemaphoreType.DMA(()), pltpu.SemaphoreType.DMA(()), pltpu.SemaphoreType.DMA((3,)), pltpu.SemaphoreType.DMA((2 * HALVES,)), pltpu.SemaphoreType.DMA((exp_loc,)), pltpu.SemaphoreType.DMA((2 * (d_model // 512) + 1,)), pltpu.SemaphoreType.DMA((4,)),
               pltpu.VMEM((r, d_model), BF16), pltpu.VMEM((r, d_model), BF16), pltpu.VMEM((tok, d_model), BF16), pltpu.VMEM((top_k, tok), F32)],
            compiler_params=pltpu.CompilerParams(collective_id=0, has_side_effects=True, vmem_limit_bytes=67000000),
            name='layer',
        )(x_tokens, dy_tokens, x_attn.reshape(tok, d_model), expert_idx.T, gate_vals.T, w_gate, w_up, w_down, wq, wk, wv, wo)

        width = 512
        steps = d_model // width
        slots = 2 * steps
        small = (attn, dgt)

        def swap(value, flip_y, flip_x):
            eo_size = mesh.shape['eo']
            pairs = [(g, (g // eo_size ^ flip_y) * eo_size + (g % eo_size ^ 2 * flip_x)) for g in range(NUM_DEV)]
            return lax.ppermute(value, GROUP_AXES, pairs)

        from_x, from_y, from_d = swap(to_x, 0, 1), swap(to_y, 1, 0), swap(to_d, 1, 1)
        dw_gate, dw_up, dw_down, attn, dgt = pl.pallas_call(
            functools.partial(weight_grads, width, slots),
            out_shape=(shape((exp_loc, d_model, d_ff), F32), shape((exp_loc, d_model, d_ff), F32), shape((exp_loc, d_ff, d_model), F32)) + tuple(shape(v.shape, v.dtype) for v in small),
            in_specs=[any_spec] * 8,
            out_specs=(any_spec,) * 5,
            scratch_shapes=[pltpu.VMEM((d_model, total), BF16), pltpu.VMEM((total, d_model), BF16), pltpu.VMEM((total, LANES), F32),
                            pltpu.VMEM((exp_loc, total, d_ff), BF16), pltpu.VMEM((exp_loc, total, d_ff), BF16), pltpu.VMEM((exp_loc, d_ff, total), BF16),
                            pltpu.VMEM((slots, width, d_ff), F32), pltpu.VMEM((slots, width, d_ff), F32), pltpu.VMEM((slots, d_ff, width), F32)]
            + [pltpu.VMEM(v.shape, v.dtype) for v in small]
            + [pltpu.SemaphoreType.DMA((steps,)), pltpu.SemaphoreType.DMA((steps,)), pltpu.SemaphoreType.DMA(()), pltpu.SemaphoreType.DMA((exp_loc, 3)),
               pltpu.SemaphoreType.DMA((slots, 3)), pltpu.SemaphoreType.DMA((2, 2))],
            compiler_params=pltpu.CompilerParams(vmem_limit_bytes=64500000),
            cost_estimate=pl.CostEstimate(flops=3 * 2 * total * d_model * d_ff * exp_loc, bytes_accessed=3 * 4 * exp_loc * d_model * d_ff, transcendentals=0),
            name='weight_grads',
        )(xt, dy_all.reshape(total, d_model), gates.reshape(total, LANES), da, db, ht, attn, dgt)
        def summed(first, width):
            cols = slice(first, first + width)
            return (own[:, cols] + from_x[:, cols] + from_y[:, cols] + from_d[:, cols]).astype(BF16)

        y = jnp.concatenate([y0, summed(0, d_model)], axis=0)
        dx = jnp.concatenate([jnp.concatenate([dx0[:, :d_model - 512], summed(2 * d_model, 512)], axis=1), summed(d_model, d_model)], axis=0)
        return y, dx, dgt.T, dw_gate, dw_up, dw_down, attn.reshape(x_attn.shape)

    spec_rows = P(TOKEN_AXES, None)
    spec_seqs = P(TOKEN_AXES, None, None)
    spec_experts = P(GROUP_AXES, None, None)
    spec_heads = P(None, GROUP_AXES, None)
    return jax.shard_map(local_step, mesh=mesh,
                         in_specs=(spec_rows, spec_rows, spec_rows, spec_rows, spec_experts, spec_experts, spec_experts, spec_seqs, spec_heads, spec_heads, spec_heads, spec_experts),
                         out_specs=(spec_rows, spec_rows, spec_rows, spec_seqs, spec_seqs, spec_seqs, spec_seqs),
                         check_vma=False)
```
